16 devices in a mesh: dp: 2 (over z), ep: 8 (over y, x, core).
Axes of the slice: x: 2, y: 2, z: 2, core: 2. Of those that a mesh axis runs over, the one named last changes fastest.
Arguments:
- hidden: bfloat16 [4096, 1536], P(('dp', 'ep')), parts along dimension 0
- router_w: float32 [1536, 32], replicated
- expert_ids: int32 [4096, 2], P(('dp', 'ep')), parts along dimension 0
- w_gate: bfloat16 [32, 1536, 2304], P('ep')
- w_up: bfloat16 [32, 1536, 2304], P('ep')
- w_down: bfloat16 [32, 2304, 1536], P('ep')
- post_scale: float32 [2], replicated
Outputs:
- output: bfloat16 [4096, 1536], P(('dp', 'ep')), parts along dimension 0
There are 2 independent parts. The reference program is written for one: setup_inputs(seed, part) draws one part's arguments, and reference() takes and returns one part's arrays. A program takes and returns all parts, laid end to end along the dimension named above; an argument that names none is the same for every part.
All inputs are finite; a program needn't handle non-finite values.
Results may differ from the reference program's by a relative error of at most 0.001.
Values are sent between devices in bfloat16 or wider.
A program may use at most 1 GiB of HBM per device.

```python
import jax
import jax.numpy as jnp
from jax import lax

GROUP_SIZE = 8
TOKENS_DEV = 256
EXPERTS = 32
HIDDEN = 1536
FFN_DIM = 2304
TOP_K = 2
BATCH_ROWS = GROUP_SIZE * TOKENS_DEV
HOT_COUNT = max(1, EXPERTS // 8)
CAPACITY = TOKENS_DEV // HOT_COUNT
MAX_ROWS = GROUP_SIZE * CAPACITY


def draw_routing(ids_key, part):
    order_key, shard_key = jax.random.split(ids_key)
    expert_order = jax.random.permutation(order_key, EXPERTS)
    hot_ids = expert_order[:HOT_COUNT]
    cold_ids = expert_order[HOT_COUNT:]
    shard_keys = jax.random.split(jax.random.fold_in(shard_key, part), GROUP_SIZE)

    def one_shard(one_key):
        tok_key, cold_key, swap_key = jax.random.split(one_key, 3)
        tok_rank = jax.random.permutation(tok_key, TOKENS_DEV)
        cold_mix = jax.random.permutation(cold_key, cold_ids)
        first_pick = hot_ids[tok_rank % HOT_COUNT]
        second_pick = cold_mix[tok_rank % (EXPERTS - HOT_COUNT)]
        swapped = jax.random.randint(swap_key, (TOKENS_DEV,), 0, 2) == 1
        return jnp.stack([jnp.where(swapped, second_pick, first_pick), jnp.where(swapped, first_pick, second_pick)], axis=1)

    return jax.vmap(one_shard)(shard_keys).reshape(BATCH_ROWS, TOP_K).astype(jnp.int32)


def draw_experts(weight_key, row_count, col_count):
    expert_keys = jax.random.split(weight_key, EXPERTS)
    return lax.map(lambda one_key: (jax.random.normal(one_key, (row_count, col_count), jnp.float32) * row_count ** -0.5).astype(jnp.bfloat16), expert_keys)


def setup_inputs(seed: int = 0, part: int = 0) -> dict:
    base_key = jax.random.key(seed)
    hid_key, route_key, gate_key, up_key, down_key, post_key, ids_key = jax.random.split(base_key, 7)
    hidden = jax.random.normal(jax.random.fold_in(hid_key, part), (BATCH_ROWS, HIDDEN), jnp.float32).astype(jnp.bfloat16)
    router_w = jax.random.normal(route_key, (HIDDEN, EXPERTS), jnp.float32) * (0.4 * HIDDEN ** -0.5)
    w_gate = draw_experts(gate_key, HIDDEN, FFN_DIM)
    w_up = draw_experts(up_key, HIDDEN, FFN_DIM)
    w_down = draw_experts(down_key, FFN_DIM, HIDDEN)
    post_scale = jax.random.uniform(post_key, (2,), jnp.float32, jnp.array([0.5, 1.0], jnp.float32), jnp.array([1.0, 2.0], jnp.float32))
    expert_ids = draw_routing(ids_key, part)
    return {'hidden': hidden, 'router_w': router_w, 'expert_ids': expert_ids, 'w_gate': w_gate, 'w_up': w_up, 'w_down': w_down, 'post_scale': post_scale}


def reference(hidden, router_w, expert_ids, w_gate, w_up, w_down, post_scale):
    hid_wide = hidden.astype(jnp.float32)
    logits = jnp.dot(hid_wide, router_w, preferred_element_type=jnp.float32)
    router_prob = jax.nn.softmax(logits, axis=-1)
    picked = jnp.take_along_axis(router_prob, expert_ids, axis=1)
    gates = picked / jnp.sum(picked, axis=1, keepdims=True)

    def add_expert(running_sum, expert):
        hit_mask = expert_ids == expert
        tok_gate = jnp.sum(jnp.where(hit_mask, gates, 0.0), axis=1)
        chosen = jnp.any(hit_mask, axis=1)
        row_index = jnp.nonzero(chosen, size=MAX_ROWS, fill_value=0)[0]
        in_range = jnp.arange(MAX_ROWS) < jnp.sum(chosen)
        tok_rows = hidden[row_index]
        gate_in = jnp.dot(tok_rows, w_gate[expert], preferred_element_type=jnp.float32)
        up_in = jnp.dot(tok_rows, w_up[expert], preferred_element_type=jnp.float32)
        middle = (jax.nn.silu(gate_in) * up_in).astype(jnp.bfloat16)
        expert_out = jnp.dot(middle, w_down[expert], preferred_element_type=jnp.float32).astype(jnp.bfloat16)
        row_weight = jnp.where(in_range, tok_gate[row_index], 0.0)
        running_sum = running_sum.at[row_index].add(row_weight[:, None] * expert_out.astype(jnp.float32))
        return running_sum, None

    mixed, _ = lax.scan(add_expert, jnp.zeros((BATCH_ROWS, HIDDEN), jnp.float32), jnp.arange(EXPERTS))
    return (post_scale[0] * hid_wide + post_scale[1] * mixed).astype(jnp.bfloat16)
```

```python
import functools

import jax
import jax.numpy as jnp
from jax import lax
from jax.experimental import pallas as pl
from jax.experimental.pallas import tpu as pltpu
from jax.sharding import PartitionSpec as P

MESH = pl.DeviceIdType.MESH
BF16, F32, I32 = jnp.bfloat16, jnp.float32, jnp.int32
GROUP = 8
WORLD = 16
LOCAL = 4
EXPERTS = GROUP * LOCAL
TOK = 256
SLOTS = 64
WIDTH = 1536
FFN = 2304
CHUNKS = 4
BUCKETS = (96, 112, 128, 160, 208, 256)
FCH = 768
NCH = FFN // FCH
RING = 4
ROWS_MAX = GROUP * SLOTS
XROWS = ROWS_MAX + SLOTS


def dot(a, b):
    return jnp.dot(a, b, preferred_element_type=F32)


def dot_t(a, b):
    return lax.dot_general(a, b, (((1,), (1,)), ((), ())), preferred_element_type=F32)


def gather_kernel(ids_ref, h_ref, wr_ref, hall, rk_ref, cnt_ref, tab_ref, top_ref,
                  idbuf, id_send, id_recv, x_send, y_send, p_send, x_recv, y_recv, d_recv, p_recv, own_sem):
    dp, me = lax.axis_index("dp"), lax.axis_index("ep")
    core, xc, yc = lax.rem(me, 2), lax.rem(me // 2, 2), me // 4
    xn, yn, pc = me + 2 - 4 * xc, me + 4 - 8 * yc, me + 1 - 2 * core
    dg = xn + 4 - 8 * yc
    my = dp * GROUP + me
    rows = TOK // CHUNKS

    barrier = pltpu.get_barrier_semaphore()
    for k in range(1, WORLD):
        g = lax.rem(my + k, WORLD)
        pl.semaphore_signal(barrier, inc=1, device_id={"dp": g // GROUP, "ep": lax.rem(g, GROUP)}, device_id_type=MESH)
    pl.semaphore_wait(barrier, WORLD - 1)

    def piece(block, q):
        return hall.at[block, pl.ds(q * rows, rows), :]

    def mine(q):
        return h_ref.at[pl.ds(q * rows, rows), :]

    def remote(src, dst, send, recv, dev):
        return pltpu.make_async_remote_copy(src_ref=src, dst_ref=dst, send_sem=send, recv_sem=recv,
                                            device_id={"ep": dev}, device_id_type=MESH)

    id_copies = []
    for k in range(1, WORLD):
        g = lax.rem(my + k, WORLD)
        copy = pltpu.make_async_remote_copy(src_ref=ids_ref, dst_ref=idbuf.at[my], send_sem=id_send.at[k], recv_sem=id_recv.at[k],
                                            device_id={"dp": g // GROUP, "ep": lax.rem(g, GROUP)}, device_id_type=MESH)
        copy.start()
        id_copies.append(copy)
    half = CHUNKS // 2
    sends = []

    def start(copy):
        copy.start()
        sends.append(copy)

    for i in range(CHUNKS):
        qx, qy = i, (i + half) % CHUNKS
        start(remote(mine(qx), piece(me, qx), x_send.at[qx], x_recv.at[qx], xn))
        start(remote(mine(qy), piece(me, qy), y_send.at[qy], y_recv.at[qy], yn))
    start(remote(h_ref, hall.at[me], p_send.at[3 * CHUNKS], p_recv.at[3 * CHUNKS], pc))
    own = pltpu.make_async_copy(h_ref, hall.at[me], own_sem.at[0])
    own.start()
    own_ids = pltpu.make_async_copy(ids_ref, idbuf.at[my], own_sem.at[1])
    own_ids.start()

    def arrived(block, q, sem):
        remote(piece(block, q), piece(block, q), x_send.at[0], sem, xn).wait_recv()

    for i in range(half):
        a, b = i, i + half
        arrived(xn, a, x_recv.at[a])
        start(remote(piece(xn, a), piece(xn, a), y_send.at[CHUNKS + i], d_recv.at[a], yn))
        start(remote(piece(xn, a), piece(xn, a), p_send.at[a], p_recv.at[a], pc))
        arrived(yn, b, y_recv.at[b])
        start(remote(piece(yn, b), piece(yn, b), x_send.at[CHUNKS + i], d_recv.at[b], xn))
        start(remote(piece(yn, b), piece(yn, b), p_send.at[CHUNKS + b], p_recv.at[CHUNKS + b], pc))

    own_ids.wait()
    for copy in id_copies:
        copy.wait()
    upper = (lax.broadcasted_iota(I32, (TOK, TOK), 0) < lax.broadcasted_iota(I32, (TOK, TOK), 1)).astype(BF16)
    hb = h_ref[...]
    wr = wr_ref[...]
    w_hi = wr.astype(BF16)
    rest = wr - w_hi.astype(F32)
    w_mid = rest.astype(BF16)
    w_lo = (rest - w_mid.astype(F32)).astype(BF16)
    logits = dot_t(w_hi, hb) + (dot_t(w_mid, hb) + dot_t(w_lo, hb))
    prob = jnp.exp(logits - jnp.max(logits, axis=0, keepdims=True))
    prob = prob / jnp.sum(prob, axis=0, keepdims=True)
    e_iota = lax.broadcasted_iota(I32, (EXPERTS, TOK), 0)
    id0, id1 = ids_ref[0:1, :], ids_ref[1:2, :]
    hit0, hit1 = e_iota == id0, e_iota == id1
    pick0 = jnp.sum(jnp.where(hit0, prob, 0.0), axis=0, keepdims=True)
    pick1 = jnp.sum(jnp.where(hit1, prob, 0.0), axis=0, keepdims=True)
    both = pick0 + pick1
    hits = jnp.where(hit0 | hit1, 1.0, 0.0)
    rank = dot(hits.astype(BF16), upper)
    er, ec = lax.broadcasted_iota(I32, (EXPERTS, EXPERTS), 0), lax.broadcasted_iota(I32, (EXPERTS, EXPERTS), 1)
    before = ((er // LOCAL == ec // LOCAL) & (ec < er)).astype(BF16)
    base = jnp.sum(dot(before, hits.astype(BF16)), axis=1, keepdims=True)
    place = rank + base
    pos0 = jnp.sum(jnp.where(hit0, place, 0.0), axis=0, keepdims=True)
    pos1 = jnp.sum(jnp.where(hit1, place, 0.0), axis=0, keepdims=True)
    own0, own1 = (id0 // LOCAL).astype(F32), (id1 // LOCAL).astype(F32)
    fields = jnp.concatenate([own0, pos0, pick0 / both, own1, pos1, pick1 / both, jnp.zeros((122, TOK), F32)], axis=0)
    tab_ref[...] = fields.T

    j_iota = lax.broadcasted_iota(I32, (8, TOK), 0)
    local_id = jnp.where(j_iota < LOCAL, me * LOCAL + j_iota, -1)
    hit_list = []
    for s in range(GROUP):
        pair = idbuf[dp * GROUP + s]
        hit_list.append((local_id == pair[0:1, :]) | (local_id == pair[1:2, :]))
    hit_f = jnp.where(jnp.concatenate(hit_list, axis=0), 1.0, 0.0)
    hit_b = hit_f.astype(BF16)
    rk_ref[...] = jnp.where(hit_f > 0.5, dot(hit_b, upper), -1.0).astype(I32)
    cnt_ref[...] = dot_t(jnp.ones((8, TOK), BF16), hit_b).astype(I32)

    d_iota = lax.broadcasted_iota(I32, (GROUP, TOK), 0)
    top = jnp.zeros((GROUP, 1), F32)
    for g in range(WORLD):
        owners = idbuf[g] // LOCAL
        n = (d_iota == owners[0:1, :]).astype(F32) + (d_iota == owners[1:2, :]).astype(F32)
        top = jnp.maximum(top, jnp.sum(n, axis=1, keepdims=True))
    top_ref[...] = jnp.broadcast_to(jnp.max(top, axis=0, keepdims=True), (8, 128)).astype(I32)

    for i in range(half):
        a, b = i + half, i
        arrived(xn, a, x_recv.at[a])
        start(remote(piece(xn, a), piece(xn, a), p_send.at[a], p_recv.at[a], pc))
        arrived(yn, b, y_recv.at[b])
        start(remote(piece(yn, b), piece(yn, b), p_send.at[CHUNKS + b], p_recv.at[CHUNKS + b], pc))
    for i in range(half):
        for q in (i, i + half):
            arrived(dg, q, d_recv.at[q])
            start(remote(piece(dg, q), piece(dg, q), p_send.at[2 * CHUNKS + q], p_recv.at[2 * CHUNKS + q], pc))
    for q in range(CHUNKS):
        arrived(xn + 1 - 2 * core, q, p_recv.at[q])
        arrived(yn + 1 - 2 * core, q, p_recv.at[CHUNKS + q])
        arrived(dg + 1 - 2 * core, q, p_recv.at[2 * CHUNKS + q])
    remote(hall.at[pc], hall.at[pc], x_send.at[0], p_recv.at[3 * CHUNKS], pc).wait_recv()
    for copy in sends:
        copy.wait_send()
    own.wait()


def gather(ids_t, hidden, wr_t):
    vmem = pl.BlockSpec(memory_space=pltpu.VMEM)
    dma = pltpu.SemaphoreType.DMA
    return pl.pallas_call(
        gather_kernel,
        name="gather_rows",
        out_shape=[
            jax.ShapeDtypeStruct((GROUP, TOK, WIDTH), BF16),
            jax.ShapeDtypeStruct((GROUP * 8, TOK), I32),
            jax.ShapeDtypeStruct((8, GROUP * 8), I32),
            jax.ShapeDtypeStruct((TOK, 128), F32),
            jax.ShapeDtypeStruct((8, 128), I32),
        ],
        in_specs=[vmem] * 3,
        out_specs=[pl.BlockSpec(memory_space=pl.ANY)] + [vmem] * 4,
        scratch_shapes=[
            pltpu.VMEM((WORLD, 2, TOK), I32),
            dma((WORLD,)), dma((WORLD,)),
            dma((2 * CHUNKS,)), dma((2 * CHUNKS,)), dma((3 * CHUNKS + 1,)),
            dma((CHUNKS,)), dma((CHUNKS,)), dma((CHUNKS,)), dma((3 * CHUNKS + 1,)),
            dma((2,)),
        ],
        compiler_params=pltpu.CompilerParams(collective_id=1, has_side_effects=True, vmem_limit_bytes=12 * 2**20),
    )(ids_t, hidden, wr_t)


def expert_kernel(cnt, rk_ref, hall, w1, w3, w2, ypack, hbuf, xbuf, acc, mid, b1, b3, b2, offs, h_sem, w_sem, y_sem):
    def weights(g, slot):
        j, f = g // NCH, lax.rem(g, NCH)
        cols = pl.ds(pl.multiple_of(f * FCH, FCH), FCH)
        return (
            pltpu.make_async_copy(w1.at[j, :, cols], b1.at[slot], w_sem.at[0, slot]),
            pltpu.make_async_copy(w3.at[j, :, cols], b3.at[slot], w_sem.at[1, slot]),
            pltpu.make_async_copy(w2.at[j, cols, :], b2.at[slot], w_sem.at[2, slot]),
        )

    def h_copy(s):
        return pltpu.make_async_copy(hall.at[s], hbuf.at[s], h_sem.at[s])

    for s in range(GROUP):
        h_copy(s).start()
    for g in range(RING):
        for copy in weights(g, g):
            copy.start()

    xbuf[...] = jnp.zeros_like(xbuf)
    totals = []
    for j in range(LOCAL):
        at = jnp.int32(0)
        for s in range(GROUP):
            offs[s, j] = at
            at = at + (cnt[0, s * 8 + j] + 15) // 16 * 16
        totals.append(at)

    r_iota = lax.broadcasted_iota(I32, (SLOTS, TOK), 0)
    for s in range(GROUP):
        h_copy(s).wait()
        table = jnp.concatenate([(r_iota == rk_ref[s * 8 + j:s * 8 + j + 1, :]).astype(F32) for j in range(LOCAL)], axis=0).astype(BF16)
        picked = dot(table, hbuf[s]).astype(BF16)
        for j in range(LOCAL):
            xbuf[j, pl.ds(pl.multiple_of(offs[s, j], 16), SLOTS), :] = picked[j * SLOTS:(j + 1) * SLOTS]

    def step(g, carry):
        slot = lax.rem(g, RING)
        j, f = g // NCH, lax.rem(g, NCH)
        for copy in weights(g, slot):
            copy.wait()
        total = jnp.where(j == 0, totals[0], jnp.where(j == 1, totals[1], jnp.where(j == 2, totals[2], totals[3])))
        blocks = (total + 127) // 128
        for nb in range(1, 5):
            @pl.when(blocks == nb)
            def _():
                n = nb * 128
                x = xbuf[j, :n, :]
                for c in range(FCH // 256):
                    cols = pl.ds(c * 256, 256)
                    up = dot(x, b1[slot, :, cols])
                    lin = dot(x, b3[slot, :, cols])
                    mid[:n, cols] = (jax.nn.silu(up) * lin).astype(BF16)
                m = mid[:n, :]
                for c in range(WIDTH // 512):
                    cols = pl.ds(c * 512, 512)
                    part = dot(m, b2[slot, :, cols])

                    @pl.when(f == 0)
                    def _():
                        acc[:n, cols] = part

                    @pl.when((f > 0) & (f < NCH - 1))
                    def _():
                        acc[:n, cols] += part

                    @pl.when(f == NCH - 1)
                    def _():
                        xbuf[j, :n, cols] = (acc[:n, cols] + part).astype(BF16)

        @pl.when(g + RING < LOCAL * NCH)
        def _():
            for copy in weights(g + RING, slot):
                copy.start()

        return carry

    lax.fori_loop(0, LOCAL * NCH, step, 0)

    lane = lax.broadcasted_iota(I32, (1, LOCAL * SLOTS), 1)
    p_iota = lax.broadcasted_iota(I32, (LOCAL * SLOTS, LOCAL * SLOTS), 0)
    r_lane = lax.rem(lane, SLOTS)
    for s in range(GROUP):
        target = jnp.full((1, LOCAL * SLOTS), -1, I32)
        at = jnp.int32(0)
        for j in range(LOCAL):
            n = cnt[0, s * 8 + j]
            target = jnp.where((lane // SLOTS == j) & (r_lane < n), at + r_lane, target)
            at = at + n
        table = (p_iota == target).astype(F32).astype(BF16)
        rows = jnp.concatenate([xbuf[j, pl.ds(pl.multiple_of(offs[s, j], 16), SLOTS), :] for j in range(LOCAL)], axis=0)
        hbuf[s] = dot(table, rows).astype(BF16)
        pltpu.make_async_copy(hbuf.at[s], ypack.at[s], y_sem.at[s]).start()
    for s in range(GROUP):
        pltpu.make_async_copy(hbuf.at[s], ypack.at[s], y_sem.at[s]).wait()


def experts(cnt, rk, hall, w1, w3, w2):
    hbm = pl.BlockSpec(memory_space=pl.ANY)
    dma = pltpu.SemaphoreType.DMA
    return pl.pallas_call(
        expert_kernel,
        name="experts",
        out_shape=jax.ShapeDtypeStruct((GROUP, TOK, WIDTH), BF16),
        in_specs=[pl.BlockSpec(memory_space=pltpu.SMEM), pl.BlockSpec(memory_space=pltpu.VMEM)] + [hbm] * 4,
        out_specs=hbm,
        scratch_shapes=[
            pltpu.VMEM((GROUP, TOK, WIDTH), BF16),
            pltpu.VMEM((LOCAL, XROWS, WIDTH), BF16),
            pltpu.VMEM((ROWS_MAX, WIDTH), F32),
            pltpu.VMEM((ROWS_MAX, FCH), BF16),
            pltpu.VMEM((RING, WIDTH, FCH), BF16),
            pltpu.VMEM((RING, WIDTH, FCH), BF16),
            pltpu.VMEM((RING, FCH, WIDTH), BF16),
            pltpu.SMEM((GROUP, LOCAL), I32),
            dma((GROUP,)), dma((3, RING)), dma((GROUP,)),
        ],
        compiler_params=pltpu.CompilerParams(vmem_limit_bytes=60 * 2**20),
        cost_estimate=pl.CostEstimate(flops=20 * 10**9, bytes_accessed=98 * 10**6, transcendentals=0),
    )(cnt, rk, hall, w1, w3, w2)


def combine_kernel(cap, scale, tab_ref, h_ref, ypack, out_ref, land, mix0, mix1, send, recv, own_sem):
    me = lax.axis_index("ep")
    barrier = pltpu.get_barrier_semaphore()
    for k in range(1, GROUP):
        pl.semaphore_signal(barrier, inc=1, device_id={"ep": lax.rem(me + k, GROUP)}, device_id_type=MESH)
    pl.semaphore_wait(barrier, GROUP - 1)
    copies = []
    for k in range(1, GROUP):
        to = lax.rem(me + k, GROUP)
        copy = pltpu.make_async_remote_copy(src_ref=ypack.at[to, pl.ds(0, cap), :], dst_ref=land.at[me], send_sem=send.at[k], recv_sem=recv.at[k],
                                            device_id={"ep": to}, device_id_type=MESH)
        copy.start()
        copies.append(copy)
    own = pltpu.make_async_copy(ypack.at[me, pl.ds(0, cap), :], land.at[me], own_sem.at[0])
    own.start()

    lane = lax.broadcasted_iota(I32, (TOK, cap), 1)
    own0, pos0 = tab_ref[:, 0:1].astype(I32), tab_ref[:, 1:2].astype(I32)
    own1, pos1 = tab_ref[:, 3:4].astype(I32), tab_ref[:, 4:5].astype(I32)
    for k in range(GROUP):
        frm = lax.rem(me + GROUP - k, GROUP)
        if k == 0:
            own.wait()
        else:
            copies[k - 1].wait_recv()
        rows = land[frm]
        t0 = ((own0 == frm) & (pos0 == lane)).astype(F32).astype(BF16)
        t1 = ((own1 == frm) & (pos1 == lane)).astype(F32).astype(BF16)
        if k == 0:
            mix0[...] = dot(t0, rows)
            mix1[...] = dot(t1, rows)
        else:
            mix0[...] += dot(t0, rows)
            mix1[...] += dot(t1, rows)
    mixed = tab_ref[:, 2:3] * mix0[...] + tab_ref[:, 5:6] * mix1[...]
    out_ref[...] = (scale[0] * h_ref[...].astype(F32) + scale[1] * mixed).astype(BF16)
    for copy in copies:
        copy.wait_send()


def combine(index, cap, scale, tab, hidden, ypack):
    vmem = pl.BlockSpec(memory_space=pltpu.VMEM)
    dma = pltpu.SemaphoreType.DMA
    return pl.pallas_call(
        functools.partial(combine_kernel, cap),
        name=f"combine_{cap}",
        out_shape=jax.ShapeDtypeStruct((TOK, WIDTH), BF16),
        in_specs=[pl.BlockSpec(memory_space=pltpu.SMEM), vmem, vmem, pl.BlockSpec(memory_space=pl.ANY)],
        out_specs=vmem,
        scratch_shapes=[
            pltpu.VMEM((GROUP, cap, WIDTH), BF16),
            pltpu.VMEM((TOK, WIDTH), F32),
            pltpu.VMEM((TOK, WIDTH), F32),
            dma((GROUP,)), dma((GROUP,)), dma((1,)),
        ],
        compiler_params=pltpu.CompilerParams(collective_id=2 + index, has_side_effects=True, vmem_limit_bytes=30 * 2**20),
    )(scale, tab, hidden, ypack)


def solution(mesh):
    def local_step(hidden, router_w, expert_ids, w_gate, w_up, w_down, post_scale):
        hall, rk, cnt, tab, top = gather(expert_ids.T, hidden, router_w.T)
        ypack = experts(cnt, rk, hall, w_gate, w_up, w_down)
        need = top[0, 0]
        which = sum((need > cap).astype(I32) for cap in BUCKETS[:-1])
        branches = [functools.partial(combine, i, cap) for i, cap in enumerate(BUCKETS)]
        return lax.switch(which, branches, post_scale, tab, hidden, ypack)

    tok_spec = P(("dp", "ep"))
    return jax.shard_map(local_step, mesh=mesh, in_specs=(tok_spec, P(), tok_spec, P("ep"), P("ep"), P("ep"), P()), out_specs=tok_spec, check_vma=False)
```

```python
import functools

import jax
import jax.numpy as jnp
from jax import lax
from jax.experimental import pallas as pl
from jax.experimental.pallas import tpu as pltpu
from jax.sharding import PartitionSpec as P

MESH = pl.DeviceIdType.MESH
BF16, F32, I32 = jnp.bfloat16, jnp.float32, jnp.int32
GROUP = 8
WORLD = 16
LOCAL = 4
EXPERTS = GROUP * LOCAL
TOK = 256
SLOTS = 64
WIDTH = 1536
FFN = 2304
CHUNKS = 4
BUCKETS = (96, 128, 160, 208, 256)
FCH = 768
NCH = FFN // FCH
DCH = 512
RING = 3
ROWS_MAX = GROUP * SLOTS
XROWS = ROWS_MAX + 128
GATHER_VMEM = 15
EXPERT_VMEM = 25


def dot(a, b):
    return jnp.dot(a, b, preferred_element_type=F32)


def dot_t(a, b):
    return lax.dot_general(a, b, (((1,), (1,)), ((), ())), preferred_element_type=F32)


def gather_kernel(ids_ref, h_ref, wr_ref, xs_ref, cnt_ref, tab_ref, top_ref,
                  hall, rk, idbuf, id_send, id_recv, x_send, y_send, p_send, x_recv, y_recv, d_recv, p_recv, own_sem):
    dp, me = lax.axis_index("dp"), lax.axis_index("ep")
    core, xc, yc = lax.rem(me, 2), lax.rem(me // 2, 2), me // 4
    xn, yn, pc = me + 2 - 4 * xc, me + 4 - 8 * yc, me + 1 - 2 * core
    dg = xn + 4 - 8 * yc
    my = dp * GROUP + me
    rows = TOK // CHUNKS

    barrier = pltpu.get_barrier_semaphore()
    for k in range(1, WORLD):
        g = lax.rem(my + k, WORLD)
        pl.semaphore_signal(barrier, inc=1, device_id={"dp": g // GROUP, "ep": lax.rem(g, GROUP)}, device_id_type=MESH)
    pl.semaphore_wait(barrier, WORLD - 1)

    def piece(block, q):
        return hall.at[block, pl.ds(q * rows, rows), :]

    def mine(q):
        return h_ref.at[pl.ds(q * rows, rows), :]

    def remote(src, dst, send, recv, dev):
        return pltpu.make_async_remote_copy(src_ref=src, dst_ref=dst, send_sem=send, recv_sem=recv,
                                            device_id={"ep": dev}, device_id_type=MESH)

    half = CHUNKS // 2
    sends = []

    def start(copy):
        copy.start()
        sends.append(copy)

    def send_x(q):
        start(remote(mine(q), piece(me, q), x_send.at[q], x_recv.at[q], xn))

    def send_y(q):
        start(remote(mine(q), piece(me, q), y_send.at[q], y_recv.at[q], yn))

    for i in range(half):
        send_x(i)
        send_y(i + half)
    id_copies = []
    for k in range(1, WORLD):
        g = lax.rem(my + k, WORLD)
        copy = pltpu.make_async_remote_copy(src_ref=ids_ref, dst_ref=idbuf.at[my], send_sem=id_send.at[k], recv_sem=id_recv.at[k],
                                            device_id={"dp": g // GROUP, "ep": lax.rem(g, GROUP)}, device_id_type=MESH)
        copy.start()
        id_copies.append(copy)
    start(remote(h_ref, hall.at[me], p_send.at[3 * CHUNKS], p_recv.at[3 * CHUNKS], pc))
    own_ids = pltpu.make_async_copy(ids_ref, idbuf.at[my], own_sem.at[0])
    own_ids.start()

    upper = (lax.broadcasted_iota(I32, (TOK, TOK), 0) < lax.broadcasted_iota(I32, (TOK, TOK), 1)).astype(BF16)
    hb = h_ref[...]
    wr = wr_ref[...]
    w_hi = wr.astype(BF16)
    rest = wr - w_hi.astype(F32)
    w_mid = rest.astype(BF16)
    w_lo = (rest - w_mid.astype(F32)).astype(BF16)
    logits = dot_t(w_hi, hb) + (dot_t(w_mid, hb) + dot_t(w_lo, hb))
    prob = jnp.exp(logits - jnp.max(logits, axis=0, keepdims=True))
    prob = prob / jnp.sum(prob, axis=0, keepdims=True)
    e_iota = lax.broadcasted_iota(I32, (EXPERTS, TOK), 0)
    id0, id1 = ids_ref[0:1, :], ids_ref[1:2, :]
    hit0, hit1 = e_iota == id0, e_iota == id1
    pick0 = jnp.sum(jnp.where(hit0, prob, 0.0), axis=0, keepdims=True)
    pick1 = jnp.sum(jnp.where(hit1, prob, 0.0), axis=0, keepdims=True)
    both = pick0 + pick1
    hits = jnp.where(hit0 | hit1, 1.0, 0.0)
    rank = dot(hits.astype(BF16), upper)
    er, ec = lax.broadcasted_iota(I32, (EXPERTS, EXPERTS), 0), lax.broadcasted_iota(I32, (EXPERTS, EXPERTS), 1)
    before = ((er // LOCAL == ec // LOCAL) & (ec < er)).astype(BF16)
    base = jnp.sum(dot(before, hits.astype(BF16)), axis=1, keepdims=True)
    place = rank + base
    pos0 = jnp.sum(jnp.where(hit0, place, 0.0), axis=0, keepdims=True)
    pos1 = jnp.sum(jnp.where(hit1, place, 0.0), axis=0, keepdims=True)
    own0, own1 = (id0 // LOCAL).astype(F32), (id1 // LOCAL).astype(F32)
    fields = jnp.concatenate([own0, pos0, pick0 / both, own1, pos1, pick1 / both, jnp.zeros((122, TOK), F32)], axis=0)
    tab_ref[...] = fields.T

    def arrived(block, q, sem):
        remote(piece(block, q), piece(block, q), x_send.at[0], sem, xn).wait_recv()

    for i in range(half):
        a, b = i, i + half
        arrived(xn, a, x_recv.at[a])
        start(remote(piece(xn, a), piece(xn, a), y_send.at[CHUNKS + i], d_recv.at[a], yn))
        send_y(a)
        start(remote(piece(xn, a), piece(xn, a), p_send.at[a], p_recv.at[a], pc))
        arrived(yn, b, y_recv.at[b])
        start(remote(piece(yn, b), piece(yn, b), x_send.at[CHUNKS + i], d_recv.at[b], xn))
        send_x(b)
        start(remote(piece(yn, b), piece(yn, b), p_send.at[CHUNKS + b], p_recv.at[CHUNKS + b], pc))
        if i == 0:
            own_ids.wait()
            for copy in id_copies:
                copy.wait()
            j_iota = lax.broadcasted_iota(I32, (8, TOK), 0)
            local_id = jnp.where(j_iota < LOCAL, me * LOCAL + j_iota, -1)
            hit_list = []
            for s in range(GROUP):
                pair = idbuf[dp * GROUP + s]
                hit_list.append((local_id == pair[0:1, :]) | (local_id == pair[1:2, :]))
            hit_f = jnp.where(jnp.concatenate(hit_list, axis=0), 1.0, 0.0)
            hit_b = hit_f.astype(BF16)
            rk[...] = jnp.where(hit_f > 0.5, dot(hit_b, upper), -1.0).astype(I32).reshape(GROUP, 8, TOK)
            cnt_ref[...] = dot_t(jnp.ones((8, TOK), BF16), hit_b).astype(I32)
            d_iota = lax.broadcasted_iota(I32, (GROUP, TOK), 0)
            top = jnp.zeros((GROUP, 1), F32)
            for g in range(WORLD):
                owners = idbuf[g] // LOCAL
                n = (d_iota == owners[0:1, :]).astype(F32) + (d_iota == owners[1:2, :]).astype(F32)
                top = jnp.maximum(top, jnp.sum(n, axis=1, keepdims=True))
            top_ref[...] = jnp.broadcast_to(jnp.max(top, axis=0, keepdims=True), (8, 128)).astype(I32)

    r_iota = lax.broadcasted_iota(I32, (SLOTS, TOK), 0)

    def pick(s, block):
        ranks = rk[s]
        table = jnp.concatenate([(r_iota == ranks[j:j + 1, :]).astype(F32) for j in range(LOCAL)], axis=0).astype(BF16)
        xs_ref[s] = dot(table, block).astype(BF16)

    pick(me, hb)
    remote(hall.at[pc], hall.at[pc], x_send.at[0], p_recv.at[3 * CHUNKS], pc).wait_recv()
    pick(pc, hall[pc])
    for i in range(half):
        a, b = i + half, i
        arrived(xn, a, x_recv.at[a])
        start(remote(piece(xn, a), piece(xn, a), p_send.at[a], p_recv.at[a], pc))
        arrived(yn, b, y_recv.at[b])
        start(remote(piece(yn, b), piece(yn, b), p_send.at[CHUNKS + b], p_recv.at[CHUNKS + b], pc))
    for i in range(half):
        for q in (i, i + half):
            arrived(dg, q, d_recv.at[q])
            start(remote(piece(dg, q), piece(dg, q), p_send.at[2 * CHUNKS + q], p_recv.at[2 * CHUNKS + q], pc))
        if i == 0:
            pick(xn, hall[xn])
            pick(yn, hall[yn])
    turn = 1 - 2 * core
    for q in range(CHUNKS):
        arrived(xn + turn, q, p_recv.at[q])
        arrived(yn + turn, q, p_recv.at[CHUNKS + q])
    pick(xn + turn, hall[xn + turn])
    pick(yn + turn, hall[yn + turn])
    pick(dg, hall[dg])
    for q in range(CHUNKS):
        arrived(dg + turn, q, p_recv.at[2 * CHUNKS + q])
    pick(dg + turn, hall[dg + turn])
    for copy in sends:
        copy.wait_send()


def gather(ids_t, hidden, wr_t):
    vmem = pl.BlockSpec(memory_space=pltpu.VMEM)
    dma = pltpu.SemaphoreType.DMA
    return pl.pallas_call(
        gather_kernel,
        name="gather_rows",
        out_shape=[
            jax.ShapeDtypeStruct((GROUP, TOK, WIDTH), BF16),
            jax.ShapeDtypeStruct((8, GROUP * 8), I32),
            jax.ShapeDtypeStruct((TOK, 128), F32),
            jax.ShapeDtypeStruct((8, 128), I32),
        ],
        in_specs=[vmem] * 3,
        out_specs=[vmem] * 4,
        scratch_shapes=[
            pltpu.VMEM((GROUP, TOK, WIDTH), BF16),
            pltpu.VMEM((GROUP, 8, TOK), I32),
            pltpu.VMEM((WORLD, 2, TOK), I32),
            dma((WORLD,)), dma((WORLD,)),
            dma((2 * CHUNKS,)), dma((2 * CHUNKS,)), dma((3 * CHUNKS + 1,)),
            dma((CHUNKS,)), dma((CHUNKS,)), dma((CHUNKS,)), dma((3 * CHUNKS + 1,)),
            dma((1,)),
        ],
        compiler_params=pltpu.CompilerParams(collective_id=1, has_side_effects=True, vmem_limit_bytes=GATHER_VMEM * 2**20),
        cost_estimate=pl.CostEstimate(flops=20 * 10**9, bytes_accessed=20 * 10**6, transcendentals=0),
    )(ids_t, hidden, wr_t)


def expert_kernel(cnt, xs_ref, w1, w3, w2, ypack, xbuf, mid, b3, b2, offs, w3_sem, w2_sem):
    def up_copy(g):
        slot = lax.rem(g, RING)
        cols = pl.ds(pl.multiple_of(lax.rem(g, NCH) * FCH, FCH), FCH)
        return pltpu.make_async_copy(w3.at[g // NCH, :, cols], b3.at[slot], w3_sem.at[slot])

    def down_copy(g):
        slot = lax.rem(g, RING)
        cols = pl.ds(pl.multiple_of(lax.rem(g, NCH) * DCH, DCH), DCH)
        return pltpu.make_async_copy(w2.at[g // NCH, :, cols], b2.at[slot], w2_sem.at[slot])

    for g in range(RING):
        up_copy(g).start()
    for g in range(RING):
        down_copy(g).start()

    totals = []
    for j in range(LOCAL):
        at = jnp.int32(0)
        for s in range(GROUP):
            offs[s, j] = at
            at = at + (cnt[0, s * 8 + j] + 15) // 16 * 16
        totals.append(at)

    def compact(s, carry):
        for j in range(LOCAL):
            xbuf[j, pl.ds(pl.multiple_of(offs[s, j], 16), SLOTS), :] = xs_ref[s, j * SLOTS:(j + 1) * SLOTS, :]
        return carry

    lax.fori_loop(0, GROUP, compact, 0)
    for j in range(LOCAL):
        xbuf[j, pl.ds(pl.multiple_of(totals[j], 16), 128), :] = jnp.zeros((128, WIDTH), BF16)

    def expert(j, carry):
        total = jnp.where(j == 0, totals[0], jnp.where(j == 1, totals[1], jnp.where(j == 2, totals[2], totals[3])))
        blocks = (total + 127) // 128

        def over_rows(body):
            def wide(i, c):
                body(pl.multiple_of(i * 256, 256), 256)
                return c

            lax.fori_loop(0, blocks // 2, wide, 0)

            @pl.when(lax.rem(blocks, 2) == 1)
            def _():
                body(pl.multiple_of((blocks // 2) * 256, 128), 128)

        def up_step(f, c):
            g = j * NCH + f
            slot = lax.rem(g, RING)
            up_copy(g).wait()

            def body(row, n):
                x = xbuf[j, pl.ds(row, n), :]
                for p in range(FCH // 256):
                    cols = pl.ds(pl.multiple_of(f * FCH + p * 256, 256), 256)
                    up = dot(x, w1[j, :, cols])
                    lin = dot(x, b3[slot, :, p * 256:(p + 1) * 256])
                    mid[pl.ds(row, n), cols] = (jax.nn.silu(up) * lin).astype(BF16)

            over_rows(body)

            @pl.when(g + RING < LOCAL * NCH)
            def _():
                up_copy(g + RING).start()

            return c

        def down_step(f, c):
            g = j * NCH + f
            slot = lax.rem(g, RING)
            down_copy(g).wait()

            def body(row, n):
                cols = pl.ds(pl.multiple_of(f * DCH, DCH), DCH)
                xbuf[j, pl.ds(row, n), cols] = dot(mid[pl.ds(row, n), :], b2[slot]).astype(BF16)

            over_rows(body)

            @pl.when(g + RING < LOCAL * NCH)
            def _():
                down_copy(g + RING).start()

            return c

        lax.fori_loop(0, NCH, up_step, 0)
        lax.fori_loop(0, NCH, down_step, 0)
        return carry

    lax.fori_loop(0, LOCAL, expert, 0)

    lane = lax.broadcasted_iota(I32, (1, LOCAL * SLOTS), 1)
    p_iota = lax.broadcasted_iota(I32, (128, LOCAL * SLOTS), 0)
    r_lane = lax.rem(lane, SLOTS)

    def pack(s, carry):
        target = jnp.full((1, LOCAL * SLOTS), -1, I32)
        at = jnp.int32(0)
        for j in range(LOCAL):
            n = cnt[0, s * 8 + j]
            target = jnp.where((lane // SLOTS == j) & (r_lane < n), at + r_lane, target)
            at = at + n
        rows = jnp.concatenate([xbuf[j, pl.ds(pl.multiple_of(offs[s, j], 16), SLOTS), :] for j in range(LOCAL)], axis=0)
        ypack[s, 0:128, :] = dot((p_iota == target).astype(F32).astype(BF16), rows).astype(BF16)

        @pl.when(at > 128)
        def _():
            ypack[s, 128:256, :] = dot((p_iota + 128 == target).astype(F32).astype(BF16), rows).astype(BF16)

        @pl.when(at <= 128)
        def _():
            ypack[s, 128:256, :] = jnp.zeros((128, WIDTH), BF16)

        return carry

    lax.fori_loop(0, GROUP, pack, 0)


def experts(cnt, xs, w1, w3, w2):
    hbm = pl.BlockSpec(memory_space=pl.ANY)
    vmem = pl.BlockSpec(memory_space=pltpu.VMEM)
    dma = pltpu.SemaphoreType.DMA
    return pl.pallas_call(
        expert_kernel,
        name="experts",
        out_shape=jax.ShapeDtypeStruct((GROUP, TOK, WIDTH), BF16),
        in_specs=[pl.BlockSpec(memory_space=pltpu.SMEM), vmem, vmem, hbm, hbm],
        out_specs=vmem,
        input_output_aliases={1: 0},
        scratch_shapes=[
            pltpu.VMEM((LOCAL, XROWS, WIDTH), BF16),
            pltpu.VMEM((ROWS_MAX, FFN), BF16),
            pltpu.VMEM((RING, WIDTH, FCH), BF16),
            pltpu.VMEM((RING, FFN, DCH), BF16),
            pltpu.SMEM((GROUP, LOCAL), I32),
            dma((RING,)), dma((RING,)),
        ],
        compiler_params=pltpu.CompilerParams(vmem_limit_bytes=EXPERT_VMEM * 2**20),
        cost_estimate=pl.CostEstimate(flops=20 * 10**9, bytes_accessed=98 * 10**6, transcendentals=0),
    )(cnt, xs, w1, w3, w2)


def combine_kernel(cap, scale, tab_ref, h_ref, ypack, out_ref, land, mix0, mix1, send, recv, own_sem):
    me = lax.axis_index("ep")
    barrier = pltpu.get_barrier_semaphore()
    for k in range(1, GROUP):
        pl.semaphore_signal(barrier, inc=1, device_id={"ep": lax.rem(me + k, GROUP)}, device_id_type=MESH)
    pl.semaphore_wait(barrier, GROUP - 1)
    copies = []
    for k in range(1, GROUP):
        to = lax.rem(me + k, GROUP)
        copy = pltpu.make_async_remote_copy(src_ref=ypack.at[to, pl.ds(0, cap), :], dst_ref=land.at[me], send_sem=send.at[k], recv_sem=recv.at[k],
                                            device_id={"ep": to}, device_id_type=MESH)
        copy.start()
        copies.append(copy)
    own = pltpu.make_async_copy(ypack.at[me, pl.ds(0, cap), :], land.at[me], own_sem.at[0])
    own.start()

    lane = lax.broadcasted_iota(I32, (TOK, cap), 1)
    own0, pos0 = tab_ref[:, 0:1].astype(I32), tab_ref[:, 1:2].astype(I32)
    own1, pos1 = tab_ref[:, 3:4].astype(I32), tab_ref[:, 4:5].astype(I32)

    def tables(frm):
        t0 = ((own0 == frm) & (pos0 == lane)).astype(F32).astype(BF16)
        t1 = ((own1 == frm) & (pos1 == lane)).astype(F32).astype(BF16)
        return t0, t1

    own.wait()
    t0, t1 = tables(me)
    mix0[...] = dot(t0, land[me])
    mix1[...] = dot(t1, land[me])

    def add(k, carry):
        frm = lax.rem(me + GROUP - k, GROUP)
        pltpu.make_async_remote_copy(src_ref=land.at[frm], dst_ref=land.at[frm], send_sem=send.at[k], recv_sem=recv.at[k],
                                     device_id={"ep": lax.rem(me + k, GROUP)}, device_id_type=MESH).wait_recv()
        t0, t1 = tables(frm)
        mix0[...] += dot(t0, land[frm])
        mix1[...] += dot(t1, land[frm])
        return carry

    lax.fori_loop(1, GROUP, add, 0)
    mixed = tab_ref[:, 2:3] * mix0[...] + tab_ref[:, 5:6] * mix1[...]
    out_ref[...] = (scale[0] * h_ref[...].astype(F32) + scale[1] * mixed).astype(BF16)
    for copy in copies:
        copy.wait_send()


def combine(index, cap, scale, tab, hidden, ypack):
    vmem = pl.BlockSpec(memory_space=pltpu.VMEM)
    dma = pltpu.SemaphoreType.DMA
    return pl.pallas_call(
        functools.partial(combine_kernel, cap),
        name=f"combine_{cap}",
        out_shape=jax.ShapeDtypeStruct((TOK, WIDTH), BF16),
        in_specs=[pl.BlockSpec(memory_space=pltpu.SMEM), vmem, vmem, pl.BlockSpec(memory_space=pl.ANY)],
        out_specs=vmem,
        scratch_shapes=[
            pltpu.VMEM((GROUP, cap, WIDTH), BF16),
            pltpu.VMEM((TOK, WIDTH), F32),
            pltpu.VMEM((TOK, WIDTH), F32),
            dma((GROUP,)), dma((GROUP,)), dma((1,)),
        ],
        compiler_params=pltpu.CompilerParams(collective_id=2 + index, has_side_effects=True, vmem_limit_bytes=30 * 2**20),
    )(scale, tab, hidden, ypack)


def solution(mesh):
    def local_step(hidden, router_w, expert_ids, w_gate, w_up, w_down, post_scale):
        xs, cnt, tab, top = gather(expert_ids.T, hidden, router_w.T)
        ypack = experts(cnt, xs, w_gate, w_up, w_down)
        need = top[0, 0]
        which = sum((need > cap).astype(I32) for cap in BUCKETS[:-1])
        branches = [functools.partial(combine, i, cap) for i, cap in enumerate(BUCKETS)]
        return lax.switch(which, branches, post_scale, tab, hidden, ypack)

    tok_spec = P(("dp", "ep"))
    return jax.shard_map(local_step, mesh=mesh, in_specs=(tok_spec, P(), tok_spec, P("ep"), P("ep"), P("ep"), P()), out_specs=tok_spec, check_vma=False)
```

```python
import functools

import jax
import jax.numpy as jnp
from jax import lax
from jax.experimental import pallas as pl
from jax.experimental.pallas import tpu as pltpu
from jax.sharding import PartitionSpec as P

MESH = pl.DeviceIdType.MESH
BF16, F32, I32 = jnp.bfloat16, jnp.float32, jnp.int32
GROUP = 8
WORLD = 16
LOCAL = 4
EXPERTS = GROUP * LOCAL
TOK = 256
SLOTS = 64
WIDTH = 1536
FFN = 2304
CHUNKS = 4
BASE = 16
EXTRA = SLOTS - BASE
BROWS = GROUP * BASE
BUCKETS = tuple(EXTRA * (i + 1) for i in range(LOCAL))
FCH = 768
NCH = FFN // FCH
DCH = 512
RING = 3
XROWS = GROUP * EXTRA + 128
GATHER_VMEM = 15
EXPERT_VMEM = 24
BASE_VMEM = 27


def dot(a, b):
    return jnp.dot(a, b, preferred_element_type=F32)


def dot_t(a, b):
    return lax.dot_general(a, b, (((1,), (1,)), ((), ())), preferred_element_type=F32)


def extra_rows(count):
    over = jnp.maximum(count - BASE, 0.0)
    return jnp.floor((over + 15.0) * (1.0 / 16.0)) * 16.0


def gather_kernel(ids_ref, h_ref, wr_ref, xb_ref, xe_ref, cnt_ref, tab_ref, top_ref,
                  hall, rk, idbuf, id_send, id_recv, x_send, y_send, p_send, x_recv, y_recv, d_recv, p_recv, own_sem):
    dp, me = lax.axis_index("dp"), lax.axis_index("ep")
    core, xc, yc = lax.rem(me, 2), lax.rem(me // 2, 2), me // 4
    xn, yn, pc = me + 2 - 4 * xc, me + 4 - 8 * yc, me + 1 - 2 * core
    dg = xn + 4 - 8 * yc
    my = dp * GROUP + me
    rows = TOK // CHUNKS

    barrier = pltpu.get_barrier_semaphore()
    for k in range(1, WORLD):
        g = lax.rem(my + k, WORLD)
        pl.semaphore_signal(barrier, inc=1, device_id={"dp": g // GROUP, "ep": lax.rem(g, GROUP)}, device_id_type=MESH)
    pl.semaphore_wait(barrier, WORLD - 1)

    def piece(block, q):
        return hall.at[block, pl.ds(q * rows, rows), :]

    def mine(q):
        return h_ref.at[pl.ds(q * rows, rows), :]

    def remote(src, dst, send, recv, dev):
        return pltpu.make_async_remote_copy(src_ref=src, dst_ref=dst, send_sem=send, recv_sem=recv,
                                            device_id={"ep": dev}, device_id_type=MESH)

    half = CHUNKS // 2
    sends = []

    def start(copy):
        copy.start()
        sends.append(copy)

    def send_x(q):
        start(remote(mine(q), piece(me, q), x_send.at[q], x_recv.at[q], xn))

    def send_y(q):
        start(remote(mine(q), piece(me, q), y_send.at[q], y_recv.at[q], yn))

    for i in range(half):
        send_x(i)
        send_y(i + half)
    id_copies = []
    for k in range(1, WORLD):
        g = lax.rem(my + k, WORLD)
        copy = pltpu.make_async_remote_copy(src_ref=ids_ref, dst_ref=idbuf.at[my], send_sem=id_send.at[k], recv_sem=id_recv.at[k],
                                            device_id={"dp": g // GROUP, "ep": lax.rem(g, GROUP)}, device_id_type=MESH)
        copy.start()
        id_copies.append(copy)
    start(remote(h_ref, hall.at[me], p_send.at[3 * CHUNKS], p_recv.at[3 * CHUNKS], pc))
    own_ids = pltpu.make_async_copy(ids_ref, idbuf.at[my], own_sem.at[0])
    own_ids.start()

    upper = (lax.broadcasted_iota(I32, (TOK, TOK), 0) < lax.broadcasted_iota(I32, (TOK, TOK), 1)).astype(BF16)
    hb = h_ref[...]
    wr = wr_ref[...]
    w_hi = wr.astype(BF16)
    rest = wr - w_hi.astype(F32)
    w_mid = rest.astype(BF16)
    w_lo = (rest - w_mid.astype(F32)).astype(BF16)
    logits = dot_t(w_hi, hb) + (dot_t(w_mid, hb) + dot_t(w_lo, hb))
    prob = jnp.exp(logits - jnp.max(logits, axis=0, keepdims=True))
    prob = prob / jnp.sum(prob, axis=0, keepdims=True)
    e_iota = lax.broadcasted_iota(I32, (EXPERTS, TOK), 0)
    id0, id1 = ids_ref[0:1, :], ids_ref[1:2, :]
    hit0, hit1 = e_iota == id0, e_iota == id1
    pick0 = jnp.sum(jnp.where(hit0, prob, 0.0), axis=0, keepdims=True)
    pick1 = jnp.sum(jnp.where(hit1, prob, 0.0), axis=0, keepdims=True)
    both = pick0 + pick1
    hits = jnp.where(hit0 | hit1, 1.0, 0.0)
    rank = dot(hits.astype(BF16), upper)
    er, ec = lax.broadcasted_iota(I32, (EXPERTS, EXPERTS), 0), lax.broadcasted_iota(I32, (EXPERTS, EXPERTS), 1)
    before = ((er // LOCAL == ec // LOCAL) & (ec < er)).astype(BF16)
    extra = extra_rows(jnp.sum(hits, axis=1, keepdims=True))
    start_e = dot(before, jnp.broadcast_to(extra, (EXPERTS, 128)).astype(BF16))[:, 0:1]
    local = (lax.broadcasted_iota(I32, (EXPERTS, 1), 0) % LOCAL).astype(F32)
    place_b = jnp.where(rank < BASE, local * BASE + rank, -1.0)
    place_e = jnp.where(rank < BASE, -1.0, start_e + rank - BASE)

    def at(hit, place):
        return jnp.sum(jnp.where(hit, place, 0.0), axis=0, keepdims=True)

    own0, own1 = (id0 // LOCAL).astype(F32), (id1 // LOCAL).astype(F32)
    fields = jnp.concatenate([own0, at(hit0, place_b), at(hit0, place_e), pick0 / both,
                              own1, at(hit1, place_b), at(hit1, place_e), pick1 / both, jnp.zeros((120, TOK), F32)], axis=0)
    tab_ref[...] = fields.T

    def arrived(block, q, sem):
        remote(piece(block, q), piece(block, q), x_send.at[0], sem, xn).wait_recv()

    for i in range(half):
        a, b = i, i + half
        arrived(xn, a, x_recv.at[a])
        start(remote(piece(xn, a), piece(xn, a), y_send.at[CHUNKS + i], d_recv.at[a], yn))
        send_y(a)
        start(remote(piece(xn, a), piece(xn, a), p_send.at[a], p_recv.at[a], pc))
        arrived(yn, b, y_recv.at[b])
        start(remote(piece(yn, b), piece(yn, b), x_send.at[CHUNKS + i], d_recv.at[b], xn))
        send_x(b)
        start(remote(piece(yn, b), piece(yn, b), p_send.at[CHUNKS + b], p_recv.at[CHUNKS + b], pc))
        if i == 0:
            own_ids.wait()
            for copy in id_copies:
                copy.wait()
            j_iota = lax.broadcasted_iota(I32, (8, TOK), 0)
            local_id = jnp.where(j_iota < LOCAL, me * LOCAL + j_iota, -1)
            hit_list = []
            for s in range(GROUP):
                pair = idbuf[dp * GROUP + s]
                hit_list.append((local_id == pair[0:1, :]) | (local_id == pair[1:2, :]))
            hit_f = jnp.where(jnp.concatenate(hit_list, axis=0), 1.0, 0.0)
            hit_b = hit_f.astype(BF16)
            rk[...] = jnp.where(hit_f > 0.5, dot(hit_b, upper), -1.0).astype(I32).reshape(GROUP, 8, TOK)
            cnt_ref[...] = dot_t(jnp.ones((8, TOK), BF16), hit_b).astype(I32)
            lane = lax.broadcasted_iota(I32, (EXPERTS, 128), 1)
            spread = jnp.zeros((EXPERTS, 128), F32)
            for g in range(WORLD):
                pair = idbuf[g]
                n = jnp.where((e_iota == pair[0:1, :]) | (e_iota == pair[1:2, :]), 1.0, 0.0)
                spread = jnp.where(lane == g, extra_rows(jnp.sum(n, axis=1, keepdims=True)), spread)
            groups = (lax.broadcasted_iota(I32, (GROUP, EXPERTS), 0) == lax.broadcasted_iota(I32, (GROUP, EXPERTS), 1) // LOCAL).astype(BF16)
            need = dot(groups, spread.astype(BF16))
            need = jnp.max(jnp.max(need, axis=1, keepdims=True), axis=0, keepdims=True)
            index = sum((need > cap).astype(I32) for cap in BUCKETS[:-1])
            top_ref[...] = jnp.broadcast_to(index, (8, 128))

    b_iota = lax.broadcasted_iota(I32, (BASE, TOK), 0)
    x_iota = lax.broadcasted_iota(I32, (EXTRA, TOK), 0) + BASE

    def pick(s, block):
        ranks = rk[s]
        table = jnp.concatenate([(b_iota == ranks[j:j + 1, :]).astype(F32) for j in range(LOCAL)]
                                + [(x_iota == ranks[j:j + 1, :]).astype(F32) for j in range(LOCAL)], axis=0).astype(BF16)
        rows = dot(table, block).astype(BF16)
        for j in range(LOCAL):
            xb_ref[j, pl.ds(pl.multiple_of(s * BASE, BASE), BASE), :] = rows[j * BASE:(j + 1) * BASE]
        xe_ref[s] = rows[LOCAL * BASE:]

    pick(me, hb)
    remote(hall.at[pc], hall.at[pc], x_send.at[0], p_recv.at[3 * CHUNKS], pc).wait_recv()
    pick(pc, hall[pc])
    for i in range(half):
        a, b = i + half, i
        arrived(xn, a, x_recv.at[a])
        start(remote(piece(xn, a), piece(xn, a), p_send.at[a], p_recv.at[a], pc))
        arrived(yn, b, y_recv.at[b])
        start(remote(piece(yn, b), piece(yn, b), p_send.at[CHUNKS + b], p_recv.at[CHUNKS + b], pc))
    for i in range(half):
        for q in (i, i + half):
            arrived(dg, q, d_recv.at[q])
            start(remote(piece(dg, q), piece(dg, q), p_send.at[2 * CHUNKS + q], p_recv.at[2 * CHUNKS + q], pc))
        if i == 0:
            pick(xn, hall[xn])
            pick(yn, hall[yn])
    turn = 1 - 2 * core
    for q in range(CHUNKS):
        arrived(xn + turn, q, p_recv.at[q])
        arrived(yn + turn, q, p_recv.at[CHUNKS + q])
    pick(xn + turn, hall[xn + turn])
    pick(yn + turn, hall[yn + turn])
    pick(dg, hall[dg])
    for q in range(CHUNKS):
        arrived(dg + turn, q, p_recv.at[2 * CHUNKS + q])
    pick(dg + turn, hall[dg + turn])
    for copy in sends:
        copy.wait_send()


def gather(ids_t, hidden, wr_t):
    vmem = pl.BlockSpec(memory_space=pltpu.VMEM)
    dma = pltpu.SemaphoreType.DMA
    return pl.pallas_call(
        gather_kernel,
        name="gather_rows",
        out_shape=[
            jax.ShapeDtypeStruct((LOCAL, BROWS, WIDTH), BF16),
            jax.ShapeDtypeStruct((GROUP, LOCAL * EXTRA, WIDTH), BF16),
            jax.ShapeDtypeStruct((8, GROUP * 8), I32),
            jax.ShapeDtypeStruct((TOK, 128), F32),
            jax.ShapeDtypeStruct((8, 128), I32),
        ],
        in_specs=[vmem] * 3,
        out_specs=[vmem] * 5,
        scratch_shapes=[
            pltpu.VMEM((GROUP, TOK, WIDTH), BF16),
            pltpu.VMEM((GROUP, 8, TOK), I32),
            pltpu.VMEM((WORLD, 2, TOK), I32),
            dma((WORLD,)), dma((WORLD,)),
            dma((2 * CHUNKS,)), dma((2 * CHUNKS,)), dma((3 * CHUNKS + 1,)),
            dma((CHUNKS,)), dma((CHUNKS,)), dma((CHUNKS,)), dma((3 * CHUNKS + 1,)),
            dma((1,)),
        ],
        compiler_params=pltpu.CompilerParams(collective_id=1, has_side_effects=True, vmem_limit_bytes=GATHER_VMEM * 2**20),
        cost_estimate=pl.CostEstimate(flops=20 * 10**9, bytes_accessed=20 * 10**6, transcendentals=0),
    )(ids_t, hidden, wr_t)


def extra_kernel(cnt, xe_ref, w1, w3, w2, ye_ref, xbuf, mid, b3, b2, offs, act, tot, w3_sem, w2_sem):
    def tiles(s, j):
        return (jnp.maximum(cnt[0, s * 8 + j] - BASE, 0) + 15) // 16 * 16

    active = jnp.int32(0)
    for j in range(LOCAL):
        at = jnp.int32(0)
        for s in range(GROUP):
            offs[s, j] = at
            at = at + tiles(s, j)
        tot[j] = at
        act[active] = j
        active = active + (at > 0).astype(I32)
    chunks = active * NCH

    def up_copy(g):
        slot = lax.rem(g, RING)
        cols = pl.ds(pl.multiple_of(lax.rem(g, NCH) * FCH, FCH), FCH)
        return pltpu.make_async_copy(w3.at[act[g // NCH], :, cols], b3.at[slot], w3_sem.at[slot])

    def down_copy(g):
        slot = lax.rem(g, RING)
        cols = pl.ds(pl.multiple_of(lax.rem(g, NCH) * DCH, DCH), DCH)
        return pltpu.make_async_copy(w2.at[act[g // NCH], :, cols], b2.at[slot], w2_sem.at[slot])

    def fetch(copy, g):
        @pl.when(g < chunks)
        def _():
            copy(g).start()

    for g in range(RING):
        fetch(up_copy, g)
    for g in range(RING):
        fetch(down_copy, g)

    def compact(s, carry):
        for j in range(LOCAL):
            @pl.when(tot[j] > 0)
            def _():
                xbuf[j, pl.ds(pl.multiple_of(offs[s, j], 16), EXTRA), :] = xe_ref[s, j * EXTRA:(j + 1) * EXTRA, :]
        return carry

    lax.fori_loop(0, GROUP, compact, 0)

    def expert(a, carry):
        j = act[a]
        total = tot[j]
        blocks = (total + 127) // 128
        xbuf[j, pl.ds(pl.multiple_of(total, 16), 128), :] = jnp.zeros((128, WIDTH), BF16)

        def over_rows(body):
            def wide(i, c):
                body(pl.multiple_of(i * 256, 256), 256)
                return c

            lax.fori_loop(0, blocks // 2, wide, 0)

            @pl.when(lax.rem(blocks, 2) == 1)
            def _():
                body(pl.multiple_of((blocks // 2) * 256, 128), 128)

        def up_step(f, c):
            g = a * NCH + f
            slot = lax.rem(g, RING)
            up_copy(g).wait()

            def body(row, n):
                x = xbuf[j, pl.ds(row, n), :]
                for p in range(FCH // 256):
                    cols = pl.ds(pl.multiple_of(f * FCH + p * 256, 256), 256)
                    up = dot(x, w1[j, :, cols])
                    lin = dot(x, b3[slot, :, p * 256:(p + 1) * 256])
                    mid[pl.ds(row, n), cols] = (jax.nn.silu(up) * lin).astype(BF16)

            over_rows(body)
            fetch(up_copy, g + RING)
            return c

        def down_step(f, c):
            g = a * NCH + f
            slot = lax.rem(g, RING)
            down_copy(g).wait()

            def body(row, n):
                cols = pl.ds(pl.multiple_of(f * DCH, DCH), DCH)
                xbuf[j, pl.ds(row, n), cols] = dot(mid[pl.ds(row, n), :], b2[slot]).astype(BF16)

            over_rows(body)
            fetch(down_copy, g + RING)
            return c

        lax.fori_loop(0, NCH, up_step, 0)
        lax.fori_loop(0, NCH, down_step, 0)
        return carry

    lax.fori_loop(0, active, expert, 0)

    def pack(s, carry):
        at = jnp.int32(0)
        for j in range(LOCAL):
            n = tiles(s, j)

            @pl.when(n > 0)
            def _():
                ye_ref[s, pl.ds(pl.multiple_of(at, 16), EXTRA), :] = xbuf[j, pl.ds(pl.multiple_of(offs[s, j], 16), EXTRA), :]
            at = at + n
        return carry

    lax.fori_loop(0, GROUP, pack, 0)


def extra(cnt, xe, w1, w3, w2):
    hbm = pl.BlockSpec(memory_space=pl.ANY)
    vmem = pl.BlockSpec(memory_space=pltpu.VMEM)
    dma = pltpu.SemaphoreType.DMA
    return pl.pallas_call(
        extra_kernel,
        name="extra_rows",
        out_shape=jax.ShapeDtypeStruct((GROUP, LOCAL * EXTRA, WIDTH), BF16),
        in_specs=[pl.BlockSpec(memory_space=pltpu.SMEM), vmem, vmem, hbm, hbm],
        out_specs=vmem,
        input_output_aliases={1: 0},
        scratch_shapes=[
            pltpu.VMEM((LOCAL, XROWS, WIDTH), BF16),
            pltpu.VMEM((GROUP * EXTRA, FFN), BF16),
            pltpu.VMEM((RING, WIDTH, FCH), BF16),
            pltpu.VMEM((RING, FFN, DCH), BF16),
            pltpu.SMEM((GROUP, LOCAL), I32),
            pltpu.SMEM((LOCAL + 1,), I32),
            pltpu.SMEM((LOCAL,), I32),
            dma((RING,)), dma((RING,)),
        ],
        compiler_params=pltpu.CompilerParams(vmem_limit_bytes=EXPERT_VMEM * 2**20),
        cost_estimate=pl.CostEstimate(flops=8 * 10**9, bytes_accessed=30 * 10**6, transcendentals=0),
    )(cnt, xe, w1, w3, w2)


def base_kernel(cap, scale, tab_ref, h_ref, xb_ref, ye_ref, w1, w3, w2, out_ref,
                land_e, land_b, yb, mid, b3, b2, mix0, mix1, w3_sem, w2_sem, e_send, e_recv, b_send, b_recv):
    me = lax.axis_index("ep")

    def up_copy(j, f):
        return pltpu.make_async_copy(w3.at[j, :, pl.ds(f * FCH, FCH)], b3.at[f], w3_sem.at[f])

    def down_copy(j, f):
        return pltpu.make_async_copy(w2.at[j, :, pl.ds(f * DCH, DCH)], b2.at[f], w2_sem.at[f])

    for f in range(NCH):
        up_copy(0, f).start()
    for f in range(NCH):
        down_copy(0, f).start()

    barrier = pltpu.get_barrier_semaphore()
    for k in range(1, GROUP):
        pl.semaphore_signal(barrier, inc=1, device_id={"ep": lax.rem(me + k, GROUP)}, device_id_type=MESH)
    pl.semaphore_wait(barrier, GROUP - 1)

    def e_copy(k):
        to = lax.rem(me + k, GROUP)
        return pltpu.make_async_remote_copy(src_ref=ye_ref.at[to, pl.ds(0, cap), :], dst_ref=land_e.at[me], send_sem=e_send.at[k], recv_sem=e_recv.at[k],
                                            device_id={"ep": to}, device_id_type=MESH)

    def b_copy(j, k):
        to = lax.rem(me + k, GROUP)
        return pltpu.make_async_remote_copy(src_ref=yb.at[j, pl.ds(pl.multiple_of(to * BASE, BASE), BASE), :],
                                            dst_ref=land_b.at[me, pl.ds(pl.multiple_of(j * BASE, BASE), BASE), :],
                                            send_sem=b_send.at[j, k], recv_sem=b_recv.at[j, k],
                                            device_id={"ep": to}, device_id_type=MESH)

    for k in range(1, GROUP):
        e_copy(k).start()
    land_e[me] = ye_ref[me, :cap, :]

    def expert(j, carry):
        x = xb_ref[j]
        for f in range(NCH):
            up_copy(j, f).wait()
            for p in range(FCH // 256):
                cols = pl.ds(f * FCH + p * 256, 256)
                up = dot(x, w1[j, :, cols])
                lin = dot(x, b3[f, :, p * 256:(p + 1) * 256])
                mid[:, cols] = (jax.nn.silu(up) * lin).astype(BF16)

            @pl.when(j + 1 < LOCAL)
            def _():
                up_copy(j + 1, f).start()
        for f in range(NCH):
            down_copy(j, f).wait()
            yb[j, :, f * DCH:(f + 1) * DCH] = dot(mid[...], b2[f]).astype(BF16)

            @pl.when(j + 1 < LOCAL)
            def _():
                down_copy(j + 1, f).start()
        land_b[me, pl.ds(pl.multiple_of(j * BASE, BASE), BASE), :] = yb[j, pl.ds(pl.multiple_of(me * BASE, BASE), BASE), :]
        for k in range(1, GROUP):
            b_copy(j, k).start()
        return carry

    lax.fori_loop(0, LOCAL, expert, 0)

    def columns(field, rows):
        place = tab_ref[:, field:field + 1]
        col = jnp.where(place < 0.0, -1.0, tab_ref[:, field // 4 * 4:field // 4 * 4 + 1] * rows + place).astype(I32)
        return (col == lax.broadcasted_iota(I32, (TOK, GROUP * rows), 1)).astype(F32).astype(BF16)

    for k in range(1, GROUP):
        e_copy(k).wait()
    far = land_e[...].reshape(GROUP * cap, WIDTH)
    mix0[...] = dot(columns(2, cap), far)
    mix1[...] = dot(columns(6, cap), far)
    for j in range(LOCAL):
        for k in range(1, GROUP):
            b_copy(j, k).wait()
    near = land_b[...].reshape(GROUP * LOCAL * BASE, WIDTH)
    y0 = mix0[...] + dot(columns(1, LOCAL * BASE), near)
    y1 = mix1[...] + dot(columns(5, LOCAL * BASE), near)
    mixed = tab_ref[:, 3:4] * y0 + tab_ref[:, 7:8] * y1
    out_ref[...] = (scale[0] * h_ref[...].astype(F32) + scale[1] * mixed).astype(BF16)


def base(index, cap, scale, tab, hidden, xb, ye, w1, w3, w2):
    vmem = pl.BlockSpec(memory_space=pltpu.VMEM)
    hbm = pl.BlockSpec(memory_space=pl.ANY)
    dma = pltpu.SemaphoreType.DMA
    return pl.pallas_call(
        functools.partial(base_kernel, cap),
        name=f"base_rows_{cap}",
        out_shape=jax.ShapeDtypeStruct((TOK, WIDTH), BF16),
        in_specs=[pl.BlockSpec(memory_space=pltpu.SMEM)] + [vmem] * 5 + [hbm] * 2,
        out_specs=vmem,
        scratch_shapes=[
            pltpu.VMEM((GROUP, cap, WIDTH), BF16),
            pltpu.VMEM((GROUP, LOCAL * BASE, WIDTH), BF16),
            pltpu.VMEM((LOCAL, BROWS, WIDTH), BF16),
            pltpu.VMEM((BROWS, FFN), BF16),
            pltpu.VMEM((RING, WIDTH, FCH), BF16),
            pltpu.VMEM((RING, FFN, DCH), BF16),
            pltpu.VMEM((TOK, WIDTH), F32),
            pltpu.VMEM((TOK, WIDTH), F32),
            dma((RING,)), dma((RING,)),
            dma((GROUP,)), dma((GROUP,)), dma((LOCAL, GROUP)), dma((LOCAL, GROUP)),
        ],
        compiler_params=pltpu.CompilerParams(collective_id=2 + index, has_side_effects=True, vmem_limit_bytes=BASE_VMEM * 2**20),
    )(scale, tab, hidden, xb, ye, w1, w3, w2)


def solution(mesh):
    def local_step(hidden, router_w, expert_ids, w_gate, w_up, w_down, post_scale):
        xb, xe, cnt, tab, top = gather(expert_ids.T, hidden, router_w.T)
        ye = extra(cnt, xe, w_gate, w_up, w_down)
        branches = [functools.partial(base, i, cap) for i, cap in enumerate(BUCKETS)]
        return lax.switch(top[0, 0], branches, post_scale, tab, hidden, xb, ye, w_gate, w_up, w_down)

    tok_spec = P(("dp", "ep"))
    return jax.shard_map(local_step, mesh=mesh, in_specs=(tok_spec, P(), tok_spec, P("ep"), P("ep"), P("ep"), P()), out_specs=tok_spec, check_vma=False)
```

```python
import functools

import jax
import jax.numpy as jnp
from jax import lax
from jax.experimental import pallas as pl
from jax.experimental.pallas import tpu as pltpu
from jax.sharding import PartitionSpec as P

MESH = pl.DeviceIdType.MESH
BF16, F32, I32 = jnp.bfloat16, jnp.float32, jnp.int32
GROUP = 8
LOCAL = 4
EXPERTS = GROUP * LOCAL
TOK = 256
SLOTS = 64
WIDTH = 1536
FFN = 2304
CHUNKS = 4
BASE = 16
EXTRA = SLOTS - BASE
BROWS = GROUP * BASE
BUCKETS = tuple(EXTRA * (i + 1) for i in range(LOCAL))
FCH = 768
NCH = FFN // FCH
DCH = 512
RING = 3
XROWS = GROUP * EXTRA + 128
GATHER_VMEM = 15
EXPERT_VMEM = 24
BASE_VMEM = 27


def dot(a, b):
    return jnp.dot(a, b, preferred_element_type=F32)


def dot_t(a, b):
    return lax.dot_general(a, b, (((1,), (1,)), ((), ())), preferred_element_type=F32)


def extra_rows(count):
    over = jnp.maximum(count - BASE, 0.0)
    return jnp.floor((over + 15.0) * (1.0 / 16.0)) * 16.0


def gather_kernel(ids_ref, h_ref, wr_ref, xb_ref, xe_ref, cnt_ref, tab_ref, top_ref,
                  hall, rk, idbuf, needs, id_send, id_recv, x_send, y_send, p_send, x_recv, y_recv, d_recv, p_recv, own_sem):
    dp, me = lax.axis_index("dp"), lax.axis_index("ep")
    core, xc, yc = lax.rem(me, 2), lax.rem(me // 2, 2), me // 4
    xn, yn, pc = me + 2 - 4 * xc, me + 4 - 8 * yc, me + 1 - 2 * core
    dg = xn + 4 - 8 * yc
    rows = TOK // CHUNKS

    barrier = pltpu.get_barrier_semaphore()
    for k in range(1, GROUP):
        pl.semaphore_signal(barrier, inc=1, device_id={"ep": lax.rem(me + k, GROUP)}, device_id_type=MESH)
    pl.semaphore_signal(barrier, inc=1, device_id={"dp": 1 - dp, "ep": me}, device_id_type=MESH)
    pl.semaphore_wait(barrier, GROUP)

    def piece(block, q):
        return hall.at[block, pl.ds(q * rows, rows), :]

    def mine(q):
        return h_ref.at[pl.ds(q * rows, rows), :]

    def remote(src, dst, send, recv, dev):
        return pltpu.make_async_remote_copy(src_ref=src, dst_ref=dst, send_sem=send, recv_sem=recv,
                                            device_id={"ep": dev}, device_id_type=MESH)

    half = CHUNKS // 2
    sends = []

    def start(copy):
        copy.start()
        sends.append(copy)

    def send_x(q):
        start(remote(mine(q), piece(me, q), x_send.at[q], x_recv.at[q], xn))

    def send_y(q):
        start(remote(mine(q), piece(me, q), y_send.at[q], y_recv.at[q], yn))

    id_copies = []
    for k in range(1, GROUP):
        id_copies.append(remote(ids_ref, idbuf.at[me], id_send.at[k], id_recv.at[k], lax.rem(me + k, GROUP)))
        id_copies[-1].start()
    for i in range(CHUNKS):
        send_x(i)
        send_y((i + half) % CHUNKS)
    start(remote(h_ref, hall.at[me], p_send.at[3 * CHUNKS], p_recv.at[3 * CHUNKS], pc))
    own_ids = pltpu.make_async_copy(ids_ref, idbuf.at[me], own_sem.at[0])
    own_ids.start()

    upper = (lax.broadcasted_iota(I32, (TOK, TOK), 0) < lax.broadcasted_iota(I32, (TOK, TOK), 1)).astype(BF16)
    hb = h_ref[...]
    wr = wr_ref[...]
    w_hi = wr.astype(BF16)
    rest = wr - w_hi.astype(F32)
    w_mid = rest.astype(BF16)
    w_lo = (rest - w_mid.astype(F32)).astype(BF16)
    logits = dot_t(w_hi, hb) + (dot_t(w_mid, hb) + dot_t(w_lo, hb))
    prob = jnp.exp(logits - jnp.max(logits, axis=0, keepdims=True))
    prob = prob / jnp.sum(prob, axis=0, keepdims=True)
    e_iota = lax.broadcasted_iota(I32, (EXPERTS, TOK), 0)
    id0, id1 = ids_ref[0:1, :], ids_ref[1:2, :]
    hit0, hit1 = e_iota == id0, e_iota == id1
    pick0 = jnp.sum(jnp.where(hit0, prob, 0.0), axis=0, keepdims=True)
    pick1 = jnp.sum(jnp.where(hit1, prob, 0.0), axis=0, keepdims=True)
    both = pick0 + pick1
    hits = jnp.where(hit0 | hit1, 1.0, 0.0)
    rank = dot(hits.astype(BF16), upper)
    er, ec = lax.broadcasted_iota(I32, (EXPERTS, EXPERTS), 0), lax.broadcasted_iota(I32, (EXPERTS, EXPERTS), 1)
    before = ((er // LOCAL == ec // LOCAL) & (ec < er)).astype(BF16)
    extra = extra_rows(jnp.sum(hits, axis=1, keepdims=True))
    start_e = dot(before, jnp.broadcast_to(extra, (EXPERTS, 128)).astype(BF16))[:, 0:1]
    local = (lax.broadcasted_iota(I32, (EXPERTS, 1), 0) % LOCAL).astype(F32)
    place_b = jnp.where(rank < BASE, local * BASE + rank, -1.0)
    place_e = jnp.where(rank < BASE, -1.0, start_e + rank - BASE)

    def at(hit, place):
        return jnp.sum(jnp.where(hit, place, 0.0), axis=0, keepdims=True)

    own0, own1 = (id0 // LOCAL).astype(F32), (id1 // LOCAL).astype(F32)
    fields = jnp.concatenate([own0, at(hit0, place_b), at(hit0, place_e), pick0 / both,
                              own1, at(hit1, place_b), at(hit1, place_e), pick1 / both, jnp.zeros((120, TOK), F32)], axis=0)
    tab_ref[...] = fields.T

    own_ids.wait()
    for copy in id_copies:
        copy.wait()
    j_iota = lax.broadcasted_iota(I32, (8, TOK), 0)
    local_id = jnp.where(j_iota < LOCAL, me * LOCAL + j_iota, -1)
    hit_list = []
    for s in range(GROUP):
        pair = idbuf[s]
        hit_list.append((local_id == pair[0:1, :]) | (local_id == pair[1:2, :]))
    hit_f = jnp.where(jnp.concatenate(hit_list, axis=0), 1.0, 0.0)
    hit_b = hit_f.astype(BF16)
    rk[...] = jnp.where(hit_f > 0.5, dot(hit_b, upper), -1.0).astype(I32).reshape(GROUP, 8, TOK)
    cnt_ref[...] = dot_t(jnp.ones((8, TOK), BF16), hit_b).astype(I32)
    lane = lax.broadcasted_iota(I32, (EXPERTS, 128), 1)
    spread = jnp.zeros((EXPERTS, 128), F32)
    for g in range(GROUP):
        pair = idbuf[g]
        n = jnp.where((e_iota == pair[0:1, :]) | (e_iota == pair[1:2, :]), 1.0, 0.0)
        spread = jnp.where(lane == g, extra_rows(jnp.sum(n, axis=1, keepdims=True)), spread)
    groups = (lax.broadcasted_iota(I32, (GROUP, EXPERTS), 0) == lax.broadcasted_iota(I32, (GROUP, EXPERTS), 1) // LOCAL).astype(BF16)
    need = dot(groups, spread.astype(BF16))
    need = jnp.max(jnp.max(need, axis=1, keepdims=True), axis=0, keepdims=True)
    needs[0] = jnp.broadcast_to(need, (8, 128))

    def arrived(block, q, sem):
        remote(piece(block, q), piece(block, q), x_send.at[0], sem, xn).wait_recv()

    for i in range(half):
        a, b = i, i + half
        arrived(xn, a, x_recv.at[a])
        start(remote(piece(xn, a), piece(xn, a), y_send.at[CHUNKS + i], d_recv.at[a], yn))
        start(remote(piece(xn, a), piece(xn, a), p_send.at[a], p_recv.at[a], pc))
        arrived(yn, b, y_recv.at[b])
        start(remote(piece(yn, b), piece(yn, b), x_send.at[CHUNKS + i], d_recv.at[b], xn))
        start(remote(piece(yn, b), piece(yn, b), p_send.at[CHUNKS + b], p_recv.at[CHUNKS + b], pc))
    other = pltpu.make_async_remote_copy(src_ref=needs.at[0], dst_ref=needs.at[1], send_sem=id_send.at[0], recv_sem=id_recv.at[0],
                                         device_id={"dp": 1 - dp, "ep": me}, device_id_type=MESH)
    other.start()

    b_iota = lax.broadcasted_iota(I32, (BASE, TOK), 0)
    x_iota = lax.broadcasted_iota(I32, (EXTRA, TOK), 0) + BASE

    def pick(s, block):
        ranks = rk[s]
        table = jnp.concatenate([(b_iota == ranks[j:j + 1, :]).astype(F32) for j in range(LOCAL)]
                                + [(x_iota == ranks[j:j + 1, :]).astype(F32) for j in range(LOCAL)], axis=0).astype(BF16)
        rows = dot(table, block).astype(BF16)
        for j in range(LOCAL):
            xb_ref[j, pl.ds(pl.multiple_of(s * BASE, BASE), BASE), :] = rows[j * BASE:(j + 1) * BASE]
        xe_ref[s] = rows[LOCAL * BASE:]

    pick(me, hb)
    remote(hall.at[pc], hall.at[pc], x_send.at[0], p_recv.at[3 * CHUNKS], pc).wait_recv()
    pick(pc, hall[pc])
    for i in range(half):
        a, b = i + half, i
        arrived(xn, a, x_recv.at[a])
        start(remote(piece(xn, a), piece(xn, a), p_send.at[a], p_recv.at[a], pc))
        arrived(yn, b, y_recv.at[b])
        start(remote(piece(yn, b), piece(yn, b), p_send.at[CHUNKS + b], p_recv.at[CHUNKS + b], pc))
    for i in range(half):
        for q in (i, i + half):
            arrived(dg, q, d_recv.at[q])
            start(remote(piece(dg, q), piece(dg, q), p_send.at[2 * CHUNKS + q], p_recv.at[2 * CHUNKS + q], pc))
        if i == 0:
            pick(xn, hall[xn])
            pick(yn, hall[yn])
    turn = 1 - 2 * core
    for q in range(CHUNKS):
        arrived(xn + turn, q, p_recv.at[q])
        arrived(yn + turn, q, p_recv.at[CHUNKS + q])
    pick(xn + turn, hall[xn + turn])
    pick(yn + turn, hall[yn + turn])
    pick(dg, hall[dg])
    for q in range(CHUNKS):
        arrived(dg + turn, q, p_recv.at[2 * CHUNKS + q])
    pick(dg + turn, hall[dg + turn])
    other.wait()
    both_need = jnp.maximum(needs[0], needs[1])
    top_ref[...] = sum((both_need > cap).astype(I32) for cap in BUCKETS[:-1])
    for copy in sends:
        copy.wait_send()


def gather(ids_t, hidden, wr_t):
    vmem = pl.BlockSpec(memory_space=pltpu.VMEM)
    dma = pltpu.SemaphoreType.DMA
    return pl.pallas_call(
        gather_kernel,
        name="gather_rows",
        out_shape=[
            jax.ShapeDtypeStruct((LOCAL, BROWS, WIDTH), BF16),
            jax.ShapeDtypeStruct((GROUP, LOCAL * EXTRA, WIDTH), BF16),
            jax.ShapeDtypeStruct((8, GROUP * 8), I32),
            jax.ShapeDtypeStruct((TOK, 128), F32),
            jax.ShapeDtypeStruct((8, 128), I32),
        ],
        in_specs=[vmem] * 3,
        out_specs=[vmem] * 5,
        scratch_shapes=[
            pltpu.VMEM((GROUP, TOK, WIDTH), BF16),
            pltpu.VMEM((GROUP, 8, TOK), I32),
            pltpu.VMEM((GROUP, 2, TOK), I32),
            pltpu.VMEM((2, 8, 128), F32),
            dma((GROUP,)), dma((GROUP,)),
            dma((2 * CHUNKS,)), dma((2 * CHUNKS,)), dma((3 * CHUNKS + 1,)),
            dma((CHUNKS,)), dma((CHUNKS,)), dma((CHUNKS,)), dma((3 * CHUNKS + 1,)),
            dma((1,)),
        ],
        compiler_params=pltpu.CompilerParams(collective_id=1, has_side_effects=True, vmem_limit_bytes=GATHER_VMEM * 2**20),
        cost_estimate=pl.CostEstimate(flops=20 * 10**9, bytes_accessed=20 * 10**6, transcendentals=0),
    )(ids_t, hidden, wr_t)


def extra_kernel(cnt, xe_ref, w1, w3, w2, ye_ref, xbuf, mid, b3, b2, offs, act, tot, w3_sem, w2_sem):
    def tiles(s, j):
        return (jnp.maximum(cnt[0, s * 8 + j] - BASE, 0) + 15) // 16 * 16

    active = jnp.int32(0)
    for j in range(LOCAL):
        at = jnp.int32(0)
        for s in range(GROUP):
            offs[s, j] = at
            at = at + tiles(s, j)
        tot[j] = at
        act[active] = j
        active = active + (at > 0).astype(I32)
    chunks = active * NCH

    def up_copy(g):
        slot = lax.rem(g, RING)
        cols = pl.ds(pl.multiple_of(lax.rem(g, NCH) * FCH, FCH), FCH)
        return pltpu.make_async_copy(w3.at[act[g // NCH], :, cols], b3.at[slot], w3_sem.at[slot])

    def down_copy(g):
        slot = lax.rem(g, RING)
        cols = pl.ds(pl.multiple_of(lax.rem(g, NCH) * DCH, DCH), DCH)
        return pltpu.make_async_copy(w2.at[act[g // NCH], :, cols], b2.at[slot], w2_sem.at[slot])

    def fetch(copy, g):
        @pl.when(g < chunks)
        def _():
            copy(g).start()

    for g in range(RING):
        fetch(up_copy, g)
    for g in range(RING):
        fetch(down_copy, g)

    def compact(s, carry):
        for j in range(LOCAL):
            @pl.when(tot[j] > 0)
            def _():
                xbuf[j, pl.ds(pl.multiple_of(offs[s, j], 16), EXTRA), :] = xe_ref[s, j * EXTRA:(j + 1) * EXTRA, :]
        return carry

    lax.fori_loop(0, GROUP, compact, 0)
    ye_ref[...] = jnp.zeros_like(ye_ref)

    def expert(a, carry):
        j = act[a]
        total = tot[j]
        blocks = (total + 127) // 128
        xbuf[j, pl.ds(pl.multiple_of(total, 16), 128), :] = jnp.zeros((128, WIDTH), BF16)

        def over_rows(body):
            def wide(i, c):
                body(pl.multiple_of(i * 256, 256), 256)
                return c

            lax.fori_loop(0, blocks // 2, wide, 0)

            @pl.when(lax.rem(blocks, 2) == 1)
            def _():
                body(pl.multiple_of((blocks // 2) * 256, 128), 128)

        def up_step(f, c):
            g = a * NCH + f
            slot = lax.rem(g, RING)
            up_copy(g).wait()

            def body(row, n):
                x = xbuf[j, pl.ds(row, n), :]
                for p in range(FCH // 256):
                    cols = pl.ds(pl.multiple_of(f * FCH + p * 256, 256), 256)
                    up = dot(x, w1[j, :, cols])
                    lin = dot(x, b3[slot, :, p * 256:(p + 1) * 256])
                    mid[pl.ds(row, n), cols] = (jax.nn.silu(up) * lin).astype(BF16)

            over_rows(body)
            fetch(up_copy, g + RING)
            return c

        def down_step(f, c):
            g = a * NCH + f
            slot = lax.rem(g, RING)
            down_copy(g).wait()

            def body(row, n):
                cols = pl.ds(pl.multiple_of(f * DCH, DCH), DCH)
                xbuf[j, pl.ds(row, n), cols] = dot(mid[pl.ds(row, n), :], b2[slot]).astype(BF16)

            over_rows(body)
            fetch(down_copy, g + RING)
            return c

        lax.fori_loop(0, NCH, up_step, 0)
        lax.fori_loop(0, NCH, down_step, 0)
        return carry

    lax.fori_loop(0, active, expert, 0)

    def pack(s, carry):
        at = jnp.int32(0)
        for j in range(LOCAL):
            n = tiles(s, j)

            @pl.when(n > 0)
            def _():
                ye_ref[s, pl.ds(pl.multiple_of(at, 16), EXTRA), :] = xbuf[j, pl.ds(pl.multiple_of(offs[s, j], 16), EXTRA), :]
            at = at + n
        return carry

    lax.fori_loop(0, GROUP, pack, 0)


def extra(cnt, xe, w1, w3, w2):
    hbm = pl.BlockSpec(memory_space=pl.ANY)
    vmem = pl.BlockSpec(memory_space=pltpu.VMEM)
    dma = pltpu.SemaphoreType.DMA
    return pl.pallas_call(
        extra_kernel,
        name="extra_rows",
        out_shape=jax.ShapeDtypeStruct((GROUP, LOCAL * EXTRA, WIDTH), BF16),
        in_specs=[pl.BlockSpec(memory_space=pltpu.SMEM), vmem, vmem, hbm, hbm],
        out_specs=vmem,
        input_output_aliases={1: 0},
        scratch_shapes=[
            pltpu.VMEM((LOCAL, XROWS, WIDTH), BF16),
            pltpu.VMEM((GROUP * EXTRA, FFN), BF16),
            pltpu.VMEM((RING, WIDTH, FCH), BF16),
            pltpu.VMEM((RING, FFN, DCH), BF16),
            pltpu.SMEM((GROUP, LOCAL), I32),
            pltpu.SMEM((LOCAL + 1,), I32),
            pltpu.SMEM((LOCAL,), I32),
            dma((RING,)), dma((RING,)),
        ],
        compiler_params=pltpu.CompilerParams(vmem_limit_bytes=EXPERT_VMEM * 2**20),
        cost_estimate=pl.CostEstimate(flops=8 * 10**9, bytes_accessed=30 * 10**6, transcendentals=0),
    )(cnt, xe, w1, w3, w2)


def base_kernel(cap, scale, tab_ref, h_ref, xb_ref, ye_ref, w1, w3, w2, out_ref,
                land_e, land_b, yb, mid, b3, b2, mix0, mix1, w3_sem, w2_sem, e_send, e_recv, b_send, b_recv):
    me = lax.axis_index("ep")

    def up_copy(j, f):
        return pltpu.make_async_copy(w3.at[j, :, pl.ds(f * FCH, FCH)], b3.at[f], w3_sem.at[f])

    def down_copy(j, f):
        return pltpu.make_async_copy(w2.at[j, :, pl.ds(f * DCH, DCH)], b2.at[f], w2_sem.at[f])

    for f in range(NCH):
        up_copy(0, f).start()
    for f in range(NCH):
        down_copy(0, f).start()

    barrier = pltpu.get_barrier_semaphore()
    for k in range(1, GROUP):
        pl.semaphore_signal(barrier, inc=1, device_id={"ep": lax.rem(me + k, GROUP)}, device_id_type=MESH)
    pl.semaphore_wait(barrier, GROUP - 1)

    def e_copy(k):
        to = lax.rem(me + k, GROUP)
        return pltpu.make_async_remote_copy(src_ref=ye_ref.at[to, pl.ds(0, cap), :], dst_ref=land_e.at[me], send_sem=e_send.at[k], recv_sem=e_recv.at[k],
                                            device_id={"ep": to}, device_id_type=MESH)

    def b_copy(j, k):
        to = lax.rem(me + k, GROUP)
        return pltpu.make_async_remote_copy(src_ref=yb.at[j, pl.ds(pl.multiple_of(to * BASE, BASE), BASE), :],
                                            dst_ref=land_b.at[me, pl.ds(pl.multiple_of(j * BASE, BASE), BASE), :],
                                            send_sem=b_send.at[j, k], recv_sem=b_recv.at[j, k],
                                            device_id={"ep": to}, device_id_type=MESH)

    for k in range(1, GROUP):
        e_copy(k).start()
    land_e[me] = ye_ref[me, :cap, :]

    def expert(j, carry):
        x = xb_ref[j]
        for f in range(NCH):
            up_copy(j, f).wait()
            for p in range(FCH // 256):
                cols = pl.ds(f * FCH + p * 256, 256)
                up = dot(x, w1[j, :, cols])
                lin = dot(x, b3[f, :, p * 256:(p + 1) * 256])
                mid[:, cols] = (jax.nn.silu(up) * lin).astype(BF16)

            @pl.when(j + 1 < LOCAL)
            def _():
                up_copy(j + 1, f).start()
        for f in range(NCH):
            down_copy(j, f).wait()
            yb[j, :, f * DCH:(f + 1) * DCH] = dot(mid[...], b2[f]).astype(BF16)

            @pl.when(j + 1 < LOCAL)
            def _():
                down_copy(j + 1, f).start()
        land_b[me, pl.ds(pl.multiple_of(j * BASE, BASE), BASE), :] = yb[j, pl.ds(pl.multiple_of(me * BASE, BASE), BASE), :]
        for k in range(1, GROUP):
            b_copy(j, k).start()
        return carry

    lax.fori_loop(0, LOCAL, expert, 0)

    def columns(field, rows):
        place = tab_ref[:, field:field + 1]
        col = jnp.where(place < 0.0, -1.0, tab_ref[:, field // 4 * 4:field // 4 * 4 + 1] * rows + place).astype(I32)
        return (col == lax.broadcasted_iota(I32, (TOK, GROUP * rows), 1)).astype(F32).astype(BF16)

    for k in range(1, GROUP):
        e_copy(k).wait()
    far = land_e[...].reshape(GROUP * cap, WIDTH)
    mix0[...] = dot(columns(2, cap), far)
    mix1[...] = dot(columns(6, cap), far)
    for j in range(LOCAL):
        for k in range(1, GROUP):
            b_copy(j, k).wait()
    near = land_b[...].reshape(GROUP * LOCAL * BASE, WIDTH)
    y0 = mix0[...] + dot(columns(1, LOCAL * BASE), near)
    y1 = mix1[...] + dot(columns(5, LOCAL * BASE), near)
    mixed = tab_ref[:, 3:4] * y0 + tab_ref[:, 7:8] * y1
    out_ref[...] = (scale[0] * h_ref[...].astype(F32) + scale[1] * mixed).astype(BF16)


def base(index, cap, scale, tab, hidden, xb, ye, w1, w3, w2):
    vmem = pl.BlockSpec(memory_space=pltpu.VMEM)
    hbm = pl.BlockSpec(memory_space=pl.ANY)
    dma = pltpu.SemaphoreType.DMA
    return pl.pallas_call(
        functools.partial(base_kernel, cap),
        name=f"base_rows_{cap}",
        out_shape=jax.ShapeDtypeStruct((TOK, WIDTH), BF16),
        in_specs=[pl.BlockSpec(memory_space=pltpu.SMEM)] + [vmem] * 5 + [hbm] * 2,
        out_specs=vmem,
        scratch_shapes=[
            pltpu.VMEM((GROUP, cap, WIDTH), BF16),
            pltpu.VMEM((GROUP, LOCAL * BASE, WIDTH), BF16),
            pltpu.VMEM((LOCAL, BROWS, WIDTH), BF16),
            pltpu.VMEM((BROWS, FFN), BF16),
            pltpu.VMEM((RING, WIDTH, FCH), BF16),
            pltpu.VMEM((RING, FFN, DCH), BF16),
            pltpu.VMEM((TOK, WIDTH), F32),
            pltpu.VMEM((TOK, WIDTH), F32),
            dma((RING,)), dma((RING,)),
            dma((GROUP,)), dma((GROUP,)), dma((LOCAL, GROUP)), dma((LOCAL, GROUP)),
        ],
        compiler_params=pltpu.CompilerParams(collective_id=2 + index, has_side_effects=True, vmem_limit_bytes=BASE_VMEM * 2**20),
    )(scale, tab, hidden, xb, ye, w1, w3, w2)


def solution(mesh):
    def local_step(hidden, router_w, expert_ids, w_gate, w_up, w_down, post_scale):
        xb, xe, cnt, tab, top = gather(expert_ids.T, hidden, router_w.T)
        ye = extra(cnt, xe, w_gate, w_up, w_down)
        branches = [functools.partial(base, i, cap) for i, cap in enumerate(BUCKETS)]
        return lax.switch(top[0, 0], branches, post_scale, tab, hidden, xb, ye, w_gate, w_up, w_down)

    tok_spec = P(("dp", "ep"))
    return jax.shard_map(local_step, mesh=mesh, in_specs=(tok_spec, P(), tok_spec, P("ep"), P("ep"), P("ep"), P()), out_specs=tok_spec, check_vma=False)
```

```python
import functools

import jax
import jax.numpy as jnp
from jax import lax
from jax.experimental import pallas as pl
from jax.experimental.pallas import tpu as pltpu
from jax.sharding import PartitionSpec as P

MESH = pl.DeviceIdType.MESH
BF16, F32, I32 = jnp.bfloat16, jnp.float32, jnp.int32
GROUP = 8
LOCAL = 4
EXPERTS = GROUP * LOCAL
TOK = 256
SLOTS = 64
WIDTH = 1536
FFN = 2304
CHUNKS = 4
BASE = 16
EXTRA = SLOTS - BASE
BROWS = GROUP * BASE
BUCKETS = tuple(EXTRA * (i + 1) for i in range(LOCAL))
FCH = 768
NCH = FFN // FCH
DCH = 512
RING = 3
XROWS = GROUP * EXTRA + 128
GATHER_VMEM = 15
EXPERT_VMEM = 24
BASE_VMEM = 27


def dot(a, b):
    return jnp.dot(a, b, preferred_element_type=F32)


def dot_t(a, b):
    return lax.dot_general(a, b, (((1,), (1,)), ((), ())), preferred_element_type=F32)


def extra_rows(count):
    over = jnp.maximum(count - BASE, 0.0)
    return jnp.floor((over + 15.0) * (1.0 / 16.0)) * 16.0


def gather_kernel(ids_hbm, h_hbm, wr_hbm, xb_ref, xe_ref, cnt_ref, tab_ref, top_ref,
                  ids_ref, h_ref, wr_ref, in_sem, hall, rk, idbuf, needs, id_send, id_recv, x_send, y_send, p_send, x_recv, y_recv, d_recv, p_recv, own_sem):
    dp, me = lax.axis_index("dp"), lax.axis_index("ep")
    core, xc, yc = lax.rem(me, 2), lax.rem(me // 2, 2), me // 4
    xn, yn, pc = me + 2 - 4 * xc, me + 4 - 8 * yc, me + 1 - 2 * core
    dg = xn + 4 - 8 * yc
    rows = TOK // CHUNKS
    inputs = [pltpu.make_async_copy(src, dst, in_sem.at[i]) for i, (src, dst) in enumerate([(ids_hbm, ids_ref), (h_hbm, h_ref), (wr_hbm, wr_ref)])]
    for copy in inputs:
        copy.start()

    barrier = pltpu.get_barrier_semaphore()
    for k in range(1, GROUP):
        pl.semaphore_signal(barrier, inc=1, device_id={"ep": lax.rem(me + k, GROUP)}, device_id_type=MESH)
    pl.semaphore_signal(barrier, inc=1, device_id={"dp": 1 - dp, "ep": me}, device_id_type=MESH)
    pl.semaphore_wait(barrier, GROUP)

    def piece(block, q):
        return hall.at[block, pl.ds(q * rows, rows), :]

    def mine(q):
        return h_ref.at[pl.ds(q * rows, rows), :]

    def remote(src, dst, send, recv, dev):
        return pltpu.make_async_remote_copy(src_ref=src, dst_ref=dst, send_sem=send, recv_sem=recv,
                                            device_id={"ep": dev}, device_id_type=MESH)

    half = CHUNKS // 2
    sends = []

    def start(copy):
        copy.start()
        sends.append(copy)

    def send_x(q):
        start(remote(mine(q), piece(me, q), x_send.at[q], x_recv.at[q], xn))

    def send_y(q):
        start(remote(mine(q), piece(me, q), y_send.at[q], y_recv.at[q], yn))

    inputs[0].wait()
    id_copies = []
    for k in range(1, GROUP):
        id_copies.append(remote(ids_ref, idbuf.at[me], id_send.at[k], id_recv.at[k], lax.rem(me + k, GROUP)))
        id_copies[-1].start()
    inputs[1].wait()
    for i in range(CHUNKS):
        send_x(i)
        send_y((i + half) % CHUNKS)
    start(remote(h_ref, hall.at[me], p_send.at[3 * CHUNKS], p_recv.at[3 * CHUNKS], pc))
    own_ids = pltpu.make_async_copy(ids_ref, idbuf.at[me], own_sem.at[0])
    own_ids.start()

    upper = (lax.broadcasted_iota(I32, (TOK, TOK), 0) < lax.broadcasted_iota(I32, (TOK, TOK), 1)).astype(BF16)
    hb = h_ref[...]
    inputs[2].wait()
    wr = wr_ref[...]
    w_hi = wr.astype(BF16)
    rest = wr - w_hi.astype(F32)
    w_mid = rest.astype(BF16)
    w_lo = (rest - w_mid.astype(F32)).astype(BF16)
    logits = dot_t(w_hi, hb) + (dot_t(w_mid, hb) + dot_t(w_lo, hb))
    prob = jnp.exp(logits - jnp.max(logits, axis=0, keepdims=True))
    prob = prob / jnp.sum(prob, axis=0, keepdims=True)
    e_iota = lax.broadcasted_iota(I32, (EXPERTS, TOK), 0)
    id0, id1 = ids_ref[0:1, :], ids_ref[1:2, :]
    hit0, hit1 = e_iota == id0, e_iota == id1
    pick0 = jnp.sum(jnp.where(hit0, prob, 0.0), axis=0, keepdims=True)
    pick1 = jnp.sum(jnp.where(hit1, prob, 0.0), axis=0, keepdims=True)
    both = pick0 + pick1
    hits = jnp.where(hit0 | hit1, 1.0, 0.0)
    rank = dot(hits.astype(BF16), upper)
    er, ec = lax.broadcasted_iota(I32, (EXPERTS, EXPERTS), 0), lax.broadcasted_iota(I32, (EXPERTS, EXPERTS), 1)
    before = ((er // LOCAL == ec // LOCAL) & (ec < er)).astype(BF16)
    extra = extra_rows(jnp.sum(hits, axis=1, keepdims=True))
    start_e = dot(before, jnp.broadcast_to(extra, (EXPERTS, 128)).astype(BF16))[:, 0:1]
    local = (lax.broadcasted_iota(I32, (EXPERTS, 1), 0) % LOCAL).astype(F32)
    place_b = jnp.where(rank < BASE, local * BASE + rank, -1.0)
    place_e = jnp.where(rank < BASE, -1.0, start_e + rank - BASE)

    def at(hit, place):
        return jnp.sum(jnp.where(hit, place, 0.0), axis=0, keepdims=True)

    own0, own1 = (id0 // LOCAL).astype(F32), (id1 // LOCAL).astype(F32)
    fields = jnp.concatenate([own0, at(hit0, place_b), at(hit0, place_e), pick0 / both,
                              own1, at(hit1, place_b), at(hit1, place_e), pick1 / both, jnp.zeros((120, TOK), F32)], axis=0)
    tab_ref[...] = fields.T

    own_ids.wait()
    for copy in id_copies:
        copy.wait()
    j_iota = lax.broadcasted_iota(I32, (8, TOK), 0)
    local_id = jnp.where(j_iota < LOCAL, me * LOCAL + j_iota, -1)
    hit_list = []
    for s in range(GROUP):
        pair = idbuf[s]
        hit_list.append((local_id == pair[0:1, :]) | (local_id == pair[1:2, :]))
    hit_f = jnp.where(jnp.concatenate(hit_list, axis=0), 1.0, 0.0)
    hit_b = hit_f.astype(BF16)
    rk[...] = jnp.where(hit_f > 0.5, dot(hit_b, upper), -1.0).astype(I32).reshape(GROUP, 8, TOK)
    cnt_ref[...] = dot_t(jnp.ones((8, TOK), BF16), hit_b).astype(I32)
    lane = lax.broadcasted_iota(I32, (EXPERTS, 128), 1)
    spread = jnp.zeros((EXPERTS, 128), F32)
    for g in range(GROUP):
        pair = idbuf[g]
        n = jnp.where((e_iota == pair[0:1, :]) | (e_iota == pair[1:2, :]), 1.0, 0.0)
        spread = jnp.where(lane == g, extra_rows(jnp.sum(n, axis=1, keepdims=True)), spread)
    groups = (lax.broadcasted_iota(I32, (GROUP, EXPERTS), 0) == lax.broadcasted_iota(I32, (GROUP, EXPERTS), 1) // LOCAL).astype(BF16)
    need = dot(groups, spread.astype(BF16))
    need = jnp.max(jnp.max(need, axis=1, keepdims=True), axis=0, keepdims=True)
    needs[0] = jnp.broadcast_to(need, (8, 128))

    def arrived(block, q, sem):
        remote(piece(block, q), piece(block, q), x_send.at[0], sem, xn).wait_recv()

    for i in range(half):
        a, b = i, i + half
        arrived(xn, a, x_recv.at[a])
        start(remote(piece(xn, a), piece(xn, a), y_send.at[CHUNKS + i], d_recv.at[a], yn))
        start(remote(piece(xn, a), piece(xn, a), p_send.at[a], p_recv.at[a], pc))
        arrived(yn, b, y_recv.at[b])
        start(remote(piece(yn, b), piece(yn, b), x_send.at[CHUNKS + i], d_recv.at[b], xn))
        start(remote(piece(yn, b), piece(yn, b), p_send.at[CHUNKS + b], p_recv.at[CHUNKS + b], pc))
    other = pltpu.make_async_remote_copy(src_ref=needs.at[0], dst_ref=needs.at[1], send_sem=id_send.at[0], recv_sem=id_recv.at[0],
                                         device_id={"dp": 1 - dp, "ep": me}, device_id_type=MESH)
    other.start()

    b_iota = lax.broadcasted_iota(I32, (BASE, TOK), 0)
    x_iota = lax.broadcasted_iota(I32, (EXTRA, TOK), 0) + BASE

    def pick(s, block):
        ranks = rk[s]
        table = jnp.concatenate([(b_iota == ranks[j:j + 1, :]).astype(F32) for j in range(LOCAL)]
                                + [(x_iota == ranks[j:j + 1, :]).astype(F32) for j in range(LOCAL)], axis=0).astype(BF16)
        rows = dot(table, block).astype(BF16)
        for j in range(LOCAL):
            xb_ref[j, pl.ds(pl.multiple_of(s * BASE, BASE), BASE), :] = rows[j * BASE:(j + 1) * BASE]
        xe_ref[s] = rows[LOCAL * BASE:]

    pick(me, hb)
    remote(hall.at[pc], hall.at[pc], x_send.at[0], p_recv.at[3 * CHUNKS], pc).wait_recv()
    pick(pc, hall[pc])
    for i in range(half):
        a, b = i + half, i
        arrived(xn, a, x_recv.at[a])
        start(remote(piece(xn, a), piece(xn, a), p_send.at[a], p_recv.at[a], pc))
        arrived(yn, b, y_recv.at[b])
        start(remote(piece(yn, b), piece(yn, b), p_send.at[CHUNKS + b], p_recv.at[CHUNKS + b], pc))
    for i in range(half):
        for q in (i, i + half):
            arrived(dg, q, d_recv.at[q])
            start(remote(piece(dg, q), piece(dg, q), p_send.at[2 * CHUNKS + q], p_recv.at[2 * CHUNKS + q], pc))
        if i == 0:
            pick(xn, hall[xn])
            pick(yn, hall[yn])
    turn = 1 - 2 * core
    for q in range(CHUNKS):
        arrived(xn + turn, q, p_recv.at[q])
        arrived(yn + turn, q, p_recv.at[CHUNKS + q])
    pick(xn + turn, hall[xn + turn])
    pick(yn + turn, hall[yn + turn])
    pick(dg, hall[dg])
    for q in range(CHUNKS):
        arrived(dg + turn, q, p_recv.at[2 * CHUNKS + q])
    pick(dg + turn, hall[dg + turn])
    other.wait()
    both_need = jnp.maximum(needs[0], needs[1])
    top_ref[...] = sum((both_need > cap).astype(I32) for cap in BUCKETS[:-1])
    for copy in sends:
        copy.wait_send()


def gather(ids_t, hidden, wr_t):
    vmem = pl.BlockSpec(memory_space=pltpu.VMEM)
    dma = pltpu.SemaphoreType.DMA
    return pl.pallas_call(
        gather_kernel,
        name="gather_rows",
        out_shape=[
            jax.ShapeDtypeStruct((LOCAL, BROWS, WIDTH), BF16),
            jax.ShapeDtypeStruct((GROUP, LOCAL * EXTRA, WIDTH), BF16),
            jax.ShapeDtypeStruct((8, GROUP * 8), I32),
            jax.ShapeDtypeStruct((TOK, 128), F32),
            jax.ShapeDtypeStruct((8, 128), I32),
        ],
        in_specs=[pl.BlockSpec(memory_space=pltpu.HBM)] * 3,
        out_specs=[vmem] * 5,
        scratch_shapes=[
            pltpu.VMEM((2, TOK), I32),
            pltpu.VMEM((TOK, WIDTH), BF16),
            pltpu.VMEM((EXPERTS, WIDTH), F32),
            dma((3,)),
            pltpu.VMEM((GROUP, TOK, WIDTH), BF16),
            pltpu.VMEM((GROUP, 8, TOK), I32),
            pltpu.VMEM((GROUP, 2, TOK), I32),
            pltpu.VMEM((2, 8, 128), F32),
            dma((GROUP,)), dma((GROUP,)),
            dma((2 * CHUNKS,)), dma((2 * CHUNKS,)), dma((3 * CHUNKS + 1,)),
            dma((CHUNKS,)), dma((CHUNKS,)), dma((CHUNKS,)), dma((3 * CHUNKS + 1,)),
            dma((1,)),
        ],
        compiler_params=pltpu.CompilerParams(collective_id=1, has_side_effects=True, vmem_limit_bytes=GATHER_VMEM * 2**20),
        cost_estimate=pl.CostEstimate(flops=20 * 10**9, bytes_accessed=20 * 10**6, transcendentals=0),
    )(ids_t, hidden, wr_t)


def extra_kernel(cnt, xe_ref, w1, w3, w2, ye_ref, xbuf, mid, b3, b2, offs, act, tot, w3_sem, w2_sem):
    def tiles(s, j):
        return (jnp.maximum(cnt[0, s * 8 + j] - BASE, 0) + 15) // 16 * 16

    active = jnp.int32(0)
    for j in range(LOCAL):
        at = jnp.int32(0)
        for s in range(GROUP):
            offs[s, j] = at
            at = at + tiles(s, j)
        tot[j] = at
        act[active] = j
        active = active + (at > 0).astype(I32)
    chunks = active * NCH

    def up_copy(g):
        slot = lax.rem(g, RING)
        cols = pl.ds(pl.multiple_of(lax.rem(g, NCH) * FCH, FCH), FCH)
        return pltpu.make_async_copy(w3.at[act[g // NCH], :, cols], b3.at[slot], w3_sem.at[slot])

    def down_copy(g):
        slot = lax.rem(g, RING)
        cols = pl.ds(pl.multiple_of(lax.rem(g, NCH) * DCH, DCH), DCH)
        return pltpu.make_async_copy(w2.at[act[g // NCH], :, cols], b2.at[slot], w2_sem.at[slot])

    def fetch(copy, g):
        @pl.when(g < chunks)
        def _():
            copy(g).start()

    for g in range(RING):
        fetch(up_copy, g)
    for g in range(RING):
        fetch(down_copy, g)

    def compact(s, carry):
        for j in range(LOCAL):
            @pl.when(tot[j] > 0)
            def _():
                xbuf[j, pl.ds(pl.multiple_of(offs[s, j], 16), EXTRA), :] = xe_ref[s, j * EXTRA:(j + 1) * EXTRA, :]
        return carry

    lax.fori_loop(0, GROUP, compact, 0)
    ye_ref[...] = jnp.zeros_like(ye_ref)

    def expert(a, carry):
        j = act[a]
        total = tot[j]
        blocks = (total + 127) // 128
        xbuf[j, pl.ds(pl.multiple_of(total, 16), 128), :] = jnp.zeros((128, WIDTH), BF16)

        def over_rows(body):
            for n in range(1, 4):
                @pl.when(blocks == n)
                def _():
                    body(n * 128)

        def up_step(f, c):
            g = a * NCH + f
            slot = lax.rem(g, RING)
            up_copy(g).wait()

            def body(n):
                x = xbuf[j, :n, :]
                for p in range(FCH // 256):
                    cols = pl.ds(pl.multiple_of(f * FCH + p * 256, 256), 256)
                    up = dot(x, w1[j, :, cols])
                    lin = dot(x, b3[slot, :, p * 256:(p + 1) * 256])
                    mid[:n, cols] = (jax.nn.silu(up) * lin).astype(BF16)

            over_rows(body)
            fetch(up_copy, g + RING)
            return c

        def down_step(f, c):
            g = a * NCH + f
            slot = lax.rem(g, RING)
            down_copy(g).wait()

            def body(n):
                cols = pl.ds(pl.multiple_of(f * DCH, DCH), DCH)
                xbuf[j, :n, cols] = dot(mid[:n, :], b2[slot]).astype(BF16)

            over_rows(body)
            fetch(down_copy, g + RING)
            return c

        lax.fori_loop(0, NCH, up_step, 0)
        lax.fori_loop(0, NCH, down_step, 0)
        return carry

    lax.fori_loop(0, active, expert, 0)

    def pack(s, carry):
        at = jnp.int32(0)
        for j in range(LOCAL):
            n = tiles(s, j)

            @pl.when(n > 0)
            def _():
                ye_ref[s, pl.ds(pl.multiple_of(at, 16), EXTRA), :] = xbuf[j, pl.ds(pl.multiple_of(offs[s, j], 16), EXTRA), :]
            at = at + n
        return carry

    lax.fori_loop(0, GROUP, pack, 0)


def extra(cnt, xe, w1, w3, w2):
    hbm = pl.BlockSpec(memory_space=pl.ANY)
    vmem = pl.BlockSpec(memory_space=pltpu.VMEM)
    dma = pltpu.SemaphoreType.DMA
    return pl.pallas_call(
        extra_kernel,
        name="extra_rows",
        out_shape=jax.ShapeDtypeStruct((GROUP, LOCAL * EXTRA, WIDTH), BF16),
        in_specs=[pl.BlockSpec(memory_space=pltpu.SMEM), vmem, vmem, hbm, hbm],
        out_specs=vmem,
        input_output_aliases={1: 0},
        scratch_shapes=[
            pltpu.VMEM((LOCAL, XROWS, WIDTH), BF16),
            pltpu.VMEM((GROUP * EXTRA, FFN), BF16),
            pltpu.VMEM((RING, WIDTH, FCH), BF16),
            pltpu.VMEM((RING, FFN, DCH), BF16),
            pltpu.SMEM((GROUP, LOCAL), I32),
            pltpu.SMEM((LOCAL + 1,), I32),
            pltpu.SMEM((LOCAL,), I32),
            dma((RING,)), dma((RING,)),
        ],
        compiler_params=pltpu.CompilerParams(vmem_limit_bytes=EXPERT_VMEM * 2**20),
        cost_estimate=pl.CostEstimate(flops=8 * 10**9, bytes_accessed=30 * 10**6, transcendentals=0),
    )(cnt, xe, w1, w3, w2)


def base_kernel(cap, scale, tab_ref, h_ref, xb_ref, ye_ref, w1, w3, w2, out_ref,
                land_e, land_b, yb, mid, b3, b2, mix0, mix1, w3_sem, w2_sem, e_send, e_recv, b_send, b_recv):
    me = lax.axis_index("ep")

    def up_copy(j, f):
        return pltpu.make_async_copy(w3.at[j, :, pl.ds(f * FCH, FCH)], b3.at[f], w3_sem.at[f])

    def down_copy(j, f):
        return pltpu.make_async_copy(w2.at[j, :, pl.ds(f * DCH, DCH)], b2.at[f], w2_sem.at[f])

    for f in range(NCH):
        up_copy(0, f).start()
    for f in range(NCH):
        down_copy(0, f).start()

    barrier = pltpu.get_barrier_semaphore()
    for k in range(1, GROUP):
        pl.semaphore_signal(barrier, inc=1, device_id={"ep": lax.rem(me + k, GROUP)}, device_id_type=MESH)
    pl.semaphore_wait(barrier, GROUP - 1)

    def e_copy(k):
        to = lax.rem(me + k, GROUP)
        return pltpu.make_async_remote_copy(src_ref=ye_ref.at[to, pl.ds(0, cap), :], dst_ref=land_e.at[me], send_sem=e_send.at[k], recv_sem=e_recv.at[k],
                                            device_id={"ep": to}, device_id_type=MESH)

    def b_copy(j, k):
        to = lax.rem(me + k, GROUP)
        return pltpu.make_async_remote_copy(src_ref=yb.at[j, pl.ds(pl.multiple_of(to * BASE, BASE), BASE), :],
                                            dst_ref=land_b.at[me, pl.ds(pl.multiple_of(j * BASE, BASE), BASE), :],
                                            send_sem=b_send.at[j, k], recv_sem=b_recv.at[j, k],
                                            device_id={"ep": to}, device_id_type=MESH)

    for k in range(1, GROUP):
        e_copy(k).start()
    land_e[me] = ye_ref[me, :cap, :]

    def expert(j, carry):
        x = xb_ref[j]
        for f in range(NCH):
            up_copy(j, f).wait()
            for p in range(FCH // 256):
                cols = pl.ds(f * FCH + p * 256, 256)
                up = dot(x, w1[j, :, cols])
                lin = dot(x, b3[f, :, p * 256:(p + 1) * 256])
                mid[:, cols] = (jax.nn.silu(up) * lin).astype(BF16)

            @pl.when(j + 1 < LOCAL)
            def _():
                up_copy(j + 1, f).start()
        for f in range(NCH):
            down_copy(j, f).wait()
            yb[j, :, f * DCH:(f + 1) * DCH] = dot(mid[...], b2[f]).astype(BF16)

            @pl.when(j + 1 < LOCAL)
            def _():
                down_copy(j + 1, f).start()
        land_b[me, pl.ds(pl.multiple_of(j * BASE, BASE), BASE), :] = yb[j, pl.ds(pl.multiple_of(me * BASE, BASE), BASE), :]
        for k in range(1, GROUP):
            b_copy(j, k).start()
        return carry

    lax.fori_loop(0, LOCAL, expert, 0)

    def table(field, start, size):
        place = tab_ref[:, field:field + 1]
        inside = (place >= start) & (place < start + size)
        col = jnp.where(inside, tab_ref[:, field // 4 * 4:field // 4 * 4 + 1] * size + place - start, -1.0).astype(I32)
        return (col == lax.broadcasted_iota(I32, (TOK, GROUP * size), 1)).astype(F32).astype(BF16)

    for k in range(1, GROUP):
        e_copy(k).wait()
    far = land_e[...].reshape(GROUP * cap, WIDTH)
    mix0[...] = dot(table(2, 0, cap), far)
    mix1[...] = dot(table(6, 0, cap), far)
    early = (LOCAL - 1) * BASE
    for first, size in ((0, early), (early, BASE)):
        for j in range(first // BASE, (first + size) // BASE):
            for k in range(1, GROUP):
                b_copy(j, k).wait()
        near = land_b[:, first:first + size, :].reshape(GROUP * size, WIDTH)
        y0 = mix0[...] + dot(table(1, first, size), near)
        y1 = mix1[...] + dot(table(5, first, size), near)
        if first == 0:
            mix0[...] = y0
            mix1[...] = y1
    mixed = tab_ref[:, 3:4] * y0 + tab_ref[:, 7:8] * y1
    out_ref[...] = (scale[0] * h_ref[...].astype(F32) + scale[1] * mixed).astype(BF16)


def base(index, cap, scale, tab, hidden, xb, ye, w1, w3, w2):
    vmem = pl.BlockSpec(memory_space=pltpu.VMEM)
    hbm = pl.BlockSpec(memory_space=pl.ANY)
    dma = pltpu.SemaphoreType.DMA
    return pl.pallas_call(
        functools.partial(base_kernel, cap),
        name=f"base_rows_{cap}",
        out_shape=jax.ShapeDtypeStruct((TOK, WIDTH), BF16),
        in_specs=[pl.BlockSpec(memory_space=pltpu.SMEM)] + [vmem] * 5 + [hbm] * 2,
        out_specs=vmem,
        scratch_shapes=[
            pltpu.VMEM((GROUP, cap, WIDTH), BF16),
            pltpu.VMEM((GROUP, LOCAL * BASE, WIDTH), BF16),
            pltpu.VMEM((LOCAL, BROWS, WIDTH), BF16),
            pltpu.VMEM((BROWS, FFN), BF16),
            pltpu.VMEM((RING, WIDTH, FCH), BF16),
            pltpu.VMEM((RING, FFN, DCH), BF16),
            pltpu.VMEM((TOK, WIDTH), F32),
            pltpu.VMEM((TOK, WIDTH), F32),
            dma((RING,)), dma((RING,)),
            dma((GROUP,)), dma((GROUP,)), dma((LOCAL, GROUP)), dma((LOCAL, GROUP)),
        ],
        compiler_params=pltpu.CompilerParams(collective_id=2 + index, has_side_effects=True, vmem_limit_bytes=BASE_VMEM * 2**20),
    )(scale, tab, hidden, xb, ye, w1, w3, w2)


def solution(mesh):
    def local_step(hidden, router_w, expert_ids, w_gate, w_up, w_down, post_scale):
        xb, xe, cnt, tab, top = gather(expert_ids.T, hidden, router_w.T)
        ye = extra(cnt, xe, w_gate, w_up, w_down)
        branches = [functools.partial(base, i, cap) for i, cap in enumerate(BUCKETS)]
        return lax.switch(top[0, 0], branches, post_scale, tab, hidden, xb, ye, w_gate, w_up, w_down)

    tok_spec = P(("dp", "ep"))
    return jax.shard_map(local_step, mesh=mesh, in_specs=(tok_spec, P(), tok_spec, P("ep"), P("ep"), P("ep"), P()), out_specs=tok_spec, check_vma=False)
```

```python
import functools

import jax
import jax.numpy as jnp
from jax import lax
from jax.experimental import pallas as pl
from jax.experimental.pallas import tpu as pltpu
from jax.sharding import PartitionSpec as P

MESH = pl.DeviceIdType.MESH
BF16, F32, I32 = jnp.bfloat16, jnp.float32, jnp.int32
GROUP = 8
LOCAL = 4
EXPERTS = GROUP * LOCAL
TOK = 256
SLOTS = 64
WIDTH = 1536
FFN = 2304
CHUNKS = 4
BASE = 16
EXTRA = SLOTS - BASE
BROWS = GROUP * BASE
BUCKETS = tuple(EXTRA * (i + 1) for i in range(LOCAL))
FCH = 768
NCH = FFN // FCH
DCH = 512
RING = 3
XROWS = GROUP * EXTRA + 128
FIELDS = 5
GATHER_VMEM = 15
EXPERT_VMEM = 24
BASE_VMEM = 27


def dot(a, b):
    return jnp.dot(a, b, preferred_element_type=F32)


def dot_t(a, b):
    return lax.dot_general(a, b, (((1,), (1,)), ((), ())), preferred_element_type=F32)


def extra_rows(count):
    over = jnp.maximum(count - BASE, 0.0)
    return jnp.floor((over + 15.0) * (1.0 / 16.0)) * 16.0


def gather_kernel(ids_hbm, h_hbm, xb_ref, xe_ref, cnt_ref, tab_ref, top_ref,
                  ids_ref, h_ref, in_sem, hall, rk, idbuf, needs, id_send, id_recv, x_send, y_send, p_send, x_recv, y_recv, d_recv, p_recv, own_sem):
    dp, me = lax.axis_index("dp"), lax.axis_index("ep")
    core, xc, yc = lax.rem(me, 2), lax.rem(me // 2, 2), me // 4
    xn, yn, pc = me + 2 - 4 * xc, me + 4 - 8 * yc, me + 1 - 2 * core
    dg = xn + 4 - 8 * yc
    rows = TOK // CHUNKS
    inputs = [pltpu.make_async_copy(src, dst, in_sem.at[i]) for i, (src, dst) in enumerate([(ids_hbm, ids_ref), (h_hbm, h_ref)])]
    for copy in inputs:
        copy.start()

    barrier = pltpu.get_barrier_semaphore()
    for k in range(1, GROUP):
        pl.semaphore_signal(barrier, inc=1, device_id={"ep": lax.rem(me + k, GROUP)}, device_id_type=MESH)
    pl.semaphore_signal(barrier, inc=1, device_id={"dp": 1 - dp, "ep": me}, device_id_type=MESH)
    pl.semaphore_wait(barrier, GROUP)

    def piece(block, q):
        return hall.at[block, pl.ds(q * rows, rows), :]

    def mine(q):
        return h_ref.at[pl.ds(q * rows, rows), :]

    def remote(src, dst, send, recv, dev):
        return pltpu.make_async_remote_copy(src_ref=src, dst_ref=dst, send_sem=send, recv_sem=recv,
                                            device_id={"ep": dev}, device_id_type=MESH)

    half = CHUNKS // 2
    sends = []

    def start(copy):
        copy.start()
        sends.append(copy)

    def send_x(q):
        start(remote(mine(q), piece(me, q), x_send.at[q], x_recv.at[q], xn))

    def send_y(q):
        start(remote(mine(q), piece(me, q), y_send.at[q], y_recv.at[q], yn))

    inputs[0].wait()
    id_copies = []
    for k in range(1, GROUP):
        id_copies.append(remote(ids_ref, idbuf.at[me], id_send.at[k], id_recv.at[k], lax.rem(me + k, GROUP)))
        id_copies[-1].start()
    inputs[1].wait()
    for i in range(CHUNKS):
        send_x(i)
        send_y((i + half) % CHUNKS)
    start(remote(h_ref, hall.at[me], p_send.at[3 * CHUNKS], p_recv.at[3 * CHUNKS], pc))
    own_ids = pltpu.make_async_copy(ids_ref, idbuf.at[me], own_sem.at[0])
    own_ids.start()

    upper = (lax.broadcasted_iota(I32, (TOK, TOK), 0) < lax.broadcasted_iota(I32, (TOK, TOK), 1)).astype(BF16)
    hb = h_ref[...]
    e_iota = lax.broadcasted_iota(I32, (EXPERTS, TOK), 0)
    id0, id1 = ids_ref[0:1, :], ids_ref[1:2, :]
    hit0, hit1 = e_iota == id0, e_iota == id1
    hits = jnp.where(hit0 | hit1, 1.0, 0.0)
    rank = dot(hits.astype(BF16), upper)
    er, ec = lax.broadcasted_iota(I32, (EXPERTS, EXPERTS), 0), lax.broadcasted_iota(I32, (EXPERTS, EXPERTS), 1)
    before = ((er // LOCAL == ec // LOCAL) & (ec < er)).astype(BF16)
    extra = extra_rows(jnp.sum(hits, axis=1, keepdims=True))
    wide = jnp.broadcast_to(extra, (EXPERTS, 128)).astype(BF16)
    start_e = dot(before, wide)[:, 0:1]
    partner = (er // (2 * LOCAL) == ec // (2 * LOCAL)) & (er // LOCAL != ec // LOCAL)
    partner_rows = dot(partner.astype(BF16), wide)[:, 0:1]
    owner = lax.broadcasted_iota(I32, (EXPERTS, 1), 0) // LOCAL
    local = (lax.broadcasted_iota(I32, (EXPERTS, 1), 0) % LOCAL).astype(F32)
    place_b = jnp.where(rank < BASE, local * BASE + rank, -1.0)
    place_e = jnp.where(rank < BASE, -1.0, start_e + rank - BASE)
    moved = place_e >= EXTRA
    place_p = jnp.where(moved, jnp.minimum(partner_rows, EXTRA) + place_e - EXTRA, place_e)
    own_p = jnp.where(moved, owner + 1 - 2 * (owner % 2), owner).astype(F32)
    rows_of = []
    for hit in (hit0, hit1):
        rows_of += [jnp.sum(jnp.where(hit, v, 0.0), axis=0, keepdims=True) for v in (owner.astype(F32), place_b, place_e, own_p, place_p)]
    tab_ref[...] = jnp.concatenate(rows_of + [jnp.zeros((128 - len(rows_of), TOK), F32)], axis=0).T

    own_ids.wait()
    for copy in id_copies:
        copy.wait()
    j_iota = lax.broadcasted_iota(I32, (8, TOK), 0)
    local_id = jnp.where(j_iota < LOCAL, me * LOCAL + j_iota, (pc - 1) * LOCAL + j_iota)
    hit_list = []
    for s in range(GROUP):
        pair = idbuf[s]
        hit_list.append((local_id == pair[0:1, :]) | (local_id == pair[1:2, :]))
    hit_f = jnp.where(jnp.concatenate(hit_list, axis=0), 1.0, 0.0)
    hit_b = hit_f.astype(BF16)
    rk[...] = jnp.where(hit_f > 0.5, dot(hit_b, upper), -1.0).astype(I32).reshape(GROUP, 8, TOK)
    cnt_ref[...] = dot_t(jnp.ones((8, TOK), BF16), hit_b).astype(I32)
    lane = lax.broadcasted_iota(I32, (EXPERTS, 128), 1)
    spread = jnp.zeros((EXPERTS, 128), F32)
    for g in range(GROUP):
        pair = idbuf[g]
        n = jnp.where((e_iota == pair[0:1, :]) | (e_iota == pair[1:2, :]), 1.0, 0.0)
        spread = jnp.where(lane == g, extra_rows(jnp.sum(n, axis=1, keepdims=True)), spread)
    d_iota, o_iota = lax.broadcasted_iota(I32, (GROUP, EXPERTS), 0), lax.broadcasted_iota(I32, (GROUP, EXPERTS), 1) // LOCAL
    spread = spread.astype(BF16)
    need = dot((d_iota == o_iota).astype(BF16), spread)
    near = dot((d_iota + 1 - 2 * (d_iota % 2) == o_iota).astype(BF16), spread)
    pooled = jnp.maximum(need - EXTRA, 0.0) + jnp.minimum(near, EXTRA)
    needs[0, 0] = jnp.broadcast_to(jnp.max(jnp.max(need, axis=1, keepdims=True), axis=0, keepdims=True), (8, 128))
    needs[0, 1] = jnp.broadcast_to(jnp.max(jnp.max(pooled, axis=1, keepdims=True), axis=0, keepdims=True), (8, 128))

    def arrived(block, q, sem):
        remote(piece(block, q), piece(block, q), x_send.at[0], sem, xn).wait_recv()

    for i in range(half):
        a, b = i, i + half
        arrived(xn, a, x_recv.at[a])
        start(remote(piece(xn, a), piece(xn, a), y_send.at[CHUNKS + i], d_recv.at[a], yn))
        start(remote(piece(xn, a), piece(xn, a), p_send.at[a], p_recv.at[a], pc))
        arrived(yn, b, y_recv.at[b])
        start(remote(piece(yn, b), piece(yn, b), x_send.at[CHUNKS + i], d_recv.at[b], xn))
        start(remote(piece(yn, b), piece(yn, b), p_send.at[CHUNKS + b], p_recv.at[CHUNKS + b], pc))
    other = pltpu.make_async_remote_copy(src_ref=needs.at[0], dst_ref=needs.at[1], send_sem=id_send.at[0], recv_sem=id_recv.at[0],
                                         device_id={"dp": 1 - dp, "ep": me}, device_id_type=MESH)
    other.start()

    b_iota = lax.broadcasted_iota(I32, (BASE, TOK), 0)
    x_iota = lax.broadcasted_iota(I32, (EXTRA, TOK), 0) + BASE

    def pick(s, block):
        ranks = rk[s]
        table = jnp.concatenate([(b_iota == ranks[j:j + 1, :]).astype(F32) for j in range(LOCAL)]
                                + [(x_iota == ranks[j:j + 1, :]).astype(F32) for j in range(LOCAL)], axis=0).astype(BF16)
        rows = dot(table, block).astype(BF16)
        for j in range(LOCAL):
            xb_ref[j, pl.ds(pl.multiple_of(s * BASE, BASE), BASE), :] = rows[j * BASE:(j + 1) * BASE]
        xe_ref[s] = rows[LOCAL * BASE:]

    pick(me, hb)
    remote(hall.at[pc], hall.at[pc], x_send.at[0], p_recv.at[3 * CHUNKS], pc).wait_recv()
    pick(pc, hall[pc])
    for i in range(half):
        a, b = i + half, i
        arrived(xn, a, x_recv.at[a])
        start(remote(piece(xn, a), piece(xn, a), p_send.at[a], p_recv.at[a], pc))
        arrived(yn, b, y_recv.at[b])
        start(remote(piece(yn, b), piece(yn, b), p_send.at[CHUNKS + b], p_recv.at[CHUNKS + b], pc))
    for i in range(half):
        for q in (i, i + half):
            arrived(dg, q, d_recv.at[q])
            start(remote(piece(dg, q), piece(dg, q), p_send.at[2 * CHUNKS + q], p_recv.at[2 * CHUNKS + q], pc))
        if i == 0:
            pick(xn, hall[xn])
            pick(yn, hall[yn])
    turn = 1 - 2 * core
    for q in range(CHUNKS):
        arrived(xn + turn, q, p_recv.at[q])
        arrived(yn + turn, q, p_recv.at[CHUNKS + q])
    pick(xn + turn, hall[xn + turn])
    pick(yn + turn, hall[yn + turn])
    pick(dg, hall[dg])
    for q in range(CHUNKS):
        arrived(dg + turn, q, p_recv.at[2 * CHUNKS + q])
    pick(dg + turn, hall[dg + turn])
    other.wait()
    need, pooled = jnp.maximum(needs[0, 0], needs[1, 0]), jnp.maximum(needs[0, 1], needs[1, 1])
    rest = sum((need > cap).astype(I32) for cap in BUCKETS[1:-1]) + 2
    top_ref[...] = jnp.where(need <= EXTRA, 0, jnp.where((pooled <= EXTRA) & (need <= 2 * EXTRA), 1, rest))
    for copy in sends:
        copy.wait_send()


def gather(ids_t, hidden):
    vmem = pl.BlockSpec(memory_space=pltpu.VMEM)
    dma = pltpu.SemaphoreType.DMA
    return pl.pallas_call(
        gather_kernel,
        name="gather_rows",
        out_shape=[
            jax.ShapeDtypeStruct((LOCAL, BROWS, WIDTH), BF16),
            jax.ShapeDtypeStruct((GROUP, LOCAL * EXTRA, WIDTH), BF16),
            jax.ShapeDtypeStruct((8, GROUP * 8), I32),
            jax.ShapeDtypeStruct((TOK, 128), F32),
            jax.ShapeDtypeStruct((8, 128), I32),
        ],
        in_specs=[pl.BlockSpec(memory_space=pltpu.HBM)] * 2,
        out_specs=[vmem] * 5,
        scratch_shapes=[
            pltpu.VMEM((2, TOK), I32),
            pltpu.VMEM((TOK, WIDTH), BF16),
            dma((2,)),
            pltpu.VMEM((GROUP, TOK, WIDTH), BF16),
            pltpu.VMEM((GROUP, 8, TOK), I32),
            pltpu.VMEM((GROUP, 2, TOK), I32),
            pltpu.VMEM((2, 2, 8, 128), F32),
            dma((GROUP,)), dma((GROUP,)),
            dma((2 * CHUNKS,)), dma((2 * CHUNKS,)), dma((3 * CHUNKS + 1,)),
            dma((CHUNKS,)), dma((CHUNKS,)), dma((CHUNKS,)), dma((3 * CHUNKS + 1,)),
            dma((1,)),
        ],
        compiler_params=pltpu.CompilerParams(collective_id=1, has_side_effects=True, vmem_limit_bytes=GATHER_VMEM * 2**20),
        cost_estimate=pl.CostEstimate(flops=20 * 10**9, bytes_accessed=20 * 10**6, transcendentals=0),
    )(ids_t, hidden)


def extra_kernel(cnt, xe_ref, w1, w3, w2, ye_ref, ov_ref, xbuf, mid, b3, b2, offs, act, tot, w3_sem, w2_sem):
    def tiles(s, j):
        return (jnp.maximum(cnt[0, s * 8 + j] - BASE, 0) + 15) // 16 * 16

    active = jnp.int32(0)
    for j in range(LOCAL):
        at = jnp.int32(0)
        for s in range(GROUP):
            offs[s, j] = at
            at = at + tiles(s, j)
        tot[j] = at
        act[active] = j
        active = active + (at > 0).astype(I32)
    chunks = active * NCH

    def up_copy(g):
        slot = lax.rem(g, RING)
        cols = pl.ds(pl.multiple_of(lax.rem(g, NCH) * FCH, FCH), FCH)
        return pltpu.make_async_copy(w3.at[act[g // NCH], :, cols], b3.at[slot], w3_sem.at[slot])

    def down_copy(g):
        slot = lax.rem(g, RING)
        cols = pl.ds(pl.multiple_of(lax.rem(g, NCH) * DCH, DCH), DCH)
        return pltpu.make_async_copy(w2.at[act[g // NCH], :, cols], b2.at[slot], w2_sem.at[slot])

    def fetch(copy, g):
        @pl.when(g < chunks)
        def _():
            copy(g).start()

    for g in range(RING):
        fetch(up_copy, g)
    for g in range(RING):
        fetch(down_copy, g)

    def compact(s, carry):
        for j in range(LOCAL):
            @pl.when(tot[j] > 0)
            def _():
                xbuf[j, pl.ds(pl.multiple_of(offs[s, j], 16), EXTRA), :] = xe_ref[s, j * EXTRA:(j + 1) * EXTRA, :]
        return carry

    lax.fori_loop(0, GROUP, compact, 0)
    ye_ref[...] = jnp.zeros_like(ye_ref)
    ov_ref[...] = jnp.zeros_like(ov_ref)

    def expert(a, carry):
        j = act[a]
        total = tot[j]
        blocks = (total + 127) // 128
        xbuf[j, pl.ds(pl.multiple_of(total, 16), 128), :] = jnp.zeros((128, WIDTH), BF16)

        def over_rows(body):
            for n in range(1, 4):
                @pl.when(blocks == n)
                def _():
                    body(n * 128)

        def up_step(f, c):
            g = a * NCH + f
            slot = lax.rem(g, RING)
            up_copy(g).wait()

            def body(n):
                x = xbuf[j, :n, :]
                for p in range(FCH // 256):
                    cols = pl.ds(pl.multiple_of(f * FCH + p * 256, 256), 256)
                    up = dot(x, w1[j, :, cols])
                    lin = dot(x, b3[slot, :, p * 256:(p + 1) * 256])
                    mid[:n, cols] = (jax.nn.silu(up) * lin).astype(BF16)

            over_rows(body)
            fetch(up_copy, g + RING)
            return c

        def down_step(f, c):
            g = a * NCH + f
            slot = lax.rem(g, RING)
            down_copy(g).wait()

            def body(n):
                cols = pl.ds(pl.multiple_of(f * DCH, DCH), DCH)
                xbuf[j, :n, cols] = dot(mid[:n, :], b2[slot]).astype(BF16)

            over_rows(body)
            fetch(down_copy, g + RING)
            return c

        lax.fori_loop(0, NCH, up_step, 0)
        lax.fori_loop(0, NCH, down_step, 0)
        return carry

    lax.fori_loop(0, active, expert, 0)

    def pack(s, carry):
        at = jnp.int32(0)
        for j in range(LOCAL):
            n = tiles(s, j)

            @pl.when(n > 0)
            def _():
                ye_ref[s, pl.ds(pl.multiple_of(at, 16), EXTRA), :] = xbuf[j, pl.ds(pl.multiple_of(offs[s, j], 16), EXTRA), :]
            at = at + n

        @pl.when(at <= (LOCAL - 1) * EXTRA)
        def _():
            ye_ref[s, pl.ds(pl.multiple_of(at, 16), EXTRA), :] = jnp.zeros((EXTRA, WIDTH), BF16)

        behind = jnp.minimum(sum(tiles(s, LOCAL + j) for j in range(LOCAL)), EXTRA)
        for t in range(EXTRA // 16):
            @pl.when((at > EXTRA + 16 * t) & (behind + 16 * t < EXTRA))
            def _():
                ov_ref[s, pl.ds(pl.multiple_of(behind + 16 * t, 16), 16), :] = ye_ref[s, EXTRA + 16 * t:EXTRA + 16 * (t + 1), :]
        return carry

    lax.fori_loop(0, GROUP, pack, 0)


def extra(cnt, xe, w1, w3, w2):
    hbm = pl.BlockSpec(memory_space=pl.ANY)
    vmem = pl.BlockSpec(memory_space=pltpu.VMEM)
    dma = pltpu.SemaphoreType.DMA
    return pl.pallas_call(
        extra_kernel,
        name="extra_rows",
        out_shape=[jax.ShapeDtypeStruct((GROUP, LOCAL * EXTRA, WIDTH), BF16), jax.ShapeDtypeStruct((GROUP, EXTRA, WIDTH), BF16)],
        in_specs=[pl.BlockSpec(memory_space=pltpu.SMEM), vmem, vmem, hbm, hbm],
        out_specs=[vmem] * 2,
        input_output_aliases={1: 0},
        scratch_shapes=[
            pltpu.VMEM((LOCAL, XROWS, WIDTH), BF16),
            pltpu.VMEM((GROUP * EXTRA, FFN), BF16),
            pltpu.VMEM((RING, WIDTH, FCH), BF16),
            pltpu.VMEM((RING, FFN, DCH), BF16),
            pltpu.SMEM((GROUP, LOCAL), I32),
            pltpu.SMEM((LOCAL + 1,), I32),
            pltpu.SMEM((LOCAL,), I32),
            dma((RING,)), dma((RING,)),
        ],
        compiler_params=pltpu.CompilerParams(vmem_limit_bytes=EXPERT_VMEM * 2**20),
        cost_estimate=pl.CostEstimate(flops=8 * 10**9, bytes_accessed=30 * 10**6, transcendentals=0),
    )(cnt, xe, w1, w3, w2)


def base_kernel(cap, pooled, scale, ids_ref, wr_ref, tab_ref, h_ref, xb_ref, ye_ref, ov_ref, w1, w3, w2, out_ref,
                land_e, land_b, yb, mid, b3, b2, mix0, mix1, pool, w3_sem, w2_sem, e_send, e_recv, b_send, b_recv):
    me = lax.axis_index("ep")

    def up_copy(j, f):
        return pltpu.make_async_copy(w3.at[j, :, pl.ds(pl.multiple_of(f * FCH, FCH), FCH)], b3.at[f], w3_sem.at[f])

    def down_copy(j, f):
        return pltpu.make_async_copy(w2.at[j, :, pl.ds(pl.multiple_of(f * DCH, DCH), DCH)], b2.at[f], w2_sem.at[f])

    for f in range(NCH):
        up_copy(0, f).start()
    for f in range(NCH):
        down_copy(0, f).start()

    barrier = pltpu.get_barrier_semaphore()
    for k in range(1, GROUP):
        pl.semaphore_signal(barrier, inc=1, device_id={"ep": lax.rem(me + k, GROUP)}, device_id_type=MESH)
    pl.semaphore_wait(barrier, GROUP - 1)

    if pooled:
        over = pltpu.make_async_remote_copy(src_ref=ov_ref, dst_ref=pool.at[0], send_sem=e_send.at[0], recv_sem=e_recv.at[0],
                                            device_id={"ep": me + 1 - 2 * lax.rem(me, 2)}, device_id_type=MESH)
        over.start()
        over.wait()
        pool[1] = ye_ref[:, :EXTRA, :] + pool[0]
        out_e = pool.at[1]
    else:
        out_e = ye_ref

    def e_copy(k):
        to = lax.rem(me + k, GROUP)
        return pltpu.make_async_remote_copy(src_ref=out_e.at[to, pl.ds(0, cap), :], dst_ref=land_e.at[me], send_sem=e_send.at[k], recv_sem=e_recv.at[k],
                                            device_id={"ep": to}, device_id_type=MESH)

    def b_copy(j, k):
        to = lax.rem(me + k, GROUP)
        return pltpu.make_async_remote_copy(src_ref=yb.at[j, pl.ds(pl.multiple_of(to * BASE, BASE), BASE), :],
                                            dst_ref=land_b.at[me, pl.ds(pl.multiple_of(j * BASE, BASE), BASE), :],
                                            send_sem=b_send.at[j, k], recv_sem=b_recv.at[j, k],
                                            device_id={"ep": to}, device_id_type=MESH)

    for k in range(1, GROUP):
        e_copy(k).start()
    land_e[me] = out_e[me, :cap, :]

    def expert(j, carry):
        def up_step(f, c):
            up_copy(j, f).wait()
            x = xb_ref[j]
            for p in range(FCH // 256):
                cols = pl.ds(pl.multiple_of(f * FCH + p * 256, 256), 256)
                up = dot(x, w1[j, :, cols])
                lin = dot(x, b3[f, :, p * 256:(p + 1) * 256])
                mid[:, cols] = (jax.nn.silu(up) * lin).astype(BF16)

            @pl.when(j + 1 < LOCAL)
            def _():
                up_copy(j + 1, f).start()
            return c

        def down_step(f, c):
            down_copy(j, f).wait()
            yb[j, :, pl.ds(pl.multiple_of(f * DCH, DCH), DCH)] = dot(mid[...], b2[f]).astype(BF16)

            @pl.when(j + 1 < LOCAL)
            def _():
                down_copy(j + 1, f).start()
            return c

        lax.fori_loop(0, NCH, up_step, 0)
        lax.fori_loop(0, NCH, down_step, 0)
        land_b[me, pl.ds(pl.multiple_of(j * BASE, BASE), BASE), :] = yb[j, pl.ds(pl.multiple_of(me * BASE, BASE), BASE), :]
        for k in range(1, GROUP):
            b_copy(j, k).start()
        return carry

    lax.fori_loop(0, LOCAL, expert, 0)

    wr = wr_ref[...]
    hb = h_ref[...]
    w_hi = wr.astype(BF16)
    rest = wr - w_hi.astype(F32)
    w_mid = rest.astype(BF16)
    w_lo = (rest - w_mid.astype(F32)).astype(BF16)
    logits = dot_t(w_hi, hb) + (dot_t(w_mid, hb) + dot_t(w_lo, hb))
    prob = jnp.exp(logits - jnp.max(logits, axis=0, keepdims=True))
    prob = prob / jnp.sum(prob, axis=0, keepdims=True)
    e_iota = lax.broadcasted_iota(I32, (EXPERTS, TOK), 0)
    pick0 = jnp.sum(jnp.where(e_iota == ids_ref[0:1, :], prob, 0.0), axis=0, keepdims=True)
    pick1 = jnp.sum(jnp.where(e_iota == ids_ref[1:2, :], prob, 0.0), axis=0, keepdims=True)
    both = pick0 + pick1
    gates = jnp.concatenate([pick0 / both, pick1 / both, jnp.zeros((126, TOK), F32)], axis=0).T

    def table(own, field, start, size):
        place = tab_ref[:, field:field + 1]
        inside = (place >= start) & (place < start + size)
        col = jnp.where(inside, tab_ref[:, own:own + 1] * size + place - start, -1.0).astype(I32)
        return (col == lax.broadcasted_iota(I32, (TOK, GROUP * size), 1)).astype(F32).astype(BF16)

    for k in range(1, GROUP):
        e_copy(k).wait()
    far = land_e[...].reshape(GROUP * cap, WIDTH)
    own_at, pos_at = (3, 4) if pooled else (0, 2)
    mix0[...] = dot(table(own_at, pos_at, 0, cap), far)
    mix1[...] = dot(table(FIELDS + own_at, FIELDS + pos_at, 0, cap), far)
    early = (LOCAL - 1) * BASE
    for first, size in ((0, early), (early, BASE)):
        for j in range(first // BASE, (first + size) // BASE):
            for k in range(1, GROUP):
                b_copy(j, k).wait()
        near = land_b[:, first:first + size, :].reshape(GROUP * size, WIDTH)
        y0 = mix0[...] + dot(table(0, 1, first, size), near)
        y1 = mix1[...] + dot(table(FIELDS, FIELDS + 1, first, size), near)
        if first == 0:
            mix0[...] = y0
            mix1[...] = y1
    mixed = gates[:, 0:1] * y0 + gates[:, 1:2] * y1
    out_ref[...] = (scale[0] * h_ref[...].astype(F32) + scale[1] * mixed).astype(BF16)


def base(index, cap, pooled, scale, ids_t, wr_t, tab, hidden, xb, ye, ov, w1, w3, w2):
    vmem = pl.BlockSpec(memory_space=pltpu.VMEM)
    hbm = pl.BlockSpec(memory_space=pl.ANY)
    dma = pltpu.SemaphoreType.DMA
    return pl.pallas_call(
        functools.partial(base_kernel, cap, pooled),
        name=f"base_{cap}{'_pooled' if pooled else ''}",
        out_shape=jax.ShapeDtypeStruct((TOK, WIDTH), BF16),
        in_specs=[pl.BlockSpec(memory_space=pltpu.SMEM)] + [vmem] * 8 + [hbm] * 2,
        out_specs=vmem,
        scratch_shapes=[
            pltpu.VMEM((GROUP, cap, WIDTH), BF16),
            pltpu.VMEM((GROUP, LOCAL * BASE, WIDTH), BF16),
            pltpu.VMEM((LOCAL, BROWS, WIDTH), BF16),
            pltpu.VMEM((BROWS, FFN), BF16),
            pltpu.VMEM((RING, WIDTH, FCH), BF16),
            pltpu.VMEM((RING, FFN, DCH), BF16),
            pltpu.VMEM((TOK, WIDTH), F32),
            pltpu.VMEM((TOK, WIDTH), F32),
            pltpu.VMEM((2, GROUP, EXTRA if pooled else 16, WIDTH), BF16),
            dma((RING,)), dma((RING,)),
            dma((GROUP,)), dma((GROUP,)), dma((LOCAL, GROUP)), dma((LOCAL, GROUP)),
        ],
        compiler_params=pltpu.CompilerParams(collective_id=2 + index, has_side_effects=True, vmem_limit_bytes=BASE_VMEM * 2**20),
    )(scale, ids_t, wr_t, tab, hidden, xb, ye, ov, w1, w3, w2)


def solution(mesh):
    def local_step(hidden, router_w, expert_ids, w_gate, w_up, w_down, post_scale):
        ids_t, wr_t = expert_ids.T, router_w.T
        xb, xe, cnt, tab, top = gather(ids_t, hidden)
        ye, ov = extra(cnt, xe, w_gate, w_up, w_down)
        plans = [(EXTRA, False), (EXTRA, True)] + [(cap, False) for cap in BUCKETS[1:]]
        branches = [functools.partial(base, i, cap, pooled) for i, (cap, pooled) in enumerate(plans)]
        return lax.switch(top[0, 0], branches, post_scale, ids_t, wr_t, tab, hidden, xb, ye, ov, w_gate, w_up, w_down)

    tok_spec = P(("dp", "ep"))
    return jax.shard_map(local_step, mesh=mesh, in_specs=(tok_spec, P(), tok_spec, P("ep"), P("ep"), P("ep"), P()), out_specs=tok_spec, check_vma=False)
```

```python
import functools

import jax
import jax.numpy as jnp
from jax import lax
from jax.experimental import pallas as pl
from jax.experimental.pallas import tpu as pltpu
from jax.sharding import PartitionSpec as P

MESH = pl.DeviceIdType.MESH
BF16, F32, I32 = jnp.bfloat16, jnp.float32, jnp.int32
GROUP = 8
LOCAL = 4
EXPERTS = GROUP * LOCAL
TOK = 256
SLOTS = 64
WIDTH = 1536
FFN = 2304
CHUNKS = 4
BASE = 16
EXTRA = SLOTS - BASE
BROWS = GROUP * BASE
BUCKETS = tuple(EXTRA * (i + 1) for i in range(LOCAL))
FCH = 768
NCH = FFN // FCH
DCH = 512
RING = 3
XROWS = GROUP * EXTRA + 128
FIELDS = 5
GATHER_VMEM = 15
EXPERT_VMEM = 20
BASE_VMEM = 27


def dot(a, b):
    return jnp.dot(a, b, preferred_element_type=F32)


def dot_t(a, b):
    return lax.dot_general(a, b, (((1,), (1,)), ((), ())), preferred_element_type=F32)


def extra_rows(count):
    over = jnp.maximum(count - BASE, 0.0)
    return jnp.floor((over + 15.0) * (1.0 / 16.0)) * 16.0


def gather_kernel(ids_hbm, h_hbm, xb_ref, xe_ref, cnt_ref, tab_ref,
                  ids_ref, h_ref, in_sem, hall, rk, idbuf, needs, id_send, id_recv, x_send, y_send, p_send, x_recv, y_recv, d_recv, p_recv, own_sem):
    dp, me = lax.axis_index("dp"), lax.axis_index("ep")
    core, xc, yc = lax.rem(me, 2), lax.rem(me // 2, 2), me // 4
    xn, yn, pc = me + 2 - 4 * xc, me + 4 - 8 * yc, me + 1 - 2 * core
    dg = xn + 4 - 8 * yc
    rows = TOK // CHUNKS
    inputs = [pltpu.make_async_copy(src, dst, in_sem.at[i]) for i, (src, dst) in enumerate([(ids_hbm, ids_ref), (h_hbm, h_ref)])]
    for copy in inputs:
        copy.start()

    barrier = pltpu.get_barrier_semaphore()
    for k in range(1, GROUP):
        pl.semaphore_signal(barrier, inc=1, device_id={"ep": lax.rem(me + k, GROUP)}, device_id_type=MESH)
    pl.semaphore_signal(barrier, inc=1, device_id={"dp": 1 - dp, "ep": me}, device_id_type=MESH)
    pl.semaphore_wait(barrier, GROUP)

    def piece(block, q):
        return hall.at[block, pl.ds(q * rows, rows), :]

    def mine(q):
        return h_ref.at[pl.ds(q * rows, rows), :]

    def remote(src, dst, send, recv, dev):
        return pltpu.make_async_remote_copy(src_ref=src, dst_ref=dst, send_sem=send, recv_sem=recv,
                                            device_id={"ep": dev}, device_id_type=MESH)

    half = CHUNKS // 2
    sends = []

    def start(copy):
        copy.start()
        sends.append(copy)

    def send_x(q):
        start(remote(mine(q), piece(me, q), x_send.at[q], x_recv.at[q], xn))

    def send_y(q):
        start(remote(mine(q), piece(me, q), y_send.at[q], y_recv.at[q], yn))

    inputs[0].wait()
    id_copies = []
    for k in range(1, GROUP):
        id_copies.append(remote(ids_ref, idbuf.at[me], id_send.at[k], id_recv.at[k], lax.rem(me + k, GROUP)))
        id_copies[-1].start()
    inputs[1].wait()
    for i in range(CHUNKS):
        send_x(i)
        send_y((i + half) % CHUNKS)
    start(remote(h_ref, hall.at[me], p_send.at[3 * CHUNKS], p_recv.at[3 * CHUNKS], pc))
    own_ids = pltpu.make_async_copy(ids_ref, idbuf.at[me], own_sem.at[0])
    own_ids.start()

    upper = (lax.broadcasted_iota(I32, (TOK, TOK), 0) < lax.broadcasted_iota(I32, (TOK, TOK), 1)).astype(BF16)
    hb = h_ref[...]
    e_iota = lax.broadcasted_iota(I32, (EXPERTS, TOK), 0)
    id0, id1 = ids_ref[0:1, :], ids_ref[1:2, :]
    hit0, hit1 = e_iota == id0, e_iota == id1
    hits = jnp.where(hit0 | hit1, 1.0, 0.0)
    rank = dot(hits.astype(BF16), upper)
    er, ec = lax.broadcasted_iota(I32, (EXPERTS, EXPERTS), 0), lax.broadcasted_iota(I32, (EXPERTS, EXPERTS), 1)
    before = ((er // LOCAL == ec // LOCAL) & (ec < er)).astype(BF16)
    extra = extra_rows(jnp.sum(hits, axis=1, keepdims=True))
    wide = jnp.broadcast_to(extra, (EXPERTS, 128)).astype(BF16)
    start_e = dot(before, wide)[:, 0:1]
    partner = (er // (2 * LOCAL) == ec // (2 * LOCAL)) & (er // LOCAL != ec // LOCAL)
    partner_rows = dot(partner.astype(BF16), wide)[:, 0:1]
    owner = lax.broadcasted_iota(I32, (EXPERTS, 1), 0) // LOCAL
    local = (lax.broadcasted_iota(I32, (EXPERTS, 1), 0) % LOCAL).astype(F32)
    place_b = jnp.where(rank < BASE, local * BASE + rank, -1.0)
    place_e = jnp.where(rank < BASE, -1.0, start_e + rank - BASE)
    moved = place_e >= EXTRA
    place_p = jnp.where(moved, jnp.minimum(partner_rows, EXTRA) + place_e - EXTRA, place_e)
    own_p = jnp.where(moved, owner + 1 - 2 * (owner % 2), owner).astype(F32)
    rows_of = []
    for hit in (hit0, hit1):
        rows_of += [jnp.sum(jnp.where(hit, v, 0.0), axis=0, keepdims=True) for v in (owner.astype(F32), place_b, place_e, own_p, place_p)]
    tab_ref[...] = jnp.concatenate(rows_of + [jnp.zeros((128 - len(rows_of), TOK), F32)], axis=0).T

    own_ids.wait()
    for copy in id_copies:
        copy.wait()
    j_iota = lax.broadcasted_iota(I32, (8, TOK), 0)
    local_id = jnp.where(j_iota < LOCAL, me * LOCAL + j_iota, (pc - 1) * LOCAL + j_iota)
    hit_list = []
    for s in range(GROUP):
        pair = idbuf[s]
        hit_list.append((local_id == pair[0:1, :]) | (local_id == pair[1:2, :]))
    hit_f = jnp.where(jnp.concatenate(hit_list, axis=0), 1.0, 0.0)
    hit_b = hit_f.astype(BF16)
    rk[...] = jnp.where(hit_f > 0.5, dot(hit_b, upper), -1.0).astype(I32).reshape(GROUP, 8, TOK)
    cnt_ref[:, 0:GROUP * 8] = extra_rows(dot_t(jnp.ones((8, TOK), BF16), hit_b)).astype(I32)
    lane = lax.broadcasted_iota(I32, (EXPERTS, 128), 1)
    spread = jnp.zeros((EXPERTS, 128), F32)
    for g in range(GROUP):
        pair = idbuf[g]
        n = jnp.where((e_iota == pair[0:1, :]) | (e_iota == pair[1:2, :]), 1.0, 0.0)
        spread = jnp.where(lane == g, extra_rows(jnp.sum(n, axis=1, keepdims=True)), spread)
    d_iota, o_iota = lax.broadcasted_iota(I32, (GROUP, EXPERTS), 0), lax.broadcasted_iota(I32, (GROUP, EXPERTS), 1) // LOCAL
    spread = spread.astype(BF16)
    need = dot((d_iota == o_iota).astype(BF16), spread)
    near = dot((d_iota + 1 - 2 * (d_iota % 2) == o_iota).astype(BF16), spread)
    pooled = jnp.maximum(need - EXTRA, 0.0) + jnp.minimum(near, EXTRA)
    needs[0, 0] = jnp.broadcast_to(jnp.max(jnp.max(need, axis=1, keepdims=True), axis=0, keepdims=True), (8, 128))
    needs[0, 1] = jnp.broadcast_to(jnp.max(jnp.max(pooled, axis=1, keepdims=True), axis=0, keepdims=True), (8, 128))

    def arrived(block, q, sem):
        remote(piece(block, q), piece(block, q), x_send.at[0], sem, xn).wait_recv()

    for i in range(half):
        a, b = i, i + half
        arrived(xn, a, x_recv.at[a])
        start(remote(piece(xn, a), piece(xn, a), y_send.at[CHUNKS + i], d_recv.at[a], yn))
        start(remote(piece(xn, a), piece(xn, a), p_send.at[a], p_recv.at[a], pc))
        arrived(yn, b, y_recv.at[b])
        start(remote(piece(yn, b), piece(yn, b), x_send.at[CHUNKS + i], d_recv.at[b], xn))
        start(remote(piece(yn, b), piece(yn, b), p_send.at[CHUNKS + b], p_recv.at[CHUNKS + b], pc))
    other = pltpu.make_async_remote_copy(src_ref=needs.at[0], dst_ref=needs.at[1], send_sem=id_send.at[0], recv_sem=id_recv.at[0],
                                         device_id={"dp": 1 - dp, "ep": me}, device_id_type=MESH)
    other.start()

    b_iota = lax.broadcasted_iota(I32, (BASE, TOK), 0)
    x_iota = lax.broadcasted_iota(I32, (EXTRA, TOK), 0) + BASE

    def pick(s, block):
        ranks = rk[s]
        table = jnp.concatenate([(b_iota == ranks[j:j + 1, :]).astype(F32) for j in range(LOCAL)]
                                + [(x_iota == ranks[j:j + 1, :]).astype(F32) for j in range(LOCAL)], axis=0).astype(BF16)
        rows = dot(table, block).astype(BF16)
        for j in range(LOCAL):
            xb_ref[j, pl.ds(pl.multiple_of(s * BASE, BASE), BASE), :] = rows[j * BASE:(j + 1) * BASE]
        xe_ref[s] = rows[LOCAL * BASE:]

    pick(me, hb)
    remote(hall.at[pc], hall.at[pc], x_send.at[0], p_recv.at[3 * CHUNKS], pc).wait_recv()
    pick(pc, hall[pc])
    for i in range(half):
        a, b = i + half, i
        arrived(xn, a, x_recv.at[a])
        start(remote(piece(xn, a), piece(xn, a), p_send.at[a], p_recv.at[a], pc))
        arrived(yn, b, y_recv.at[b])
        start(remote(piece(yn, b), piece(yn, b), p_send.at[CHUNKS + b], p_recv.at[CHUNKS + b], pc))
    for i in range(half):
        for q in (i, i + half):
            arrived(dg, q, d_recv.at[q])
            start(remote(piece(dg, q), piece(dg, q), p_send.at[2 * CHUNKS + q], p_recv.at[2 * CHUNKS + q], pc))
        if i == 0:
            pick(xn, hall[xn])
            pick(yn, hall[yn])
    turn = 1 - 2 * core
    for q in range(CHUNKS):
        arrived(xn + turn, q, p_recv.at[q])
        arrived(yn + turn, q, p_recv.at[CHUNKS + q])
    pick(xn + turn, hall[xn + turn])
    pick(yn + turn, hall[yn + turn])
    pick(dg, hall[dg])
    for q in range(CHUNKS):
        arrived(dg + turn, q, p_recv.at[2 * CHUNKS + q])
    pick(dg + turn, hall[dg + turn])
    other.wait()
    need, pooled = jnp.maximum(needs[0, 0], needs[1, 0]), jnp.maximum(needs[0, 1], needs[1, 1])
    rest = sum((need > cap).astype(I32) for cap in BUCKETS[1:-1]) + 2
    index = jnp.where(need <= EXTRA, 0, jnp.where((pooled <= EXTRA) & (need <= 2 * EXTRA), 1, rest))
    cnt_ref[:, GROUP * 8:] = index[:, GROUP * 8:]
    for copy in sends:
        copy.wait_send()


def gather(ids_t, hidden):
    vmem = pl.BlockSpec(memory_space=pltpu.VMEM)
    dma = pltpu.SemaphoreType.DMA
    return pl.pallas_call(
        gather_kernel,
        name="gather_rows",
        out_shape=[
            jax.ShapeDtypeStruct((LOCAL, BROWS, WIDTH), BF16),
            jax.ShapeDtypeStruct((GROUP, LOCAL * EXTRA, WIDTH), BF16),
            jax.ShapeDtypeStruct((8, 128), I32),
            jax.ShapeDtypeStruct((TOK, 128), F32),
        ],
        in_specs=[pl.BlockSpec(memory_space=pltpu.HBM)] * 2,
        out_specs=[vmem] * 4,
        scratch_shapes=[
            pltpu.VMEM((2, TOK), I32),
            pltpu.VMEM((TOK, WIDTH), BF16),
            dma((2,)),
            pltpu.VMEM((GROUP, TOK, WIDTH), BF16),
            pltpu.VMEM((GROUP, 8, TOK), I32),
            pltpu.VMEM((GROUP, 2, TOK), I32),
            pltpu.VMEM((2, 2, 8, 128), F32),
            dma((GROUP,)), dma((GROUP,)),
            dma((2 * CHUNKS,)), dma((2 * CHUNKS,)), dma((3 * CHUNKS + 1,)),
            dma((CHUNKS,)), dma((CHUNKS,)), dma((CHUNKS,)), dma((3 * CHUNKS + 1,)),
            dma((1,)),
        ],
        compiler_params=pltpu.CompilerParams(collective_id=1, has_side_effects=True, vmem_limit_bytes=GATHER_VMEM * 2**20),
        cost_estimate=pl.CostEstimate(flops=20 * 10**9, bytes_accessed=20 * 10**6, transcendentals=0),
    )(ids_t, hidden)


def extra_kernel(cnt, xe_ref, w1, w3, w2, ye_ref, ov_ref, top_ref, xbuf, mid, b3, b2, act, pos, w3_sem, w2_sem):
    def tiles(s, j):
        return cnt[0, s * 8 + j]

    active = jnp.int32(0)
    for j in range(LOCAL):
        act[active] = j
        active = active + jnp.minimum(sum(tiles(s, j) for s in range(GROUP)), 1)
    chunks = active * NCH
    index = cnt[0, GROUP * 8]
    top_ref[0] = index

    def up_copy(g):
        slot = lax.rem(g, RING)
        cols = pl.ds(pl.multiple_of(lax.rem(g, NCH) * FCH, FCH), FCH)
        return pltpu.make_async_copy(w3.at[act[g // NCH], :, cols], b3.at[slot], w3_sem.at[slot])

    def down_copy(g):
        slot = lax.rem(g, RING)
        cols = pl.ds(pl.multiple_of(lax.rem(g, NCH) * DCH, DCH), DCH)
        return pltpu.make_async_copy(w2.at[act[g // NCH], :, cols], b2.at[slot], w2_sem.at[slot])

    def fetch(copy, g):
        @pl.when(g < chunks)
        def _():
            copy(g).start()

    for g in range(RING):
        fetch(up_copy, g)
    for g in range(RING):
        fetch(down_copy, g)

    ye_ref[:, :EXTRA, :] = jnp.zeros((GROUP, EXTRA, WIDTH), BF16)
    for s in range(GROUP):
        pos[s] = 0

    @pl.when(index == 1)
    def _():
        ov_ref[...] = jnp.zeros_like(ov_ref)

    @pl.when(index > 1)
    def _():
        ye_ref[:, EXTRA:, :] = jnp.zeros((GROUP, (LOCAL - 1) * EXTRA, WIDTH), BF16)

    def expert(a, carry):
        j = act[a]
        total = jnp.int32(0)
        for s in range(GROUP):
            xbuf[pl.ds(pl.multiple_of(total, 16), EXTRA), :] = xe_ref[s, pl.ds(pl.multiple_of(j * EXTRA, 16), EXTRA), :]
            total = total + tiles(s, j)
        blocks = (total + 127) // 128
        xbuf[pl.ds(pl.multiple_of(total, 16), 128), :] = jnp.zeros((128, WIDTH), BF16)

        def over_rows(body):
            for n in range(1, 4):
                @pl.when(blocks == n)
                def _():
                    body(n * 128)

        def up_step(f, c):
            g = a * NCH + f
            slot = lax.rem(g, RING)
            up_copy(g).wait()

            def body(n):
                x = xbuf[:n, :]
                for p in range(FCH // 256):
                    cols = pl.ds(pl.multiple_of(f * FCH + p * 256, 256), 256)
                    up = dot(x, w1[j, :, cols])
                    lin = dot(x, b3[slot, :, p * 256:(p + 1) * 256])
                    mid[:n, cols] = (jax.nn.silu(up) * lin).astype(BF16)

            over_rows(body)
            fetch(up_copy, g + RING)
            return c

        def down_step(f, c):
            g = a * NCH + f
            slot = lax.rem(g, RING)
            down_copy(g).wait()

            def body(n):
                cols = pl.ds(pl.multiple_of(f * DCH, DCH), DCH)
                xbuf[:n, cols] = dot(mid[:n, :], b2[slot]).astype(BF16)

            over_rows(body)
            fetch(down_copy, g + RING)
            return c

        lax.fori_loop(0, NCH, up_step, 0)
        lax.fori_loop(0, NCH, down_step, 0)
        at = jnp.int32(0)
        for s in range(GROUP):
            put = pos[s]
            ye_ref[s, pl.ds(pl.multiple_of(put, 16), EXTRA), :] = xbuf[pl.ds(pl.multiple_of(at, 16), EXTRA), :]
            at = at + tiles(s, j)
            pos[s] = put + tiles(s, j)
        return carry

    lax.fori_loop(0, active, expert, 0)

    @pl.when(index == 1)
    def _():
        def pool(s, carry):
            own = pos[s]

            @pl.when(own < EXTRA)
            def _():
                ye_ref[s, pl.ds(pl.multiple_of(own, 16), EXTRA), :] = jnp.zeros((EXTRA, WIDTH), BF16)

            behind = jnp.minimum(sum(tiles(s, LOCAL + j) for j in range(LOCAL)), EXTRA)
            for t in range(EXTRA // 16):
                @pl.when((own > EXTRA + 16 * t) & (behind + 16 * t < EXTRA))
                def _():
                    ov_ref[s, pl.ds(pl.multiple_of(behind + 16 * t, 16), 16), :] = ye_ref[s, EXTRA + 16 * t:EXTRA + 16 * (t + 1), :]
            return carry

        lax.fori_loop(0, GROUP, pool, 0)


def extra(cnt, xe, w1, w3, w2):
    hbm = pl.BlockSpec(memory_space=pl.ANY)
    vmem = pl.BlockSpec(memory_space=pltpu.VMEM)
    dma = pltpu.SemaphoreType.DMA
    return pl.pallas_call(
        extra_kernel,
        name="extra_rows",
        out_shape=[jax.ShapeDtypeStruct((GROUP, LOCAL * EXTRA, WIDTH), BF16), jax.ShapeDtypeStruct((GROUP, EXTRA, WIDTH), BF16),
                   jax.ShapeDtypeStruct((1,), I32)],
        in_specs=[pl.BlockSpec(memory_space=pltpu.SMEM), vmem, vmem, hbm, hbm],
        out_specs=[vmem] * 2 + [pl.BlockSpec(memory_space=pltpu.SMEM)],
        scratch_shapes=[
            pltpu.VMEM((XROWS, WIDTH), BF16),
            pltpu.VMEM((GROUP * EXTRA, FFN), BF16),
            pltpu.VMEM((RING, WIDTH, FCH), BF16),
            pltpu.VMEM((RING, FFN, DCH), BF16),
            pltpu.SMEM((LOCAL + 1,), I32),
            pltpu.SMEM((GROUP,), I32),
            dma((RING,)), dma((RING,)),
        ],
        compiler_params=pltpu.CompilerParams(vmem_limit_bytes=EXPERT_VMEM * 2**20),
        cost_estimate=pl.CostEstimate(flops=8 * 10**9, bytes_accessed=30 * 10**6, transcendentals=0),
    )(cnt, xe, w1, w3, w2)


def base_kernel(cap, pooled, scale, ids_ref, wr_ref, tab_ref, h_ref, xb_ref, ye_ref, ov_ref, w1, w3, w2, out_ref,
                land_e, land_b, yb, mid, b3, b2, mix, pool, w3_sem, w2_sem, e_send, e_recv, b_send, b_recv):
    me = lax.axis_index("ep")

    def up_copy(j, f):
        return pltpu.make_async_copy(w3.at[j, :, pl.ds(pl.multiple_of(f * FCH, FCH), FCH)], b3.at[f], w3_sem.at[f])

    def down_copy(j, f):
        return pltpu.make_async_copy(w2.at[j, :, pl.ds(pl.multiple_of(f * DCH, DCH), DCH)], b2.at[f], w2_sem.at[f])

    for f in range(NCH):
        up_copy(0, f).start()
    for f in range(NCH):
        down_copy(0, f).start()

    barrier = pltpu.get_barrier_semaphore()
    for k in range(1, GROUP):
        pl.semaphore_signal(barrier, inc=1, device_id={"ep": lax.rem(me + k, GROUP)}, device_id_type=MESH)
    pl.semaphore_wait(barrier, GROUP - 1)

    if pooled:
        over = pltpu.make_async_remote_copy(src_ref=ov_ref, dst_ref=pool.at[0], send_sem=e_send.at[0], recv_sem=e_recv.at[0],
                                            device_id={"ep": me + 1 - 2 * lax.rem(me, 2)}, device_id_type=MESH)
        over.start()
        over.wait()
        pool[1] = ye_ref[:, :EXTRA, :] + pool[0]
        out_e = pool.at[1]
    else:
        out_e = ye_ref

    def e_copy(k):
        to = lax.rem(me + k, GROUP)
        return pltpu.make_async_remote_copy(src_ref=out_e.at[to, pl.ds(0, cap), :], dst_ref=land_e.at[me], send_sem=e_send.at[k], recv_sem=e_recv.at[k],
                                            device_id={"ep": to}, device_id_type=MESH)

    def b_copy(j, k):
        to = lax.rem(me + k, GROUP)
        return pltpu.make_async_remote_copy(src_ref=yb.at[j, pl.ds(pl.multiple_of(to * BASE, BASE), BASE), :],
                                            dst_ref=land_b.at[me, pl.ds(pl.multiple_of(j * BASE, BASE), BASE), :],
                                            send_sem=b_send.at[j, k], recv_sem=b_recv.at[j, k],
                                            device_id={"ep": to}, device_id_type=MESH)

    for k in range(1, GROUP):
        e_copy(k).start()
    land_e[me] = out_e[me, :cap, :]

    def expert(j, carry):
        def up_step(f, c):
            up_copy(j, f).wait()
            x = xb_ref[j]
            for p in range(FCH // 256):
                cols = pl.ds(pl.multiple_of(f * FCH + p * 256, 256), 256)
                up = dot(x, w1[j, :, cols])
                lin = dot(x, b3[f, :, p * 256:(p + 1) * 256])
                mid[:, cols] = (jax.nn.silu(up) * lin).astype(BF16)

            @pl.when(j + 1 < LOCAL)
            def _():
                up_copy(j + 1, f).start()
            return c

        def down_step(f, c):
            down_copy(j, f).wait()
            yb[j, :, pl.ds(pl.multiple_of(f * DCH, DCH), DCH)] = dot(mid[...], b2[f]).astype(BF16)

            @pl.when(j + 1 < LOCAL)
            def _():
                down_copy(j + 1, f).start()
            return c

        lax.fori_loop(0, NCH, up_step, 0)
        lax.fori_loop(0, NCH, down_step, 0)
        land_b[me, pl.ds(pl.multiple_of(j * BASE, BASE), BASE), :] = yb[j, pl.ds(pl.multiple_of(me * BASE, BASE), BASE), :]
        for k in range(1, GROUP):
            b_copy(j, k).start()
        return carry

    lax.fori_loop(0, LOCAL, expert, 0)

    wr = wr_ref[...]
    hb = h_ref[...]
    w_hi = wr.astype(BF16)
    rest = wr - w_hi.astype(F32)
    w_mid = rest.astype(BF16)
    w_lo = (rest - w_mid.astype(F32)).astype(BF16)
    logits = dot_t(w_hi, hb) + (dot_t(w_mid, hb) + dot_t(w_lo, hb))
    prob = jnp.exp(logits - jnp.max(logits, axis=0, keepdims=True))
    prob = prob / jnp.sum(prob, axis=0, keepdims=True)
    e_iota = lax.broadcasted_iota(I32, (EXPERTS, TOK), 0)
    pick0 = jnp.sum(jnp.where(e_iota == ids_ref[0:1, :], prob, 0.0), axis=0, keepdims=True)
    pick1 = jnp.sum(jnp.where(e_iota == ids_ref[1:2, :], prob, 0.0), axis=0, keepdims=True)
    both = pick0 + pick1
    gates = jnp.concatenate([pick0 / both, pick1 / both, jnp.zeros((126, TOK), F32)], axis=0).T

    def table(own, field, start, size):
        place = tab_ref[:, field:field + 1]
        inside = (place >= start) & (place < start + size)
        col = jnp.where(inside, tab_ref[:, own:own + 1] * size + place - start, -1.0).astype(I32)
        return (col == lax.broadcasted_iota(I32, (TOK, GROUP * size), 1)).astype(F32).astype(BF16)

    own_at, pos_at = (3, 4) if pooled else (0, 2)
    early = (LOCAL - 1) * BASE
    gate0, gate1 = scale[1] * gates[:, 0:1], scale[1] * gates[:, 1:2]
    far0, far1 = table(own_at, pos_at, 0, cap), table(FIELDS + own_at, FIELDS + pos_at, 0, cap)
    near0, near1 = table(0, 1, 0, early), table(FIELDS, FIELDS + 1, 0, early)
    last0, last1 = table(0, 1, early, BASE), table(FIELDS, FIELDS + 1, early, BASE)
    for k in range(1, GROUP):
        e_copy(k).wait()
    far = land_e[...].reshape(GROUP * cap, WIDTH)
    mix[...] = scale[0] * h_ref[...].astype(F32) + (gate0 * dot(far0, far) + gate1 * dot(far1, far))
    for j in range(LOCAL - 1):
        for k in range(1, GROUP):
            b_copy(j, k).wait()
    near = land_b[:, :early, :].reshape(GROUP * early, WIDTH)
    mix[...] += gate0 * dot(near0, near) + gate1 * dot(near1, near)
    for k in range(1, GROUP):
        b_copy(LOCAL - 1, k).wait()
    last = land_b[:, early:, :].reshape(GROUP * BASE, WIDTH)
    out_ref[...] = (mix[...] + (gate0 * dot(last0, last) + gate1 * dot(last1, last))).astype(BF16)


def base(index, cap, pooled, scale, ids_t, wr_t, tab, hidden, xb, ye, ov, w1, w3, w2):
    vmem = pl.BlockSpec(memory_space=pltpu.VMEM)
    hbm = pl.BlockSpec(memory_space=pl.ANY)
    dma = pltpu.SemaphoreType.DMA
    return pl.pallas_call(
        functools.partial(base_kernel, cap, pooled),
        name=f"base_{cap}{'_pooled' if pooled else ''}",
        out_shape=jax.ShapeDtypeStruct((TOK, WIDTH), BF16),
        in_specs=[pl.BlockSpec(memory_space=pltpu.SMEM)] + [vmem] * 8 + [hbm] * 2,
        out_specs=vmem,
        scratch_shapes=[
            pltpu.VMEM((GROUP, cap, WIDTH), BF16),
            pltpu.VMEM((GROUP, LOCAL * BASE, WIDTH), BF16),
            pltpu.VMEM((LOCAL, BROWS, WIDTH), BF16),
            pltpu.VMEM((BROWS, FFN), BF16),
            pltpu.VMEM((RING, WIDTH, FCH), BF16),
            pltpu.VMEM((RING, FFN, DCH), BF16),
            pltpu.VMEM((TOK, WIDTH), F32),
            pltpu.VMEM((2, GROUP, EXTRA if pooled else 16, WIDTH), BF16),
            dma((RING,)), dma((RING,)),
            dma((GROUP,)), dma((GROUP,)), dma((LOCAL, GROUP)), dma((LOCAL, GROUP)),
        ],
        compiler_params=pltpu.CompilerParams(collective_id=2 + index, has_side_effects=True, vmem_limit_bytes=BASE_VMEM * 2**20),
    )(scale, ids_t, wr_t, tab, hidden, xb, ye, ov, w1, w3, w2)


def solution(mesh):
    def local_step(hidden, router_w, expert_ids, w_gate, w_up, w_down, post_scale):
        ids_t, wr_t = expert_ids.T, router_w.T
        xb, xe, cnt, tab = gather(ids_t, hidden)
        ye, ov, top = extra(cnt, xe, w_gate, w_up, w_down)
        plans = [(EXTRA, False), (EXTRA, True)] + [(cap, False) for cap in BUCKETS[1:]]
        branches = [functools.partial(base, i, cap, pooled) for i, (cap, pooled) in enumerate(plans)]
        return lax.switch(top[0], branches, post_scale, ids_t, wr_t, tab, hidden, xb, ye, ov, w_gate, w_up, w_down)

    tok_spec = P(("dp", "ep"))
    return jax.shard_map(local_step, mesh=mesh, in_specs=(tok_spec, P(), tok_spec, P("ep"), P("ep"), P("ep"), P()), out_specs=tok_spec, check_vma=False)
```

```python
import functools

import jax
import jax.numpy as jnp
from jax import lax
from jax.experimental import pallas as pl
from jax.experimental.pallas import tpu as pltpu
from jax.sharding import PartitionSpec as P

MESH = pl.DeviceIdType.MESH
BF16, F32, I32 = jnp.bfloat16, jnp.float32, jnp.int32
GROUP = 8
LOCAL = 4
EXPERTS = GROUP * LOCAL
TOK = 256
SLOTS = 64
WIDTH = 1536
FFN = 2304
CHUNKS = 4
BASE = 16
EXTRA = SLOTS - BASE
BROWS = GROUP * BASE
BUCKETS = tuple(EXTRA * (i + 1) for i in range(LOCAL))
FCH = 768
NCH = FFN // FCH
DCH = 512
RING = 3
XROWS = GROUP * EXTRA + 128
FIELDS = 5
GATHER_VMEM = 15
EXPERT_VMEM = 20
BASE_VMEM = 27


def dot(a, b):
    return jnp.dot(a, b, preferred_element_type=F32)


def dot_t(a, b):
    return lax.dot_general(a, b, (((1,), (1,)), ((), ())), preferred_element_type=F32)


def extra_rows(count):
    over = jnp.maximum(count - BASE, 0.0)
    return jnp.floor((over + 15.0) * (1.0 / 16.0)) * 16.0


def gather_kernel(ids_hbm, h_hbm, xb_ref, xe_ref, cnt_ref, tab_ref,
                  ids_ref, h_ref, in_sem, hall, rk, idbuf, needs, id_send, id_recv, x_send, y_send, p_send, x_recv, y_recv, d_recv, p_recv, own_sem):
    dp, me = lax.axis_index("dp"), lax.axis_index("ep")
    core, xc, yc = lax.rem(me, 2), lax.rem(me // 2, 2), me // 4
    xn, yn, pc = me + 2 - 4 * xc, me + 4 - 8 * yc, me + 1 - 2 * core
    dg = xn + 4 - 8 * yc
    rows = TOK // CHUNKS
    inputs = [pltpu.make_async_copy(src, dst, in_sem.at[i]) for i, (src, dst) in enumerate([(ids_hbm, ids_ref), (h_hbm, h_ref)])]
    for copy in inputs:
        copy.start()

    barrier = pltpu.get_barrier_semaphore()
    for k in range(1, GROUP):
        pl.semaphore_signal(barrier, inc=1, device_id={"ep": lax.rem(me + k, GROUP)}, device_id_type=MESH)
    pl.semaphore_signal(barrier, inc=1, device_id={"dp": 1 - dp, "ep": me}, device_id_type=MESH)
    pl.semaphore_wait(barrier, GROUP)

    def piece(block, q):
        return hall.at[block, pl.ds(q * rows, rows), :]

    def mine(q):
        return h_ref.at[pl.ds(q * rows, rows), :]

    def remote(src, dst, send, recv, dev):
        return pltpu.make_async_remote_copy(src_ref=src, dst_ref=dst, send_sem=send, recv_sem=recv,
                                            device_id={"ep": dev}, device_id_type=MESH)

    half = CHUNKS // 2
    sends = []

    def start(copy):
        copy.start()
        sends.append(copy)

    def send_x(q):
        start(remote(mine(q), piece(me, q), x_send.at[q], x_recv.at[q], xn))

    def send_y(q):
        start(remote(mine(q), piece(me, q), y_send.at[q], y_recv.at[q], yn))

    inputs[0].wait()
    id_copies = []
    for k in range(1, GROUP):
        id_copies.append(remote(ids_ref, idbuf.at[me], id_send.at[k], id_recv.at[k], lax.rem(me + k, GROUP)))
        id_copies[-1].start()
    inputs[1].wait()
    for i in range(CHUNKS):
        send_x(i)
        send_y((i + half) % CHUNKS)
    start(remote(h_ref, hall.at[me], p_send.at[3 * CHUNKS], p_recv.at[3 * CHUNKS], pc))
    own_ids = pltpu.make_async_copy(ids_ref, idbuf.at[me], own_sem.at[0])
    own_ids.start()

    upper = (lax.broadcasted_iota(I32, (TOK, TOK), 0) < lax.broadcasted_iota(I32, (TOK, TOK), 1)).astype(BF16)
    hb = h_ref[...]
    e_iota = lax.broadcasted_iota(I32, (EXPERTS, TOK), 0)
    id0, id1 = ids_ref[0:1, :], ids_ref[1:2, :]
    hit0, hit1 = e_iota == id0, e_iota == id1
    hits = jnp.where(hit0 | hit1, 1.0, 0.0)
    rank = dot(hits.astype(BF16), upper)
    er, ec = lax.broadcasted_iota(I32, (EXPERTS, EXPERTS), 0), lax.broadcasted_iota(I32, (EXPERTS, EXPERTS), 1)
    before = ((er // LOCAL == ec // LOCAL) & (ec < er)).astype(BF16)
    extra = extra_rows(jnp.sum(hits, axis=1, keepdims=True))
    wide = jnp.broadcast_to(extra, (EXPERTS, 128)).astype(BF16)
    start_e = dot(before, wide)[:, 0:1]
    partner = (er // (2 * LOCAL) == ec // (2 * LOCAL)) & (er // LOCAL != ec // LOCAL)
    partner_rows = dot(partner.astype(BF16), wide)[:, 0:1]
    owner = lax.broadcasted_iota(I32, (EXPERTS, 1), 0) // LOCAL
    local = (lax.broadcasted_iota(I32, (EXPERTS, 1), 0) % LOCAL).astype(F32)
    place_b = jnp.where(rank < BASE, local * BASE + rank, -1.0)
    place_e = jnp.where(rank < BASE, -1.0, start_e + rank - BASE)
    moved = place_e >= EXTRA
    place_p = jnp.where(moved, jnp.minimum(partner_rows, EXTRA) + place_e - EXTRA, place_e)
    own_p = jnp.where(moved, owner + 1 - 2 * (owner % 2), owner).astype(F32)
    rows_of = []
    for hit in (hit0, hit1):
        rows_of += [jnp.sum(jnp.where(hit, v, 0.0), axis=0, keepdims=True) for v in (owner.astype(F32), place_b, place_e, own_p, place_p)]
    tab_ref[...] = jnp.concatenate(rows_of + [jnp.zeros((128 - len(rows_of), TOK), F32)], axis=0).T

    own_ids.wait()
    for copy in id_copies:
        copy.wait()
    j_iota = lax.broadcasted_iota(I32, (8, TOK), 0)
    local_id = jnp.where(j_iota < LOCAL, me * LOCAL + j_iota, (pc - 1) * LOCAL + j_iota)
    hit_list = []
    for s in range(GROUP):
        pair = idbuf[s]
        hit_list.append((local_id == pair[0:1, :]) | (local_id == pair[1:2, :]))
    hit_f = jnp.where(jnp.concatenate(hit_list, axis=0), 1.0, 0.0)
    hit_b = hit_f.astype(BF16)
    rk[...] = jnp.where(hit_f > 0.5, dot(hit_b, upper), -1.0).astype(I32).reshape(GROUP, 8, TOK)
    cnt_ref[:, 0:GROUP * 8] = extra_rows(dot_t(jnp.ones((8, TOK), BF16), hit_b)).astype(I32)
    lane = lax.broadcasted_iota(I32, (EXPERTS, 128), 1)
    spread = jnp.zeros((EXPERTS, 128), F32)
    for g in range(GROUP):
        pair = idbuf[g]
        n = jnp.where((e_iota == pair[0:1, :]) | (e_iota == pair[1:2, :]), 1.0, 0.0)
        spread = jnp.where(lane == g, extra_rows(jnp.sum(n, axis=1, keepdims=True)), spread)
    d_iota, o_iota = lax.broadcasted_iota(I32, (GROUP, EXPERTS), 0), lax.broadcasted_iota(I32, (GROUP, EXPERTS), 1) // LOCAL
    spread = spread.astype(BF16)
    need = dot((d_iota == o_iota).astype(BF16), spread)
    near = dot((d_iota + 1 - 2 * (d_iota % 2) == o_iota).astype(BF16), spread)
    pooled = jnp.maximum(need - EXTRA, 0.0) + jnp.minimum(near, EXTRA)
    needs[0, 0] = jnp.broadcast_to(jnp.max(jnp.max(need, axis=1, keepdims=True), axis=0, keepdims=True), (8, 128))
    needs[0, 1] = jnp.broadcast_to(jnp.max(jnp.max(pooled, axis=1, keepdims=True), axis=0, keepdims=True), (8, 128))

    def arrived(block, q, sem):
        remote(piece(block, q), piece(block, q), x_send.at[0], sem, xn).wait_recv()

    for i in range(half):
        a, b = i, i + half
        arrived(xn, a, x_recv.at[a])
        start(remote(piece(xn, a), piece(xn, a), y_send.at[CHUNKS + i], d_recv.at[a], yn))
        start(remote(piece(xn, a), piece(xn, a), p_send.at[a], p_recv.at[a], pc))
        arrived(yn, b, y_recv.at[b])
        start(remote(piece(yn, b), piece(yn, b), x_send.at[CHUNKS + i], d_recv.at[b], xn))
        start(remote(piece(yn, b), piece(yn, b), p_send.at[CHUNKS + b], p_recv.at[CHUNKS + b], pc))
    other = pltpu.make_async_remote_copy(src_ref=needs.at[0], dst_ref=needs.at[1], send_sem=id_send.at[0], recv_sem=id_recv.at[0],
                                         device_id={"dp": 1 - dp, "ep": me}, device_id_type=MESH)
    other.start()

    b_iota = lax.broadcasted_iota(I32, (BASE, TOK), 0)
    x_iota = lax.broadcasted_iota(I32, (EXTRA, TOK), 0) + BASE

    def pick(s, block):
        ranks = rk[s]
        table = jnp.concatenate([(b_iota == ranks[j:j + 1, :]).astype(F32) for j in range(LOCAL)]
                                + [(x_iota == ranks[j:j + 1, :]).astype(F32) for j in range(LOCAL)], axis=0).astype(BF16)
        rows = dot(table, block).astype(BF16)
        for j in range(LOCAL):
            xb_ref[j, pl.ds(pl.multiple_of(s * BASE, BASE), BASE), :] = rows[j * BASE:(j + 1) * BASE]
        xe_ref[s] = rows[LOCAL * BASE:]

    pick(me, hb)
    remote(hall.at[pc], hall.at[pc], x_send.at[0], p_recv.at[3 * CHUNKS], pc).wait_recv()
    pick(pc, hall[pc])
    for i in range(half):
        a, b = i + half, i
        arrived(xn, a, x_recv.at[a])
        start(remote(piece(xn, a), piece(xn, a), p_send.at[a], p_recv.at[a], pc))
        arrived(yn, b, y_recv.at[b])
        start(remote(piece(yn, b), piece(yn, b), p_send.at[CHUNKS + b], p_recv.at[CHUNKS + b], pc))
    for i in range(half):
        for q in (i, i + half):
            arrived(dg, q, d_recv.at[q])
            start(remote(piece(dg, q), piece(dg, q), p_send.at[2 * CHUNKS + q], p_recv.at[2 * CHUNKS + q], pc))
        if i == 0:
            pick(xn, hall[xn])
            pick(yn, hall[yn])
    turn = 1 - 2 * core
    for q in range(CHUNKS):
        arrived(xn + turn, q, p_recv.at[q])
        arrived(yn + turn, q, p_recv.at[CHUNKS + q])
    pick(xn + turn, hall[xn + turn])
    pick(yn + turn, hall[yn + turn])
    pick(dg, hall[dg])
    for q in range(CHUNKS):
        arrived(dg + turn, q, p_recv.at[2 * CHUNKS + q])
    pick(dg + turn, hall[dg + turn])
    other.wait()
    need, pooled = jnp.maximum(needs[0, 0], needs[1, 0]), jnp.maximum(needs[0, 1], needs[1, 1])
    rest = sum((need > cap).astype(I32) for cap in BUCKETS[1:-1]) + 2
    index = jnp.where(need <= EXTRA, 0, jnp.where((pooled <= EXTRA) & (need <= 2 * EXTRA), 1, rest))
    cnt_ref[:, GROUP * 8:] = index[:, GROUP * 8:]
    for copy in sends:
        copy.wait_send()


def gather(ids_t, hidden):
    vmem = pl.BlockSpec(memory_space=pltpu.VMEM)
    dma = pltpu.SemaphoreType.DMA
    return pl.pallas_call(
        gather_kernel,
        name="gather_rows",
        out_shape=[
            jax.ShapeDtypeStruct((LOCAL, BROWS, WIDTH), BF16),
            jax.ShapeDtypeStruct((GROUP, LOCAL * EXTRA, WIDTH), BF16),
            jax.ShapeDtypeStruct((8, 128), I32),
            jax.ShapeDtypeStruct((TOK, 128), F32),
        ],
        in_specs=[pl.BlockSpec(memory_space=pltpu.HBM)] * 2,
        out_specs=[vmem] * 4,
        scratch_shapes=[
            pltpu.VMEM((2, TOK), I32),
            pltpu.VMEM((TOK, WIDTH), BF16),
            dma((2,)),
            pltpu.VMEM((GROUP, TOK, WIDTH), BF16),
            pltpu.VMEM((GROUP, 8, TOK), I32),
            pltpu.VMEM((GROUP, 2, TOK), I32),
            pltpu.VMEM((2, 2, 8, 128), F32),
            dma((GROUP,)), dma((GROUP,)),
            dma((2 * CHUNKS,)), dma((2 * CHUNKS,)), dma((3 * CHUNKS + 1,)),
            dma((CHUNKS,)), dma((CHUNKS,)), dma((CHUNKS,)), dma((3 * CHUNKS + 1,)),
            dma((1,)),
        ],
        compiler_params=pltpu.CompilerParams(collective_id=1, has_side_effects=True, vmem_limit_bytes=GATHER_VMEM * 2**20),
        cost_estimate=pl.CostEstimate(flops=20 * 10**9, bytes_accessed=20 * 10**6, transcendentals=0),
    )(ids_t, hidden)


def extra_kernel(cnt, xe_ref, w1, w3, w2, ye_ref, ov_ref, top_ref, xbuf, mid, b3, b2, act, pos, w3_sem, w2_sem):
    def tiles(s, j):
        return cnt[0, s * 8 + j]

    active = jnp.int32(0)
    for j in range(LOCAL):
        act[active] = j
        active = active + jnp.minimum(sum(tiles(s, j) for s in range(GROUP)), 1)
    chunks = active * NCH
    index = cnt[0, GROUP * 8]
    top_ref[0] = index

    def up_copy(g):
        slot = lax.rem(g, RING)
        cols = pl.ds(pl.multiple_of(lax.rem(g, NCH) * FCH, FCH), FCH)
        return pltpu.make_async_copy(w3.at[act[g // NCH], :, cols], b3.at[slot], w3_sem.at[slot])

    def down_copy(g):
        slot = lax.rem(g, RING)
        cols = pl.ds(pl.multiple_of(lax.rem(g, NCH) * DCH, DCH), DCH)
        return pltpu.make_async_copy(w2.at[act[g // NCH], :, cols], b2.at[slot], w2_sem.at[slot])

    def fetch(copy, g):
        @pl.when(g < chunks)
        def _():
            copy(g).start()

    for g in range(RING):
        fetch(up_copy, g)
    for g in range(RING):
        fetch(down_copy, g)

    ye_ref[:, :EXTRA, :] = jnp.zeros((GROUP, EXTRA, WIDTH), BF16)
    for s in range(GROUP):
        pos[s] = 0

    @pl.when(index == 1)
    def _():
        ov_ref[...] = jnp.zeros_like(ov_ref)

    @pl.when(index > 1)
    def _():
        ye_ref[:, EXTRA:, :] = jnp.zeros((GROUP, (LOCAL - 1) * EXTRA, WIDTH), BF16)

    def expert(a, carry):
        j = act[a]
        total = jnp.int32(0)
        for s in range(GROUP):
            xbuf[pl.ds(pl.multiple_of(total, 16), EXTRA), :] = xe_ref[s, pl.ds(pl.multiple_of(j * EXTRA, 16), EXTRA), :]
            total = total + tiles(s, j)
        xbuf[pl.ds(pl.multiple_of(total, 16), 128), :] = jnp.zeros((128, WIDTH), BF16)

        @pl.when((total > 128) & (total < GROUP * EXTRA - 128))
        def _():
            xbuf[pl.ds(pl.multiple_of(total + 128, 16), 128), :] = jnp.zeros((128, WIDTH), BF16)

        def over_rows(body):
            @pl.when(total <= 128)
            def _():
                body(128)

            @pl.when(total > 128)
            def _():
                body(GROUP * EXTRA)

        def up_step(f, c):
            g = a * NCH + f
            slot = lax.rem(g, RING)
            up_copy(g).wait()

            def body(n):
                x = xbuf[:n, :]
                for p in range(FCH // 256):
                    cols = pl.ds(pl.multiple_of(f * FCH + p * 256, 256), 256)
                    up = dot(x, w1[j, :, cols])
                    lin = dot(x, b3[slot, :, p * 256:(p + 1) * 256])
                    mid[:n, cols] = (jax.nn.silu(up) * lin).astype(BF16)

            over_rows(body)
            fetch(up_copy, g + RING)
            return c

        def down_step(f, c):
            g = a * NCH + f
            slot = lax.rem(g, RING)
            down_copy(g).wait()

            def body(n):
                cols = pl.ds(pl.multiple_of(f * DCH, DCH), DCH)
                xbuf[:n, cols] = dot(mid[:n, :], b2[slot]).astype(BF16)

            over_rows(body)
            fetch(down_copy, g + RING)
            return c

        lax.fori_loop(0, NCH, up_step, 0)
        lax.fori_loop(0, NCH, down_step, 0)
        at = jnp.int32(0)
        for s in range(GROUP):
            put = pos[s]
            ye_ref[s, pl.ds(pl.multiple_of(put, 16), EXTRA), :] = xbuf[pl.ds(pl.multiple_of(at, 16), EXTRA), :]
            at = at + tiles(s, j)
            pos[s] = put + tiles(s, j)
        return carry

    lax.fori_loop(0, active, expert, 0)

    @pl.when(index == 1)
    def _():
        def pool(s, carry):
            own = pos[s]

            @pl.when(own < EXTRA)
            def _():
                ye_ref[s, pl.ds(pl.multiple_of(own, 16), EXTRA), :] = jnp.zeros((EXTRA, WIDTH), BF16)

            behind = jnp.minimum(sum(tiles(s, LOCAL + j) for j in range(LOCAL)), EXTRA)
            for t in range(EXTRA // 16):
                @pl.when((own > EXTRA + 16 * t) & (behind + 16 * t < EXTRA))
                def _():
                    ov_ref[s, pl.ds(pl.multiple_of(behind + 16 * t, 16), 16), :] = ye_ref[s, EXTRA + 16 * t:EXTRA + 16 * (t + 1), :]
            return carry

        lax.fori_loop(0, GROUP, pool, 0)


def extra(cnt, xe, w1, w3, w2):
    hbm = pl.BlockSpec(memory_space=pl.ANY)
    vmem = pl.BlockSpec(memory_space=pltpu.VMEM)
    dma = pltpu.SemaphoreType.DMA
    return pl.pallas_call(
        extra_kernel,
        name="extra_rows",
        out_shape=[jax.ShapeDtypeStruct((GROUP, LOCAL * EXTRA, WIDTH), BF16), jax.ShapeDtypeStruct((GROUP, EXTRA, WIDTH), BF16),
                   jax.ShapeDtypeStruct((1,), I32)],
        in_specs=[pl.BlockSpec(memory_space=pltpu.SMEM), vmem, vmem, hbm, hbm],
        out_specs=[vmem] * 2 + [pl.BlockSpec(memory_space=pltpu.SMEM)],
        scratch_shapes=[
            pltpu.VMEM((XROWS, WIDTH), BF16),
            pltpu.VMEM((GROUP * EXTRA, FFN), BF16),
            pltpu.VMEM((RING, WIDTH, FCH), BF16),
            pltpu.VMEM((RING, FFN, DCH), BF16),
            pltpu.SMEM((LOCAL + 1,), I32),
            pltpu.SMEM((GROUP,), I32),
            dma((RING,)), dma((RING,)),
        ],
        compiler_params=pltpu.CompilerParams(vmem_limit_bytes=EXPERT_VMEM * 2**20),
        cost_estimate=pl.CostEstimate(flops=8 * 10**9, bytes_accessed=30 * 10**6, transcendentals=0),
    )(cnt, xe, w1, w3, w2)


def base_kernel(cap, pooled, scale, ids_ref, wr_ref, tab_ref, h_ref, xb_ref, ye_ref, ov_ref, w1, w3, w2, out_ref,
                land_e, land_b, yb, mid, b3, b2, mix, pool, w3_sem, w2_sem, e_send, e_recv, o_send, o_recv, b_send, b_recv):
    me = lax.axis_index("ep")

    def up_copy(j, f):
        return pltpu.make_async_copy(w3.at[j, :, pl.ds(pl.multiple_of(f * FCH, FCH), FCH)], b3.at[f], w3_sem.at[f])

    def down_copy(j, f):
        return pltpu.make_async_copy(w2.at[j, :, pl.ds(pl.multiple_of(f * DCH, DCH), DCH)], b2.at[f], w2_sem.at[f])

    for f in range(NCH):
        up_copy(0, f).start()
    for f in range(NCH):
        down_copy(0, f).start()

    barrier = pltpu.get_barrier_semaphore()
    for k in range(1, GROUP):
        pl.semaphore_signal(barrier, inc=1, device_id={"ep": lax.rem(me + k, GROUP)}, device_id_type=MESH)
    pl.semaphore_wait(barrier, GROUP - 1)

    out_e = pool.at[1] if pooled else ye_ref

    def e_copy(k):
        to = lax.rem(me + k, GROUP)
        return pltpu.make_async_remote_copy(src_ref=out_e.at[to, pl.ds(0, cap), :], dst_ref=land_e.at[me], send_sem=e_send.at[k], recv_sem=e_recv.at[k],
                                            device_id={"ep": to}, device_id_type=MESH)

    if pooled:
        mate = me + 1 - 2 * lax.rem(me, 2)

        def over(sender, to, k):
            return pltpu.make_async_remote_copy(src_ref=ov_ref.at[to], dst_ref=pool.at[0, to], send_sem=o_send.at[k], recv_sem=o_recv.at[k],
                                                device_id={"ep": sender}, device_id_type=MESH)

        order = [1, 2, 3, 4, 5, 6, 7, 0]
        for k in order:
            over(mate, lax.rem(mate + k, GROUP), k).start()
        for k in order:
            to = lax.rem(me + k, GROUP)
            over(mate, to, k).wait_recv()
            pool[1, to] = ye_ref[to, :EXTRA, :] + pool[0, to]
            if k > 0:
                e_copy(k).start()
    else:
        for k in range(1, GROUP):
            e_copy(k).start()
    land_e[me] = out_e[me, :cap, :]

    def b_copy(j, k):
        to = lax.rem(me + k, GROUP)
        return pltpu.make_async_remote_copy(src_ref=yb.at[j, pl.ds(pl.multiple_of(to * BASE, BASE), BASE), :],
                                            dst_ref=land_b.at[me, pl.ds(pl.multiple_of(j * BASE, BASE), BASE), :],
                                            send_sem=b_send.at[j, k], recv_sem=b_recv.at[j, k],
                                            device_id={"ep": to}, device_id_type=MESH)

    def expert(j, carry):
        def up_step(f, c):
            up_copy(j, f).wait()
            x = xb_ref[j]
            for p in range(FCH // 256):
                cols = pl.ds(pl.multiple_of(f * FCH + p * 256, 256), 256)
                up = dot(x, w1[j, :, cols])
                lin = dot(x, b3[f, :, p * 256:(p + 1) * 256])
                mid[:, cols] = (jax.nn.silu(up) * lin).astype(BF16)

            @pl.when(j + 1 < LOCAL)
            def _():
                up_copy(j + 1, f).start()
            return c

        def down_step(f, c):
            down_copy(j, f).wait()
            yb[j, :, pl.ds(pl.multiple_of(f * DCH, DCH), DCH)] = dot(mid[...], b2[f]).astype(BF16)

            @pl.when(j + 1 < LOCAL)
            def _():
                down_copy(j + 1, f).start()
            return c

        lax.fori_loop(0, NCH, up_step, 0)
        lax.fori_loop(0, NCH, down_step, 0)
        land_b[me, pl.ds(pl.multiple_of(j * BASE, BASE), BASE), :] = yb[j, pl.ds(pl.multiple_of(me * BASE, BASE), BASE), :]
        for k in range(1, GROUP):
            b_copy(j, k).start()
        return carry

    lax.fori_loop(0, LOCAL, expert, 0)

    wr = wr_ref[...]
    hb = h_ref[...]
    w_hi = wr.astype(BF16)
    rest = wr - w_hi.astype(F32)
    w_mid = rest.astype(BF16)
    w_lo = (rest - w_mid.astype(F32)).astype(BF16)
    logits = dot_t(w_hi, hb) + (dot_t(w_mid, hb) + dot_t(w_lo, hb))
    prob = jnp.exp(logits - jnp.max(logits, axis=0, keepdims=True))
    prob = prob / jnp.sum(prob, axis=0, keepdims=True)
    e_iota = lax.broadcasted_iota(I32, (EXPERTS, TOK), 0)
    pick0 = jnp.sum(jnp.where(e_iota == ids_ref[0:1, :], prob, 0.0), axis=0, keepdims=True)
    pick1 = jnp.sum(jnp.where(e_iota == ids_ref[1:2, :], prob, 0.0), axis=0, keepdims=True)
    both = pick0 + pick1
    gates = jnp.concatenate([pick0 / both, pick1 / both, jnp.zeros((126, TOK), F32)], axis=0).T

    def table(own, field, start, size):
        place = tab_ref[:, field:field + 1]
        inside = (place >= start) & (place < start + size)
        col = jnp.where(inside, tab_ref[:, own:own + 1] * size + place - start, -1.0).astype(I32)
        return (col == lax.broadcasted_iota(I32, (TOK, GROUP * size), 1)).astype(F32).astype(BF16)

    own_at, pos_at = (3, 4) if pooled else (0, 2)
    early = (LOCAL - 1) * BASE
    gate0, gate1 = scale[1] * gates[:, 0:1], scale[1] * gates[:, 1:2]
    far0, far1 = table(own_at, pos_at, 0, cap), table(FIELDS + own_at, FIELDS + pos_at, 0, cap)
    near0, near1 = table(0, 1, 0, early), table(FIELDS, FIELDS + 1, 0, early)
    last0, last1 = table(0, 1, early, BASE), table(FIELDS, FIELDS + 1, early, BASE)
    for k in range(1, GROUP):
        e_copy(k).wait()
    if pooled:
        for k in range(GROUP):
            over(mate, lax.rem(mate + k, GROUP), k).wait_send()
    far = land_e[...].reshape(GROUP * cap, WIDTH)
    mix[...] = scale[0] * h_ref[...].astype(F32) + (gate0 * dot(far0, far) + gate1 * dot(far1, far))
    for j in range(LOCAL - 1):
        for k in range(1, GROUP):
            b_copy(j, k).wait()
    near = land_b[:, :early, :].reshape(GROUP * early, WIDTH)
    mix[...] += gate0 * dot(near0, near) + gate1 * dot(near1, near)
    for k in range(1, GROUP):
        b_copy(LOCAL - 1, k).wait()
    last = land_b[:, early:, :].reshape(GROUP * BASE, WIDTH)
    out_ref[...] = (mix[...] + (gate0 * dot(last0, last) + gate1 * dot(last1, last))).astype(BF16)


def base(index, cap, pooled, scale, ids_t, wr_t, tab, hidden, xb, ye, ov, w1, w3, w2):
    vmem = pl.BlockSpec(memory_space=pltpu.VMEM)
    hbm = pl.BlockSpec(memory_space=pl.ANY)
    dma = pltpu.SemaphoreType.DMA
    return pl.pallas_call(
        functools.partial(base_kernel, cap, pooled),
        name=f"base_{cap}{'_pooled' if pooled else ''}",
        out_shape=jax.ShapeDtypeStruct((TOK, WIDTH), BF16),
        in_specs=[pl.BlockSpec(memory_space=pltpu.SMEM)] + [vmem] * 8 + [hbm] * 2,
        out_specs=vmem,
        scratch_shapes=[
            pltpu.VMEM((GROUP, cap, WIDTH), BF16),
            pltpu.VMEM((GROUP, LOCAL * BASE, WIDTH), BF16),
            pltpu.VMEM((LOCAL, BROWS, WIDTH), BF16),
            pltpu.VMEM((BROWS, FFN), BF16),
            pltpu.VMEM((RING, WIDTH, FCH), BF16),
            pltpu.VMEM((RING, FFN, DCH), BF16),
            pltpu.VMEM((TOK, WIDTH), F32),
            pltpu.VMEM((2, GROUP, EXTRA if pooled else 16, WIDTH), BF16),
            dma((RING,)), dma((RING,)),
            dma((GROUP,)), dma((GROUP,)), dma((GROUP,)), dma((GROUP,)), dma((LOCAL, GROUP)), dma((LOCAL, GROUP)),
        ],
        compiler_params=pltpu.CompilerParams(collective_id=2 + index, has_side_effects=True, vmem_limit_bytes=BASE_VMEM * 2**20),
    )(scale, ids_t, wr_t, tab, hidden, xb, ye, ov, w1, w3, w2)


def solution(mesh):
    def local_step(hidden, router_w, expert_ids, w_gate, w_up, w_down, post_scale):
        ids_t, wr_t = expert_ids.T, router_w.T
        xb, xe, cnt, tab = gather(ids_t, hidden)
        ye, ov, top = extra(cnt, xe, w_gate, w_up, w_down)
        plans = [(EXTRA, False), (EXTRA, True)] + [(cap, False) for cap in BUCKETS[1:]]
        branches = [functools.partial(base, i, cap, pooled) for i, (cap, pooled) in enumerate(plans)]
        return lax.switch(top[0], branches, post_scale, ids_t, wr_t, tab, hidden, xb, ye, ov, w_gate, w_up, w_down)

    tok_spec = P(("dp", "ep"))
    return jax.shard_map(local_step, mesh=mesh, in_specs=(tok_spec, P(), tok_spec, P("ep"), P("ep"), P("ep"), P()), out_specs=tok_spec, check_vma=False)
```

```python
import functools

import jax
import jax.numpy as jnp
from jax import lax
from jax.experimental import pallas as pl
from jax.experimental.pallas import tpu as pltpu
from jax.sharding import PartitionSpec as P

MESH = pl.DeviceIdType.MESH
BF16, F32, I32 = jnp.bfloat16, jnp.float32, jnp.int32
GROUP = 8
LOCAL = 4
EXPERTS = GROUP * LOCAL
TOK = 256
SLOTS = 64
WIDTH = 1536
FFN = 2304
CHUNKS = 4
BASE = 16
EXTRA = SLOTS - BASE
BROWS = GROUP * BASE
BUCKETS = tuple(EXTRA * (i + 1) for i in range(LOCAL))
FCH = 768
NCH = FFN // FCH
DCH = 512
RING = NCH
XROWS = GROUP * EXTRA + 128
FIELDS = 5
GATHER_VMEM = 15
EXPERT_VMEM = 20
BASE_VMEM = 27


def dot(a, b):
    return jnp.dot(a, b, preferred_element_type=F32)


def dot_t(a, b):
    return lax.dot_general(a, b, (((1,), (1,)), ((), ())), preferred_element_type=F32)


def extra_rows(count):
    over = jnp.maximum(count - BASE, 0.0)
    return jnp.floor((over + 15.0) * (1.0 / 16.0)) * 16.0


def gather_kernel(ids_hbm, h_hbm, xb_ref, xe_ref, cnt_ref, tab_ref,
                  ids_ref, h_ref, in_sem, hall, rk, idbuf, needs, id_send, id_recv, x_send, y_send, p_send, x_recv, y_recv, d_recv, p_recv, own_sem):
    dp, me = lax.axis_index("dp"), lax.axis_index("ep")
    core, xc, yc = lax.rem(me, 2), lax.rem(me // 2, 2), me // 4
    xn, yn, pc = me + 2 - 4 * xc, me + 4 - 8 * yc, me + 1 - 2 * core
    dg = xn + 4 - 8 * yc
    rows = TOK // CHUNKS
    inputs = [pltpu.make_async_copy(src, dst, in_sem.at[i]) for i, (src, dst) in enumerate([(ids_hbm, ids_ref), (h_hbm, h_ref)])]
    for copy in inputs:
        copy.start()

    barrier = pltpu.get_barrier_semaphore()
    for k in range(1, GROUP):
        pl.semaphore_signal(barrier, inc=1, device_id={"ep": lax.rem(me + k, GROUP)}, device_id_type=MESH)
    pl.semaphore_signal(barrier, inc=1, device_id={"dp": 1 - dp, "ep": me}, device_id_type=MESH)
    pl.semaphore_wait(barrier, GROUP)

    def piece(block, q):
        return hall.at[block, pl.ds(q * rows, rows), :]

    def mine(q):
        return h_ref.at[pl.ds(q * rows, rows), :]

    def remote(src, dst, send, recv, dev):
        return pltpu.make_async_remote_copy(src_ref=src, dst_ref=dst, send_sem=send, recv_sem=recv,
                                            device_id={"ep": dev}, device_id_type=MESH)

    half = CHUNKS // 2
    sends = []

    def start(copy):
        copy.start()
        sends.append(copy)

    def send_x(q):
        start(remote(mine(q), piece(me, q), x_send.at[q], x_recv.at[q], xn))

    def send_y(q):
        start(remote(mine(q), piece(me, q), y_send.at[q], y_recv.at[q], yn))

    inputs[0].wait()
    id_copies = []
    for k in range(1, GROUP):
        id_copies.append(remote(ids_ref, idbuf.at[me], id_send.at[k], id_recv.at[k], lax.rem(me + k, GROUP)))
        id_copies[-1].start()
    inputs[1].wait()
    for i in range(CHUNKS):
        send_x(i)
        send_y((i + half) % CHUNKS)
    start(remote(h_ref, hall.at[me], p_send.at[3 * CHUNKS], p_recv.at[3 * CHUNKS], pc))
    own_ids = pltpu.make_async_copy(ids_ref, idbuf.at[me], own_sem.at[0])
    own_ids.start()

    upper = (lax.broadcasted_iota(I32, (TOK, TOK), 0) < lax.broadcasted_iota(I32, (TOK, TOK), 1)).astype(BF16)
    hb = h_ref[...]
    e_iota = lax.broadcasted_iota(I32, (EXPERTS, TOK), 0)
    id0, id1 = ids_ref[0:1, :], ids_ref[1:2, :]
    hit0, hit1 = e_iota == id0, e_iota == id1
    hits = jnp.where(hit0 | hit1, 1.0, 0.0)
    rank = dot(hits.astype(BF16), upper)
    er, ec = lax.broadcasted_iota(I32, (EXPERTS, EXPERTS), 0), lax.broadcasted_iota(I32, (EXPERTS, EXPERTS), 1)
    before = ((er // LOCAL == ec // LOCAL) & (ec < er)).astype(BF16)
    extra = extra_rows(jnp.sum(hits, axis=1, keepdims=True))
    wide = jnp.broadcast_to(extra, (EXPERTS, 128)).astype(BF16)
    start_e = dot(before, wide)[:, 0:1]
    partner = (er // (2 * LOCAL) == ec // (2 * LOCAL)) & (er // LOCAL != ec // LOCAL)
    partner_rows = dot(partner.astype(BF16), wide)[:, 0:1]
    owner = lax.broadcasted_iota(I32, (EXPERTS, 1), 0) // LOCAL
    local = (lax.broadcasted_iota(I32, (EXPERTS, 1), 0) % LOCAL).astype(F32)
    place_b = jnp.where(rank < BASE, local * BASE + rank, -1.0)
    place_e = jnp.where(rank < BASE, -1.0, start_e + rank - BASE)
    moved = place_e >= EXTRA
    place_p = jnp.where(moved, jnp.minimum(partner_rows, EXTRA) + place_e - EXTRA, place_e)
    own_p = jnp.where(moved, owner + 1 - 2 * (owner % 2), owner).astype(F32)
    rows_of = []
    for hit in (hit0, hit1):
        rows_of += [jnp.sum(jnp.where(hit, v, 0.0), axis=0, keepdims=True) for v in (owner.astype(F32), place_b, place_e, own_p, place_p)]
    tab_ref[...] = jnp.concatenate(rows_of + [jnp.zeros((128 - len(rows_of), TOK), F32)], axis=0).T

    own_ids.wait()
    for copy in id_copies:
        copy.wait()
    j_iota = lax.broadcasted_iota(I32, (8, TOK), 0)
    local_id = jnp.where(j_iota < LOCAL, me * LOCAL + j_iota, (pc - 1) * LOCAL + j_iota)
    hit_list = []
    for s in range(GROUP):
        pair = idbuf[s]
        hit_list.append((local_id == pair[0:1, :]) | (local_id == pair[1:2, :]))
    hit_f = jnp.where(jnp.concatenate(hit_list, axis=0), 1.0, 0.0)
    hit_b = hit_f.astype(BF16)
    rk[...] = jnp.where(hit_f > 0.5, dot(hit_b, upper), -1.0).astype(I32).reshape(GROUP, 8, TOK)
    cnt_ref[:, 0:GROUP * 8] = extra_rows(dot_t(jnp.ones((8, TOK), BF16), hit_b)).astype(I32)
    lane = lax.broadcasted_iota(I32, (EXPERTS, 128), 1)
    spread = jnp.zeros((EXPERTS, 128), F32)
    for g in range(GROUP):
        pair = idbuf[g]
        n = jnp.where((e_iota == pair[0:1, :]) | (e_iota == pair[1:2, :]), 1.0, 0.0)
        spread = jnp.where(lane == g, extra_rows(jnp.sum(n, axis=1, keepdims=True)), spread)
    d_iota, o_iota = lax.broadcasted_iota(I32, (GROUP, EXPERTS), 0), lax.broadcasted_iota(I32, (GROUP, EXPERTS), 1) // LOCAL
    spread = spread.astype(BF16)
    need = dot((d_iota == o_iota).astype(BF16), spread)
    near = dot((d_iota + 1 - 2 * (d_iota % 2) == o_iota).astype(BF16), spread)
    pooled = jnp.maximum(need - EXTRA, 0.0) + jnp.minimum(near, EXTRA)
    needs[0, 0] = jnp.broadcast_to(jnp.max(jnp.max(need, axis=1, keepdims=True), axis=0, keepdims=True), (8, 128))
    needs[0, 1] = jnp.broadcast_to(jnp.max(jnp.max(pooled, axis=1, keepdims=True), axis=0, keepdims=True), (8, 128))

    def arrived(block, q, sem):
        remote(piece(block, q), piece(block, q), x_send.at[0], sem, xn).wait_recv()

    for i in range(half):
        a, b = i, i + half
        arrived(xn, a, x_recv.at[a])
        start(remote(piece(xn, a), piece(xn, a), y_send.at[CHUNKS + i], d_recv.at[a], yn))
        start(remote(piece(xn, a), piece(xn, a), p_send.at[a], p_recv.at[a], pc))
        arrived(yn, b, y_recv.at[b])
        start(remote(piece(yn, b), piece(yn, b), x_send.at[CHUNKS + i], d_recv.at[b], xn))
        start(remote(piece(yn, b), piece(yn, b), p_send.at[CHUNKS + b], p_recv.at[CHUNKS + b], pc))
    other = pltpu.make_async_remote_copy(src_ref=needs.at[0], dst_ref=needs.at[1], send_sem=id_send.at[0], recv_sem=id_recv.at[0],
                                         device_id={"dp": 1 - dp, "ep": me}, device_id_type=MESH)
    other.start()

    b_iota = lax.broadcasted_iota(I32, (BASE, TOK), 0)
    x_iota = lax.broadcasted_iota(I32, (EXTRA, TOK), 0) + BASE

    def pick(s, block):
        ranks = rk[s]
        table = jnp.concatenate([(b_iota == ranks[j:j + 1, :]).astype(F32) for j in range(LOCAL)]
                                + [(x_iota == ranks[j:j + 1, :]).astype(F32) for j in range(LOCAL)], axis=0).astype(BF16)
        rows = dot(table, block).astype(BF16)
        for j in range(LOCAL):
            xb_ref[j, pl.ds(pl.multiple_of(s * BASE, BASE), BASE), :] = rows[j * BASE:(j + 1) * BASE]
        xe_ref[s] = rows[LOCAL * BASE:]

    pick(me, hb)
    remote(hall.at[pc], hall.at[pc], x_send.at[0], p_recv.at[3 * CHUNKS], pc).wait_recv()
    pick(pc, hall[pc])
    for i in range(half):
        a, b = i + half, i
        arrived(xn, a, x_recv.at[a])
        start(remote(piece(xn, a), piece(xn, a), p_send.at[a], p_recv.at[a], pc))
        arrived(yn, b, y_recv.at[b])
        start(remote(piece(yn, b), piece(yn, b), p_send.at[CHUNKS + b], p_recv.at[CHUNKS + b], pc))
    for i in range(half):
        for q in (i, i + half):
            arrived(dg, q, d_recv.at[q])
            start(remote(piece(dg, q), piece(dg, q), p_send.at[2 * CHUNKS + q], p_recv.at[2 * CHUNKS + q], pc))
        if i == 0:
            pick(xn, hall[xn])
            pick(yn, hall[yn])
    turn = 1 - 2 * core
    for q in range(CHUNKS):
        arrived(xn + turn, q, p_recv.at[q])
        arrived(yn + turn, q, p_recv.at[CHUNKS + q])
    pick(xn + turn, hall[xn + turn])
    pick(yn + turn, hall[yn + turn])
    pick(dg, hall[dg])
    for q in range(CHUNKS):
        arrived(dg + turn, q, p_recv.at[2 * CHUNKS + q])
    pick(dg + turn, hall[dg + turn])
    other.wait()
    need, pooled = jnp.maximum(needs[0, 0], needs[1, 0]), jnp.maximum(needs[0, 1], needs[1, 1])
    rest = sum((need > cap).astype(I32) for cap in BUCKETS[1:-1]) + 2
    index = jnp.where(need <= EXTRA, 0, jnp.where((pooled <= EXTRA) & (need <= 2 * EXTRA), 1, rest))
    cnt_ref[:, GROUP * 8:] = index[:, GROUP * 8:]
    for copy in sends:
        copy.wait_send()


def gather(ids_t, hidden):
    vmem = pl.BlockSpec(memory_space=pltpu.VMEM)
    dma = pltpu.SemaphoreType.DMA
    return pl.pallas_call(
        gather_kernel,
        name="gather_rows",
        out_shape=[
            jax.ShapeDtypeStruct((LOCAL, BROWS, WIDTH), BF16),
            jax.ShapeDtypeStruct((GROUP, LOCAL * EXTRA, WIDTH), BF16),
            jax.ShapeDtypeStruct((8, 128), I32),
            jax.ShapeDtypeStruct((TOK, 128), F32),
        ],
        in_specs=[pl.BlockSpec(memory_space=pltpu.HBM)] * 2,
        out_specs=[vmem] * 4,
        scratch_shapes=[
            pltpu.VMEM((2, TOK), I32),
            pltpu.VMEM((TOK, WIDTH), BF16),
            dma((2,)),
            pltpu.VMEM((GROUP, TOK, WIDTH), BF16),
            pltpu.VMEM((GROUP, 8, TOK), I32),
            pltpu.VMEM((GROUP, 2, TOK), I32),
            pltpu.VMEM((2, 2, 8, 128), F32),
            dma((GROUP,)), dma((GROUP,)),
            dma((2 * CHUNKS,)), dma((2 * CHUNKS,)), dma((3 * CHUNKS + 1,)),
            dma((CHUNKS,)), dma((CHUNKS,)), dma((CHUNKS,)), dma((3 * CHUNKS + 1,)),
            dma((1,)),
        ],
        compiler_params=pltpu.CompilerParams(collective_id=1, has_side_effects=True, vmem_limit_bytes=GATHER_VMEM * 2**20),
        cost_estimate=pl.CostEstimate(flops=20 * 10**9, bytes_accessed=20 * 10**6, transcendentals=0),
    )(ids_t, hidden)


def extra_kernel(cnt, xe_ref, w1, w3, w2, ye_ref, ov_ref, top_ref, xbuf, mid, b3, b2, act, pos, w3_sem, w2_sem):
    def tiles(s, j):
        return cnt[0, s * 8 + j]

    active = jnp.int32(0)
    for j in range(LOCAL):
        act[active] = j
        active = active + jnp.minimum(sum(tiles(s, j) for s in range(GROUP)), 1)
    chunks = active * NCH
    index = cnt[0, GROUP * 8]
    top_ref[0] = index

    def up_copy(g):
        slot = lax.rem(g, RING)
        cols = pl.ds(pl.multiple_of(lax.rem(g, NCH) * FCH, FCH), FCH)
        return pltpu.make_async_copy(w3.at[act[g // NCH], :, cols], b3.at[slot], w3_sem.at[slot])

    def down_copy(g):
        slot = lax.rem(g, RING)
        cols = pl.ds(pl.multiple_of(lax.rem(g, NCH) * DCH, DCH), DCH)
        return pltpu.make_async_copy(w2.at[act[g // NCH], :, cols], b2.at[slot], w2_sem.at[slot])

    def fetch(copy, g):
        @pl.when(g < chunks)
        def _():
            copy(g).start()

    for g in range(RING):
        fetch(up_copy, g)
    for g in range(RING):
        fetch(down_copy, g)

    ye_ref[:, :EXTRA, :] = jnp.zeros((GROUP, EXTRA, WIDTH), BF16)
    for s in range(GROUP):
        pos[s] = 0

    @pl.when(index == 1)
    def _():
        ov_ref[...] = jnp.zeros_like(ov_ref)

    @pl.when(index > 1)
    def _():
        ye_ref[:, EXTRA:, :] = jnp.zeros((GROUP, (LOCAL - 1) * EXTRA, WIDTH), BF16)

    def expert(a, carry):
        j = act[a]
        total = jnp.int32(0)
        for s in range(GROUP):
            xbuf[pl.ds(pl.multiple_of(total, 16), EXTRA), :] = xe_ref[s, pl.ds(pl.multiple_of(j * EXTRA, 16), EXTRA), :]
            total = total + tiles(s, j)
        xbuf[pl.ds(pl.multiple_of(total, 16), 128), :] = jnp.zeros((128, WIDTH), BF16)

        @pl.when((total > 128) & (total < GROUP * EXTRA - 128))
        def _():
            xbuf[pl.ds(pl.multiple_of(total + 128, 16), 128), :] = jnp.zeros((128, WIDTH), BF16)

        def over_rows(body):
            @pl.when(total <= 128)
            def _():
                body(128)

            @pl.when(total > 128)
            def _():
                body(GROUP * EXTRA)

        def up_step(f, c):
            g = a * NCH + f
            slot = lax.rem(g, RING)
            up_copy(g).wait()

            def body(n):
                x = xbuf[:n, :]
                for p in range(FCH // 256):
                    cols = pl.ds(pl.multiple_of(f * FCH + p * 256, 256), 256)
                    up = dot(x, w1[j, :, cols])
                    lin = dot(x, b3[slot, :, p * 256:(p + 1) * 256])
                    mid[:n, cols] = (jax.nn.silu(up) * lin).astype(BF16)

            over_rows(body)
            fetch(up_copy, g + RING)
            return c

        def down(n):
            for f in range(NCH):
                xbuf[:n, f * DCH:(f + 1) * DCH] = dot(mid[:n, :], b2[f]).astype(BF16)

        lax.fori_loop(0, NCH, up_step, 0)
        for f in range(NCH):
            down_copy(a * NCH + f).wait()
        over_rows(down)
        for f in range(NCH):
            fetch(down_copy, (a + 1) * NCH + f)
        at = jnp.int32(0)
        for s in range(GROUP):
            put = pos[s]
            ye_ref[s, pl.ds(pl.multiple_of(put, 16), EXTRA), :] = xbuf[pl.ds(pl.multiple_of(at, 16), EXTRA), :]
            at = at + tiles(s, j)
            pos[s] = put + tiles(s, j)
        return carry

    lax.fori_loop(0, active, expert, 0)

    @pl.when(index == 1)
    def _():
        def pool(s, carry):
            own = pos[s]

            @pl.when(own < EXTRA)
            def _():
                ye_ref[s, pl.ds(pl.multiple_of(own, 16), EXTRA), :] = jnp.zeros((EXTRA, WIDTH), BF16)

            behind = jnp.minimum(sum(tiles(s, LOCAL + j) for j in range(LOCAL)), EXTRA)
            for t in range(EXTRA // 16):
                @pl.when((own > EXTRA + 16 * t) & (behind + 16 * t < EXTRA))
                def _():
                    ov_ref[s, pl.ds(pl.multiple_of(behind + 16 * t, 16), 16), :] = ye_ref[s, EXTRA + 16 * t:EXTRA + 16 * (t + 1), :]
            return carry

        lax.fori_loop(0, GROUP, pool, 0)


def extra(cnt, xe, w1, w3, w2):
    hbm = pl.BlockSpec(memory_space=pl.ANY)
    vmem = pl.BlockSpec(memory_space=pltpu.VMEM)
    dma = pltpu.SemaphoreType.DMA
    return pl.pallas_call(
        extra_kernel,
        name="extra_rows",
        out_shape=[jax.ShapeDtypeStruct((GROUP, LOCAL * EXTRA, WIDTH), BF16), jax.ShapeDtypeStruct((GROUP, EXTRA, WIDTH), BF16),
                   jax.ShapeDtypeStruct((1,), I32)],
        in_specs=[pl.BlockSpec(memory_space=pltpu.SMEM), vmem, vmem, hbm, hbm],
        out_specs=[vmem] * 2 + [pl.BlockSpec(memory_space=pltpu.SMEM)],
        scratch_shapes=[
            pltpu.VMEM((XROWS, WIDTH), BF16),
            pltpu.VMEM((GROUP * EXTRA, FFN), BF16),
            pltpu.VMEM((RING, WIDTH, FCH), BF16),
            pltpu.VMEM((RING, FFN, DCH), BF16),
            pltpu.SMEM((LOCAL + 1,), I32),
            pltpu.SMEM((GROUP,), I32),
            dma((RING,)), dma((RING,)),
        ],
        compiler_params=pltpu.CompilerParams(vmem_limit_bytes=EXPERT_VMEM * 2**20),
        cost_estimate=pl.CostEstimate(flops=8 * 10**9, bytes_accessed=30 * 10**6, transcendentals=0),
    )(cnt, xe, w1, w3, w2)


def base_kernel(cap, pooled, scale, ids_ref, wr_ref, tab_ref, h_ref, xb_ref, ye_ref, ov_ref, w1, w3, w2, out_ref,
                land_e, land_b, yb, mid, b3, b2, mix, pool, w3_sem, w2_sem, e_send, e_recv, o_send, o_recv, b_send, b_recv):
    me = lax.axis_index("ep")

    def up_copy(j, f):
        return pltpu.make_async_copy(w3.at[j, :, pl.ds(pl.multiple_of(f * FCH, FCH), FCH)], b3.at[f], w3_sem.at[f])

    def down_copy(j, f):
        return pltpu.make_async_copy(w2.at[j, :, pl.ds(pl.multiple_of(f * DCH, DCH), DCH)], b2.at[f], w2_sem.at[f])

    for f in range(NCH):
        up_copy(0, f).start()
    for f in range(NCH):
        down_copy(0, f).start()

    barrier = pltpu.get_barrier_semaphore()
    for k in range(1, GROUP):
        pl.semaphore_signal(barrier, inc=1, device_id={"ep": lax.rem(me + k, GROUP)}, device_id_type=MESH)
    pl.semaphore_wait(barrier, GROUP - 1)

    out_e = pool.at[1] if pooled else ye_ref

    def e_copy(k):
        to = lax.rem(me + k, GROUP)
        return pltpu.make_async_remote_copy(src_ref=out_e.at[to, pl.ds(0, cap), :], dst_ref=land_e.at[me], send_sem=e_send.at[k], recv_sem=e_recv.at[k],
                                            device_id={"ep": to}, device_id_type=MESH)

    if pooled:
        mate = me + 1 - 2 * lax.rem(me, 2)

        def over(sender, to, k):
            return pltpu.make_async_remote_copy(src_ref=ov_ref.at[to], dst_ref=pool.at[0, to], send_sem=o_send.at[k], recv_sem=o_recv.at[k],
                                                device_id={"ep": sender}, device_id_type=MESH)

        order = [1, 2, 3, 4, 5, 6, 7, 0]
        for k in order:
            over(mate, lax.rem(mate + k, GROUP), k).start()
        for k in order:
            to = lax.rem(me + k, GROUP)
            over(mate, to, k).wait_recv()
            pool[1, to] = ye_ref[to, :EXTRA, :] + pool[0, to]
            if k > 0:
                e_copy(k).start()
    else:
        for k in range(1, GROUP):
            e_copy(k).start()
    land_e[me] = out_e[me, :cap, :]

    def b_copy(j, k):
        to = lax.rem(me + k, GROUP)
        return pltpu.make_async_remote_copy(src_ref=yb.at[j, pl.ds(pl.multiple_of(to * BASE, BASE), BASE), :],
                                            dst_ref=land_b.at[me, pl.ds(pl.multiple_of(j * BASE, BASE), BASE), :],
                                            send_sem=b_send.at[j, k], recv_sem=b_recv.at[j, k],
                                            device_id={"ep": to}, device_id_type=MESH)

    def expert(j, carry):
        def up_step(f, c):
            up_copy(j, f).wait()
            x = xb_ref[j]

            def part(p, d):
                cols = pl.ds(pl.multiple_of(f * FCH + p * 256, 256), 256)
                up = dot(x, w1[j, :, cols])
                lin = dot(x, b3[f, :, pl.ds(pl.multiple_of(p * 256, 256), 256)])
                mid[:, cols] = (jax.nn.silu(up) * lin).astype(BF16)
                return d

            lax.fori_loop(0, FCH // 256, part, 0)

            @pl.when(j + 1 < LOCAL)
            def _():
                up_copy(j + 1, f).start()
            return c

        def down_step(f, c):
            down_copy(j, f).wait()
            yb[j, :, pl.ds(pl.multiple_of(f * DCH, DCH), DCH)] = dot(mid[...], b2[f]).astype(BF16)

            @pl.when(j + 1 < LOCAL)
            def _():
                down_copy(j + 1, f).start()
            return c

        lax.fori_loop(0, NCH, up_step, 0)
        lax.fori_loop(0, NCH, down_step, 0)
        land_b[me, pl.ds(pl.multiple_of(j * BASE, BASE), BASE), :] = yb[j, pl.ds(pl.multiple_of(me * BASE, BASE), BASE), :]
        for k in range(1, GROUP):
            b_copy(j, k).start()
        return carry

    lax.fori_loop(0, LOCAL, expert, 0)

    wr = wr_ref[...]
    hb = h_ref[...]
    w_hi = wr.astype(BF16)
    rest = wr - w_hi.astype(F32)
    w_mid = rest.astype(BF16)
    w_lo = (rest - w_mid.astype(F32)).astype(BF16)
    logits = dot_t(w_hi, hb) + (dot_t(w_mid, hb) + dot_t(w_lo, hb))
    prob = jnp.exp(logits - jnp.max(logits, axis=0, keepdims=True))
    prob = prob / jnp.sum(prob, axis=0, keepdims=True)
    e_iota = lax.broadcasted_iota(I32, (EXPERTS, TOK), 0)
    pick0 = jnp.sum(jnp.where(e_iota == ids_ref[0:1, :], prob, 0.0), axis=0, keepdims=True)
    pick1 = jnp.sum(jnp.where(e_iota == ids_ref[1:2, :], prob, 0.0), axis=0, keepdims=True)
    both = pick0 + pick1
    gates = jnp.concatenate([pick0 / both, pick1 / both, jnp.zeros((126, TOK), F32)], axis=0).T

    def table(own, field, start, size):
        place = tab_ref[:, field:field + 1]
        inside = (place >= start) & (place < start + size)
        col = jnp.where(inside, tab_ref[:, own:own + 1] * size + place - start, -1.0).astype(I32)
        return (col == lax.broadcasted_iota(I32, (TOK, GROUP * size), 1)).astype(F32).astype(BF16)

    own_at, pos_at = (3, 4) if pooled else (0, 2)
    early = (LOCAL - 1) * BASE
    gate0, gate1 = scale[1] * gates[:, 0:1], scale[1] * gates[:, 1:2]
    far0, far1 = table(own_at, pos_at, 0, cap), table(FIELDS + own_at, FIELDS + pos_at, 0, cap)
    near0, near1 = table(0, 1, 0, early), table(FIELDS, FIELDS + 1, 0, early)
    last0, last1 = table(0, 1, early, BASE), table(FIELDS, FIELDS + 1, early, BASE)
    for k in range(1, GROUP):
        e_copy(k).wait()
    if pooled:
        for k in range(GROUP):
            over(mate, lax.rem(mate + k, GROUP), k).wait_send()
    far = land_e[...].reshape(GROUP * cap, WIDTH)
    mix[...] = scale[0] * h_ref[...].astype(F32) + (gate0 * dot(far0, far) + gate1 * dot(far1, far))
    for j in range(LOCAL - 1):
        for k in range(1, GROUP):
            b_copy(j, k).wait()
    near = land_b[:, :early, :].reshape(GROUP * early, WIDTH)
    mix[...] += gate0 * dot(near0, near) + gate1 * dot(near1, near)
    for k in range(1, GROUP):
        b_copy(LOCAL - 1, k).wait()
    last = land_b[:, early:, :].reshape(GROUP * BASE, WIDTH)
    out_ref[...] = (mix[...] + (gate0 * dot(last0, last) + gate1 * dot(last1, last))).astype(BF16)


def base(index, cap, pooled, scale, ids_t, wr_t, tab, hidden, xb, ye, ov, w1, w3, w2):
    vmem = pl.BlockSpec(memory_space=pltpu.VMEM)
    hbm = pl.BlockSpec(memory_space=pl.ANY)
    dma = pltpu.SemaphoreType.DMA
    return pl.pallas_call(
        functools.partial(base_kernel, cap, pooled),
        name=f"base_{cap}{'_pooled' if pooled else ''}",
        out_shape=jax.ShapeDtypeStruct((TOK, WIDTH), BF16),
        in_specs=[pl.BlockSpec(memory_space=pltpu.SMEM)] + [vmem] * 8 + [hbm] * 2,
        out_specs=vmem,
        scratch_shapes=[
            pltpu.VMEM((GROUP, cap, WIDTH), BF16),
            pltpu.VMEM((GROUP, LOCAL * BASE, WIDTH), BF16),
            pltpu.VMEM((LOCAL, BROWS, WIDTH), BF16),
            pltpu.VMEM((BROWS, FFN), BF16),
            pltpu.VMEM((RING, WIDTH, FCH), BF16),
            pltpu.VMEM((RING, FFN, DCH), BF16),
            pltpu.VMEM((TOK, WIDTH), F32),
            pltpu.VMEM((2, GROUP, EXTRA if pooled else 16, WIDTH), BF16),
            dma((RING,)), dma((RING,)),
            dma((GROUP,)), dma((GROUP,)), dma((GROUP,)), dma((GROUP,)), dma((LOCAL, GROUP)), dma((LOCAL, GROUP)),
        ],
        compiler_params=pltpu.CompilerParams(collective_id=2 + index, has_side_effects=True, vmem_limit_bytes=BASE_VMEM * 2**20),
    )(scale, ids_t, wr_t, tab, hidden, xb, ye, ov, w1, w3, w2)


def solution(mesh):
    def local_step(hidden, router_w, expert_ids, w_gate, w_up, w_down, post_scale):
        ids_t, wr_t = expert_ids.T, router_w.T
        xb, xe, cnt, tab = gather(ids_t, hidden)
        ye, ov, top = extra(cnt, xe, w_gate, w_up, w_down)
        plans = [(EXTRA, False), (EXTRA, True)] + [(cap, False) for cap in BUCKETS[1:]]
        branches = [functools.partial(base, i, cap, pooled) for i, (cap, pooled) in enumerate(plans)]
        return lax.switch(top[0], branches, post_scale, ids_t, wr_t, tab, hidden, xb, ye, ov, w_gate, w_up, w_down)

    tok_spec = P(("dp", "ep"))
    return jax.shard_map(local_step, mesh=mesh, in_specs=(tok_spec, P(), tok_spec, P("ep"), P("ep"), P("ep"), P()), out_specs=tok_spec, check_vma=False)
```
